32 devices in a mesh: facet: 8 (over z, x), col: 4 (over y, core).
Axes of the slice: x: 2, y: 2, z: 4, core: 2. Of those that a mesh axis runs over, the one named last changes fastest.
Arguments:
- facets: bfloat16 [2, 8192, 1024], P(None, ('facet', 'col')), may hold values from -6 to 6
- observed: float32 [2, 32, 1024], P(None, 'col'), may hold values from -6 to 6
- uv_cells: int32 [2, 32, 1024], P(None, 'col'), may hold values from 0 to 511
- counts: int32 [32], P('col'), may hold values from 64 to 1024, as said below
Outputs:
- facet_residual: float32 [2, 8192, 1024], P(None, ('facet', 'col'))
The draws below stay inside these ranges and needn't reach their ends.
Inputs may be any that keep to these rules, and one draw needn't show every extreme that they name: Live slots of a subgrid are its first counts[s] slots; in every column some subgrid has all 1024 slots live.
All inputs are finite; a program needn't handle non-finite values.
Results may differ from the reference program's by a relative error of at most 0.008.
Values may be sent and summed in bfloat16 or wider, within the bound.
A program may use at most 64 MiB of HBM per device.

```python
import math
import jax
import jax.numpy as jnp
from jax import lax

F = 1024
S = 512
IMAGE = 65536
VIS = 1024
SUB_W = 1
NFACET = 8
SUBCOL = 8
NSUB = 32
N_FACET = 8
N_COL = 4


def draw_counts(key, part):
    key_expo, key_drop, key_full = jax.random.split(key, 3)
    exponent = jax.random.randint(key_expo, (NSUB,), 0, 4)
    ceiling = VIS // jnp.left_shift(jnp.ones((NSUB,), jnp.int32), exponent)
    lowered = jax.random.randint(key_drop, (NSUB,), 0, VIS) % (ceiling // 2 + 1)
    column_rows = NSUB // SUBCOL
    shaped = (ceiling - lowered).reshape(column_rows, SUBCOL)
    chosen = jax.random.randint(key_full, (column_rows, 1), 0, SUBCOL)
    filled = jnp.where(jnp.arange(SUBCOL, dtype=jnp.int32)[None, :] == chosen, VIS, shaped)
    return filled.reshape(NSUB).astype(jnp.int32)


def touch_ends(values, key, least, high):
    longest = values.shape.index(max(values.shape))
    spots = []
    for shift in (0, 1):
        where = [jax.random.randint(jax.random.fold_in(key, axis), (), 0, length) for axis, length in enumerate(values.shape)]
        where[longest] = (where[longest] + shift) % values.shape[longest]
        spots.append(tuple(where))
    return values.at[spots[0]].set(least).at[spots[1]].set(high)


def shard_levels(stream_key, shape, cuts, low, high):
    def one(axis_at, blocks):
        draws = jax.random.uniform(jax.random.fold_in(jax.random.fold_in(stream_key, 6), axis_at), (blocks,), jnp.float32, low / len(cuts), high / len(cuts))
        return jnp.repeat(jnp.exp(draws), shape[axis_at] // blocks).reshape((-1,) + (1,) * (len(shape) - axis_at - 1))

    gain = one(*cuts[0])
    for cut in cuts[1:]:
        gain = gain * one(*cut)
    return gain


def scatter_about(key, dims, width, limit, pieces=(), held_as=jnp.bfloat16):
    values = jax.random.normal(key, dims, jnp.float32) * width
    if len(pieces) > 0:
        values = shard_levels(key, dims, pieces, -0.22, 0.18) * values
    return jnp.clip(values, min=-limit, max=limit).astype(held_as)


def setup_inputs(seed: int = 0) -> dict:
    key_of = jax.random.split(jax.random.key(seed), 5)
    return {
        "facets": scatter_about(key_of[0], (2, NFACET * F, F), 1.0, 6.0, ((1, 32),)),
        "observed": scatter_about(key_of[1], (2, NSUB, VIS), 1.0, 6.0, ((1, 4),), jnp.float32),
        "uv_cells": touch_ends(jax.random.randint(key_of[2], (2, NSUB, VIS), 0, S), jax.random.fold_in(key_of[2], 1), 0, S - 1).astype(jnp.int32),
        "counts": draw_counts(jax.random.fold_in(key_of[4], 71), 0),
    }


def multiply_mod(left_value, right_value):
    low_part = right_value % 256
    high_part = right_value // 256
    return (left_value * low_part + left_value * high_part % IMAGE * 256) % IMAGE

def taper_values(extent):
    position = (jnp.arange(extent, dtype=jnp.int32).astype(jnp.float32) + 0.5) / extent
    return 0.6 + 0.4 * jnp.sin(math.pi * position) ** 2

def unit_table(ticks, scale, modulus):
    angle = ticks.astype(jnp.float32) * (-2.0 * math.pi / modulus)
    return jnp.stack([jnp.cos(angle) * scale, jnp.sin(angle) * scale])

def row_table(facet_id, window, spacing, extent):
    cells = facet_id // 8 * extent + jnp.arange(extent, dtype=jnp.int32)
    freqs = IMAGE // window * jnp.arange(window, dtype=jnp.int32)
    ticks = multiply_mod(cells[None, :], freqs[:, None])
    weights = taper_values(extent)[None, :] / math.sqrt(extent)
    return unit_table(ticks, weights, IMAGE).astype(jnp.bfloat16)

def column_table(facet_id, columns, window, spacing, extent):
    cells = facet_id % 8 * extent + jnp.arange(extent, dtype=jnp.int32)
    anchor = columns * (IMAGE // 4) + (29 * columns + 3) % spacing
    freqs = (anchor[:, None] + spacing * jnp.arange(window, dtype=jnp.int32)[None, :]).reshape(-1)
    ticks = multiply_mod(cells[None, :], freqs[:, None])
    weights = taper_values(extent)[None, :] / math.sqrt(extent)
    return unit_table(ticks, weights, IMAGE).astype(jnp.bfloat16)

def phase_table(facet_id, subgrid_ids, spacing, extent):
    cells = facet_id // 8 * extent + jnp.arange(extent, dtype=jnp.int32)
    anchor = subgrid_ids * (IMAGE // 64) + (37 * subgrid_ids + 5) % (IMAGE * 8 // S)
    ticks = multiply_mod(cells[None, :], anchor[:, None])
    return unit_table(ticks, 1.0, IMAGE)

def facet_windows(row_tab, phases, strip):
    phase_real = phases[0][:, :, None]
    phase_imag = phases[1][:, :, None]
    strip_real = strip[0][None].astype(jnp.float32)
    strip_imag = strip[1][None].astype(jnp.float32)
    turned_real = (phase_real * strip_real - phase_imag * strip_imag).astype(jnp.bfloat16)
    turned_imag = (phase_real * strip_imag + phase_imag * strip_real).astype(jnp.bfloat16)

    def contract(table, turned):
        return jnp.einsum('ki,sil->skl', table.astype(jnp.float32), turned.astype(jnp.float32))
    window_real = contract(row_tab[0], turned_real) - contract(row_tab[1], turned_imag)
    window_imag = contract(row_tab[0], turned_imag) + contract(row_tab[1], turned_real)
    return jnp.stack([window_real, window_imag], axis=1).astype(jnp.bfloat16)

def facet_adjoint(row_tab, phases, returned):

    def contract(table, part):
        return jnp.einsum('ki,skl->sil', table.astype(jnp.float32), part.astype(jnp.float32))
    mixed_real = contract(row_tab[0], returned[:, 0]) + contract(row_tab[1], returned[:, 1])
    mixed_imag = contract(row_tab[0], returned[:, 1]) - contract(row_tab[1], returned[:, 0])

    def weigh(phase, mixed):
        return jnp.einsum('si,sil->il', phase, mixed, precision=lax.Precision.HIGHEST)
    real_part = weigh(phases[0], mixed_real) + weigh(phases[1], mixed_imag)
    imag_part = weigh(phases[0], mixed_imag) - weigh(phases[1], mixed_real)
    return jnp.stack([real_part, imag_part])

def regrid_block(subgrid_b, observed_part, first_cells, second_cells, is_live, extent):
    cell_axis = jnp.arange(extent, dtype=jnp.int32)
    left_tab = unit_table(first_cells[:, None] * cell_axis[None, :] % extent, 1.0, extent).astype(jnp.bfloat16)
    right_tab = unit_table(second_cells[:, None] * cell_axis[None, :] % extent, 1.0, extent)

    def product(alpha, beta):
        return jnp.dot(alpha, beta, preferred_element_type=jnp.float32)
    inner_real = product(left_tab[0], subgrid_b[0]) - product(left_tab[1], subgrid_b[1])
    inner_imag = product(left_tab[0], subgrid_b[1]) + product(left_tab[1], subgrid_b[0])
    predicted_real = lax.optimization_barrier(jnp.sum(inner_real * right_tab[0] - inner_imag * right_tab[1], axis=1)) / extent
    predicted_imag = lax.optimization_barrier(jnp.sum(inner_real * right_tab[1] + inner_imag * right_tab[0], axis=1)) / extent
    resid_real = jnp.where(is_live, observed_part[0] - predicted_real, 0.0)
    resid_imag = jnp.where(is_live, observed_part[1] - predicted_imag, 0.0)
    weighted_real = (resid_real[:, None] * right_tab[0] + resid_imag[:, None] * right_tab[1]).astype(jnp.bfloat16)
    weighted_imag = (resid_imag[:, None] * right_tab[0] - resid_real[:, None] * right_tab[1]).astype(jnp.bfloat16)
    regrid_real = product(left_tab[0].T, weighted_real) + product(left_tab[1].T, weighted_imag)
    regrid_imag = product(left_tab[0].T, weighted_imag) - product(left_tab[1].T, weighted_real)
    return (regrid_real, regrid_imag)

def reference(facets, observed, uv_cells, counts):
    facet_count = N_FACET
    column_count = N_COL
    per_column = SUB_W * N_FACET
    window = S // 8
    spacing = IMAGE // F
    stacked = facets.reshape(2, facet_count, F, F).transpose(1, 0, 2, 3)
    subgrid_ids = jnp.arange(per_column, dtype=jnp.int32)
    facet_ids = jnp.arange(facet_count, dtype=jnp.int32)
    accumulated = jnp.zeros((facet_count, 2, F, F), jnp.float32)
    for column_index in range(column_count):
        columns = jnp.array([column_index], jnp.int32)

        def forward(carried, item):
            facet_id, pixels = item
            colt = column_table(facet_id, columns, window, spacing, F)
            strip_real = jnp.dot(pixels[0], colt[0].T, preferred_element_type=jnp.float32) - jnp.dot(pixels[1], colt[1].T, preferred_element_type=jnp.float32)
            strip_imag = jnp.dot(pixels[0], colt[1].T, preferred_element_type=jnp.float32) + jnp.dot(pixels[1], colt[0].T, preferred_element_type=jnp.float32)
            strip = jnp.stack([strip_real, strip_imag]).astype(jnp.bfloat16)
            windows = facet_windows(row_table(facet_id, window, spacing, F), phase_table(facet_id, subgrid_ids, spacing, F), strip)
            zero_index = jnp.zeros((), jnp.int32)
            corner = (zero_index, zero_index, (facet_id % 32 // 8 * window).astype(jnp.int32), (facet_id % 8 * window).astype(jnp.int32))
            current = lax.dynamic_slice(carried, corner, (per_column, 2, window, window))
            carried = lax.dynamic_update_slice(carried, current + windows.astype(jnp.float32), corner)
            return (carried, None)
        initial = jnp.zeros((per_column, 2, S, S), jnp.float32)
        summed, unused = lax.scan(forward, initial, (facet_ids, stacked))
        subgrid_b = summed.astype(jnp.bfloat16)
        first_row = column_index * per_column
        column_obs = observed[:, first_row:first_row + per_column].transpose(1, 0, 2)
        column_uv = uv_cells[:, first_row:first_row + per_column]
        column_counts = counts[first_row:first_row + per_column]

        def per_subgrid(item):
            grid_part, observed_part, first_cells, second_cells, live_count = item
            is_live = jnp.arange(VIS, dtype=jnp.int32) < live_count
            regrid_real, regrid_imag = regrid_block(grid_part, observed_part, first_cells, second_cells, is_live, S)
            return jnp.stack([regrid_real, regrid_imag]) * (1.0 / math.sqrt(VIS))
        regridded = lax.map(per_subgrid, (subgrid_b, column_obs, column_uv[0], column_uv[1], column_counts))

        def backward(facet_id):
            colt = column_table(facet_id, columns, window, spacing, F)
            zero_index = jnp.zeros((), jnp.int32)
            corner = (zero_index, zero_index, (facet_id % 32 // 8 * window).astype(jnp.int32), (facet_id % 8 * window).astype(jnp.int32))
            returned = lax.dynamic_slice(regridded, corner, (per_column, 2, window, window)).astype(jnp.bfloat16)
            backstrip = facet_adjoint(row_table(facet_id, window, spacing, F), phase_table(facet_id, subgrid_ids, spacing, F), returned).astype(jnp.bfloat16)
            image_real = jnp.dot(backstrip[0], colt[0], preferred_element_type=jnp.float32) + jnp.dot(backstrip[1], colt[1], preferred_element_type=jnp.float32)
            image_imag = jnp.dot(backstrip[1], colt[0], preferred_element_type=jnp.float32) - jnp.dot(backstrip[0], colt[1], preferred_element_type=jnp.float32)
            return jnp.stack([image_real, image_imag])
        accumulated = accumulated + lax.map(backward, facet_ids)
    return accumulated.transpose(1, 0, 2, 3).reshape(2, facet_count * F, F)
```

```python
import functools
import math

import jax
import jax.numpy as jnp
import numpy as np
from jax import lax
from jax.experimental import pallas as pl
from jax.experimental.pallas import tpu as pltpu
from jax.sharding import PartitionSpec as P

S = 512
IMAGE = 65536
MESH = pl.DeviceIdType.MESH
BF = jnp.bfloat16
F32 = jnp.float32
NT = (((1,), (1,)), ((), ()))


def unit(ticks):
    angle = (np.asarray(ticks, np.int64) % IMAGE) * (-2.0 * math.pi / IMAGE)
    return np.cos(angle), np.sin(angle)


def make_constants(facets, columns, per_column, extent):
    window = S // 8
    spacing = IMAGE // extent
    cells = np.arange(extent, dtype=np.int64)
    weight = (0.6 + 0.4 * np.sin(math.pi * (cells + 0.5) / extent) ** 2) / math.sqrt(extent)
    step = np.arange(window, dtype=np.int64)
    col = np.arange(columns, dtype=np.int64)
    vc = col * (IMAGE // 4) + (29 * col + 3) % spacing
    sub = np.arange(per_column, dtype=np.int64)
    us = sub * (IMAGE // 64) + (37 * sub + 5) % (IMAGE * 8 // S)

    def table(start, stride):
        real, imag = unit((start[:, None] + stride * step)[:, :, None] * cells)
        rows = np.concatenate([real * weight, imag * weight], axis=1)
        return rows.reshape(-1, extent).astype(np.float32).astype(BF)

    col_tab = table(vc, spacing)
    wide = 2 - columns % 2
    strip_tab = col_tab.reshape(columns // wide, -1, extent).transpose(0, 2, 1)
    row_tab = table(us, IMAGE // window)
    assert extent % window == 0
    fy = extent * (np.arange(facets, dtype=np.int64) % 8)
    fx = extent * (np.arange(facets, dtype=np.int64) // 8)
    real, imag = unit((fy[:, None] * vc)[:, :, None] + (fx[:, None] * us)[:, None, :])
    same = np.stack([real, real], axis=-1)
    cross = np.stack([-imag, imag], axis=-1)
    turn = np.repeat(np.stack([same, cross], axis=3), window, axis=4)
    flat = np.ascontiguousarray
    return col_tab, flat(strip_tab), row_tab, flat(row_tab.T), turn.astype(np.float32)


def spin(value, first, second):
    half = value.shape[1] // 2
    lane = lax.broadcasted_iota(jnp.int32, value.shape, 1)
    return pltpu.roll(value, half, 1) * jnp.where(lane < half, first, second)


def sign(value, first, second):
    lane = lax.broadcasted_iota(jnp.int32, value.shape, 1)
    return value * jnp.where(lane < value.shape[1] // 2, first, second)


def cycle_kernel(
    nf, nc, x_hbm, obs_hbm, cells_hbm, counts_hbm, ctab_hbm, stab_hbm, rtab_hbm, ttab_hbm, turn_hbm,
    back_out, tab,
    xbuf, stab, obs, cells, counts, turn_in, turn_out, t2, tt, acc, bacc,
    s_send, s_recv, g_send, g_recv, right, right_t, r1r, r1i, left, obs_t, inner, held, r_send, r_recv, b_send, b_recv,
    tok, in_sem, tab_sem, sa, ra, sb, rb, sc, rc, sd, rd,
):
    f = lax.axis_index("facet")
    c = lax.axis_index("col")
    window = S // 8
    two = 2 * window
    parts = window // 16
    pc = nf
    rows = xbuf.shape[0] // 2
    groups = nf // 8
    vis = obs.shape[2]
    if nc % 2:
        col_steps = [(d, 0) for d in range(1, nc)]
        wide = 1
    else:
        col_steps = [(d, k) for d in range(nc // 2 - 1, -1, -1) for k in range(2) if d or k]
        wide = 2

    def col_at(step, sign):
        if nc % 2:
            return lax.rem(c + nc + sign * step[0], nc)
        top = lax.rem(c // 2 + nc // 2 + sign * step[0], nc // 2)
        return 2 * top + lax.rem(c + step[1], 2)

    def pair_at(q):
        return lax.rem(f // 2 + q, 4)

    def facet_link(src_buf, dst_buf, send, recv, peer, slot):
        return pltpu.make_async_remote_copy(
            src_buf.at[peer], dst_buf.at[slot], send.at[peer], recv.at[slot], (peer, c), MESH
        )

    def col_link(src_buf, dst_buf, send, recv, peer, slot):
        return pltpu.make_async_remote_copy(
            src_buf.at[peer], dst_buf.at[slot], send.at[peer], recv.at[slot], (f, peer), MESH
        )

    barrier = pltpu.get_barrier_semaphore()
    place, last_place = f // 2, nf // 2 - 1
    mate = f + 1 - 2 * lax.rem(f, 2)
    low, high = place > 0, place < last_place

    def signal(sem, facet, col):
        pl.semaphore_signal(sem, inc=1, device_id=(facet, col), device_id_type=MESH)

    inside = low & high

    def pass_on(way):
        pl.semaphore_wait(tok.at[way], 1)
        signal(tok.at[way], f + 2 - 4 * way, c)

    for d in range(1, nc):
        signal(barrier, f, lax.rem(c + d, nc))
    signal(barrier, mate, c)
    pl.when(high)(lambda: signal(barrier, f + 2, c))
    pl.when(low)(lambda: signal(barrier, f - 2, c))

    n_groups = nc // wide

    def group_at(d):
        return lax.rem(c // wide + n_groups + d, n_groups)

    group_order = list(range(n_groups - 1, -1, -1)) if wide == 2 else list(range(1, nc)) + [0]

    def tab_load(d):
        at = group_at(d)
        return pltpu.make_async_copy(stab_hbm.at[at], stab.at[at], tab_sem.at[d])

    x_loads = [
        pltpu.make_async_copy(x_hbm.at[k], xbuf.at[k * rows : (k + 1) * rows], in_sem.at[k])
        for k in range(2)
    ]
    row_load = pltpu.make_async_copy(rtab_hbm, t2, in_sem.at[2])
    small_loads = [
        pltpu.make_async_copy(turn_hbm.at[f, c], turn_in, in_sem.at[3]),
        pltpu.make_async_copy(turn_hbm.at[:, c, f], turn_out, in_sem.at[4]),
        pltpu.make_async_copy(obs_hbm, obs, in_sem.at[5]),
        pltpu.make_async_copy(cells_hbm, cells, in_sem.at[6]),
        pltpu.make_async_copy(counts_hbm, counts, in_sem.at[7]),
    ]
    image_load = pltpu.make_async_copy(ctab_hbm, tab, in_sem.at[9])
    back_load = pltpu.make_async_copy(ttab_hbm, tt, in_sem.at[8])
    for n, d in enumerate(group_order):
        tab_load(d).start()
        if n == 0:
            for load in x_loads:
                load.start()
    for load in small_loads:
        load.start()

    pl.semaphore_wait(barrier, nc + low.astype(jnp.int32) + high.astype(jnp.int32))
    pl.when(~low)(lambda: signal(tok.at[0], f + 2, c))
    pl.when(~high)(lambda: signal(tok.at[1], f - 2, c))

    for load in x_loads:
        load.wait()
    row_load.start()
    for n, d in enumerate(group_order):
        start = wide * group_at(d)
        tab_load(d).wait()
        both = jnp.dot(xbuf[...], stab[group_at(d)], preferred_element_type=F32)
        for k in range(wide):
            block = both[:, k * two : (k + 1) * two]
            s_send[start + k] = (block[:rows] + spin(block[rows:], -1.0, 1.0)).astype(BF)
        for step in col_steps:
            if step[0] == d:
                peer = col_at(step, 1)
                col_link(s_send, s_recv, sa, ra, peer, c).start()
        if n == 0:
            pl.when(inside & (place == last_place - 1))(functools.partial(pass_on, 1))
    pl.when(inside & (place == 1))(functools.partial(pass_on, 0))

    row_load.wait()

    def part_product(src, block, at, count):
        start = pl.multiple_of(src * rows, rows)
        return jnp.dot(
            t2[pl.ds(at, count), pl.ds(start, rows)], block, preferred_element_type=F32
        )

    acc[...] = part_product(c, s_send[c], 0, pc * two)

    pl.when(inside & (place != 1))(functools.partial(pass_on, 0))
    pl.when(inside & (place != last_place - 1))(functools.partial(pass_on, 1))

    for load in small_loads:
        load.wait()
    first = cells[0, pl.ds(f, 1), :]
    second = cells[1, pl.ds(f, 1), :]

    def wave(count, step, cell):
        index = step * lax.broadcasted_iota(jnp.int32, (count, vis), 0)
        angle = (index * cell & (S - 1)).astype(F32) * (-2.0 * math.pi / S)
        return jnp.cos(angle), jnp.sin(angle)

    scale = 1.0 / math.sqrt(vis)
    live = lax.broadcasted_iota(jnp.int32, (1, vis), 1) < counts[f]
    gain = jnp.where(live, scale, 0.0)
    m0r, m0i = wave(16, 1, second)
    m0r, m0i = m0r * gain, m0i * gain
    r1r[...], r1i[...] = wave(S // 16, 16, second)

    def right_body(i, carry):
        er, ei = r1r[pl.ds(i, 1), :], r1i[pl.ds(i, 1), :]
        b = i // parts
        at = pl.multiple_of(b * two + (i - b * parts) * 16, 16)
        right[pl.ds(at, 16), :] = (m0r * er - m0i * ei).astype(BF)
        right[pl.ds(at + window, 16), :] = (m0r * ei + m0i * er).astype(BF)
        return carry

    lax.fori_loop(0, S // 16, right_body, 0)

    def turn_body(i, carry):
        at = pl.multiple_of(i * two, two)
        block = right[pl.ds(at, two), :].astype(F32) * (1.0 / (scale * S))
        right_t[:, pl.ds(at, two)] = block.T.astype(BF)
        return carry

    lax.fori_loop(0, S // window, turn_body, 0)

    for step in col_steps[:0:-1]:
        src = col_at(step, -1)
        col_link(s_send, s_recv, sa, ra, src, src).wait_recv()
        acc[...] += part_product(src, s_recv[src], 0, pc * two)

    def each_facet(q, act):
        pair = pair_at(q)
        for g in range(groups):
            for h in range(2):
                index = g * 8 + 2 * pair + h
                if q == 0:
                    pl.when(index != f)(functools.partial(act, index))
                else:
                    act(index)

    def send_window(index):
        facet_link(g_send, g_recv, sb, rb, index, f).start()

    def take_window(index):
        facet_link(g_send, g_recv, sb, rb, index, index).wait_recv()

    def send_back(index):
        facet_link(r_send, r_recv, sc, rc, index, f).start()

    def take_back(index):
        facet_link(r_send, r_recv, sc, rc, index, index).wait_recv()

    far_first = (2, 3, 1, 0)
    src = col_at(col_steps[0], -1)
    col_link(s_send, s_recv, sa, ra, src, src).wait_recv()
    pl.when(~low)(lambda: pl.semaphore_wait(tok.at[1], 1))
    pl.when(~high)(lambda: pl.semaphore_wait(tok.at[0], 1))
    total = acc[...] + part_product(src, s_recv[src], 0, pc * two)
    for j in range(pc):
        u = total[j * two : j * two + window]
        v = total[j * two + window : (j + 1) * two]
        turn = turn_in[j]
        same, cross = turn[0:1], turn[1:2]
        win = u * same + spin(v, -1.0, 1.0) * same
        win += pltpu.roll(u, window, 1) * cross + v * sign(cross, 1.0, -1.0)
        g_send[j] = win.astype(BF)
    for q in far_first:
        each_facet(q, send_window)
    g_recv[f] = g_send[f]
    back_load.start()
    image_load.start()

    l0r, l0i = wave(16, 1, first)
    l1r, l1i = wave(max(groups * parts, 8), 16, first)
    for g in range(groups):
        reals, imags = [], []
        for k in range(parts):
            i = g * parts + k
            er, ei = l1r[i : i + 1], l1i[i : i + 1]
            reals.append(l0r * er - l0i * ei)
            imags.append(-(l0r * ei + l0i * er))
        turned = jnp.concatenate(reals + imags, axis=0).astype(BF).astype(F32)
        turned = turned.T
        left[0, :, g * two : (g + 1) * two] = turned
        left[1, :, g * two : (g + 1) * two] = spin(turned, -1.0, 1.0)
    for k in range(2):
        obs_t[k] = jnp.broadcast_to(obs[k, pl.ds(f, 1), :], (two, vis)).T

    def pred_chunk(q, g):
        pieces = []
        for h in range(2):
            block = g_recv[g * 8 + 2 * pair_at(q) + h].astype(F32)
            pieces.append(
                jnp.concatenate([sign(block, 1.0, -1.0), pltpu.roll(block, window, 1)], axis=0)
            )
        lanes = pl.multiple_of(pair_at(q) * 2 * two, 2 * two)
        return lax.dot_general(
            right_t[:, pl.ds(lanes, 2 * two)],
            jnp.concatenate(pieces, axis=1).astype(BF),
            NT,
            preferred_element_type=F32,
        )

    nearest = far_first[::-1]
    for q in nearest[:-1]:
        each_facet(q, take_window)
        for g in range(groups):
            at = slice(g * two, (g + 1) * two)
            if q == nearest[0]:
                inner[:, at] = pred_chunk(q, g)
            else:
                inner[:, at] += pred_chunk(q, g)
    each_facet(nearest[-1], take_window)
    ones = jnp.ones((two, two), BF)
    rest = [obs_t[0], obs_t[1]]
    for g in range(groups):
        at = slice(g * two, (g + 1) * two)
        value = inner[:, at] + pred_chunk(nearest[-1], g)
        for k in range(2):
            rest[k] -= jnp.dot(
                (value * left[k, :, at]).astype(BF), ones, preferred_element_type=F32
            )
    for g in range(groups):
        at = slice(g * two, (g + 1) * two)
        held[:, at] = (rest[0] * left[0, :, at] + rest[1] * left[1, :, at]).astype(BF)

    for n, q in enumerate(far_first):
        at = pl.multiple_of(pair_at(q) * 2 * two, 2 * two)
        grid = jnp.dot(right[pl.ds(at, 2 * two), :], held[...], preferred_element_type=F32)
        for g in range(groups):
            lanes = slice(g * two, (g + 1) * two)
            for h in range(2):
                u = grid[h * two : h * two + window, lanes]
                v = grid[h * two + window : (h + 1) * two, lanes]
                index = g * 8 + 2 * pair_at(q) + h
                turn = turn_out[index]
                same, cross = turn[0:1], turn[1:2]
                block = (u + spin(v, 1.0, -1.0)) * same
                block -= pltpu.roll(u, window, 1) * cross + v * sign(cross, -1.0, 1.0)
                r_send[index] = block.astype(BF)
        if n % 2:
            for far in far_first[n - 1 : n + 1]:
                each_facet(far, send_back)
    r_recv[f] = r_send[f]

    back_load.wait()
    image_load.wait()

    def back_chunk(q, g):
        first = g * 8 + 2 * pair_at(q)
        pieces = []
        for h in range(2):
            ret = r_recv[first + h]
            other = spin(ret.astype(F32), 1.0, -1.0).astype(BF)
            pieces.append(jnp.concatenate([ret, other], axis=0))
        return pl.multiple_of(first * two, 2 * two), jnp.concatenate(pieces, axis=1)

    for q in nearest[:-1]:
        each_facet(q, take_back)
        for g in range(groups):
            at, chunk = back_chunk(q, g)
            term = lax.dot_general(
                tt[:, pl.ds(at, 2 * two)], chunk, NT, preferred_element_type=F32
            )
            if q == nearest[0] and g == 0:
                bacc[...] = term
            else:
                bacc[...] += term
    each_facet(nearest[-1], take_back)
    chunks = [back_chunk(nearest[-1], g) for g in range(groups)]

    def back_strip(cp):
        at = pl.ds(pl.multiple_of(cp * rows, rows), rows)
        strip = bacc[at]
        for lane, chunk in chunks:
            strip += lax.dot_general(
                tt[at, pl.ds(lane, 2 * two)], chunk, NT, preferred_element_type=F32
            )
        return strip.astype(BF)

    for step in col_steps:
        peer = col_at(step, 1)
        b_send[peer] = back_strip(peer)
        col_link(b_send, b_recv, sd, rd, peer, c).start()
    back_out[c] = back_strip(c)
    for step in col_steps[::-1]:
        src = col_at(step, -1)
        col_link(b_send, b_recv, sd, rd, src, src).wait_recv()
        back_out[src] = b_recv[src]
    for step in col_steps:
        peer = col_at(step, 1)
        col_link(s_send, s_recv, sa, ra, peer, c).wait_send()
        col_link(b_send, b_recv, sd, rd, peer, c).wait_send()
    for d in range(1, nf):
        peer = lax.rem(f + d, nf)
        facet_link(g_send, g_recv, sb, rb, peer, f).wait_send()
        facet_link(r_send, r_recv, sc, rc, peer, f).wait_send()


def image_kernel(nc, back, tab, out, buf, sem):
    tiles, rows, tile = buf.shape[0], buf.shape[2], buf.shape[3]
    strip = jnp.concatenate([back[k] for k in range(nc)], axis=1)
    spun = [spin(back[k].astype(F32), 1.0, -1.0).astype(BF) for k in range(nc)]
    strip = jnp.concatenate([strip, jnp.concatenate(spun, axis=1)], axis=0)
    stores = []
    for t in range(tiles):
        piece = jnp.dot(strip, tab[:, t * tile : (t + 1) * tile], preferred_element_type=F32)
        for part in range(2):
            buf[t, part] = piece[part * rows : (part + 1) * rows]
        store = pltpu.make_async_copy(
            buf.at[t], out.at[:, :, t * tile : (t + 1) * tile], sem.at[t]
        )
        store.start()
        stores.append(store)
    for store in stores:
        store.wait()


def solution(mesh):
    nf, nc = mesh.shape["facet"], mesh.shape["col"]

    def on_device(facets, observed, uv_cells, counts):
        rows, extent = facets.shape[1:]
        vis = observed.shape[2]
        pc = counts.shape[0]
        window = S // 8
        two = 2 * window
        groups = nf // 8
        assert pc == nf and nf % 8 == 0 and nf <= 32
        constants = make_constants(nf, nc, pc, extent)
        vmem = pl.BlockSpec(memory_space=pltpu.VMEM)
        hbm = pl.BlockSpec(memory_space=pltpu.HBM)
        dma = pltpu.SemaphoreType.DMA
        fixed = functools.partial(pltpu.with_memory_space_constraint, memory_space=pltpu.HBM)
        back, tab = pl.pallas_call(
            functools.partial(cycle_kernel, nf, nc),
            out_shape=(
                jax.ShapeDtypeStruct((nc, rows, two), BF),
                jax.ShapeDtypeStruct((nc * two, extent), BF),
            ),
            in_specs=[hbm] * 9,
            out_specs=(vmem, vmem),
            scratch_shapes=[
                pltpu.VMEM((2 * rows, extent), BF),
                pltpu.VMEM(constants[1].shape, BF),
                pltpu.VMEM((2, pc, vis), F32),
                pltpu.VMEM((2, pc, vis), jnp.int32),
                pltpu.SMEM((pc,), jnp.int32),
                pltpu.VMEM((pc, 2, two), F32),
                pltpu.VMEM((nf, 2, two), F32),
                pltpu.VMEM((pc * two, extent), BF),
                pltpu.VMEM((extent, pc * two), BF),
                pltpu.VMEM((pc * two, two), F32),
                pltpu.VMEM((extent, two), F32),
                pltpu.VMEM((nc, rows, two), BF),
                pltpu.VMEM((nc, rows, two), BF),
                pltpu.VMEM((pc, window, two), BF),
                pltpu.VMEM((nf, window, two), BF),
                pltpu.VMEM((2 * S, vis), BF),
                pltpu.VMEM((vis, 2 * S), BF),
                pltpu.VMEM((S // 16, vis), F32),
                pltpu.VMEM((S // 16, vis), F32),
                pltpu.VMEM((2, vis, groups * two), F32),
                pltpu.VMEM((2, vis, two), F32),
                pltpu.VMEM((vis, groups * two), F32),
                pltpu.VMEM((vis, groups * two), BF),
                pltpu.VMEM((nf, window, two), BF),
                pltpu.VMEM((pc, window, two), BF),
                pltpu.VMEM((nc, rows, two), BF),
                pltpu.VMEM((nc, rows, two), BF),
                pltpu.SemaphoreType.REGULAR((2,)),
                dma((10,)), dma((nc,)),
                dma((nc,)), dma((nc,)), dma((nf,)), dma((nf,)),
                dma((nf,)), dma((nf,)), dma((nc,)), dma((nc,)),
            ],
            compiler_params=pltpu.CompilerParams(
                collective_id=0, has_side_effects=True, vmem_limit_bytes=44 * 2**20
            ),
            name="cycle",
        )(
            fixed(facets), fixed(observed), fixed(uv_cells), fixed(counts),
            *(fixed(jnp.asarray(constant)) for constant in constants),
        )
        tile = 256
        return pl.pallas_call(
            functools.partial(image_kernel, nc),
            out_shape=jax.ShapeDtypeStruct((2, rows, extent), F32),
            in_specs=[vmem, vmem],
            out_specs=hbm,
            scratch_shapes=[
                pltpu.VMEM((extent // tile, 2, rows, tile), F32),
                dma((extent // tile,)),
            ],
            compiler_params=pltpu.CompilerParams(vmem_limit_bytes=16 * 2**20),
            name="image",
        )(back, tab)

    return jax.shard_map(
        on_device,
        mesh=mesh,
        in_specs=(
            P(None, ("facet", "col"), None),
            P(None, "col", None),
            P(None, "col", None),
            P("col"),
        ),
        out_specs=P(None, ("facet", "col"), None),
        check_vma=False,
    )
```

```python
import functools
import math

import jax
import jax.numpy as jnp
import numpy as np
from jax import lax
from jax.experimental import pallas as pl
from jax.experimental.pallas import tpu as pltpu
from jax.sharding import PartitionSpec as P

S = 512
IMAGE = 65536
MESH = pl.DeviceIdType.MESH
BF = jnp.bfloat16
F32 = jnp.float32
NT = (((1,), (1,)), ((), ()))


def unit(ticks):
    angle = (np.asarray(ticks, np.int64) % IMAGE) * (-2.0 * math.pi / IMAGE)
    return np.cos(angle), np.sin(angle)


def make_constants(facets, columns, per_column, extent):
    window = S // 8
    spacing = IMAGE // extent
    cells = np.arange(extent, dtype=np.int64)
    weight = (0.6 + 0.4 * np.sin(math.pi * (cells + 0.5) / extent) ** 2) / math.sqrt(extent)
    step = np.arange(window, dtype=np.int64)
    col = np.arange(columns, dtype=np.int64)
    vc = col * (IMAGE // 4) + (29 * col + 3) % spacing
    sub = np.arange(per_column, dtype=np.int64)
    us = sub * (IMAGE // 64) + (37 * sub + 5) % (IMAGE * 8 // S)

    def table(start, stride):
        real, imag = unit((start[:, None] + stride * step)[:, :, None] * cells)
        return np.stack([real * weight, imag * weight], axis=1).astype(np.float32).astype(BF)

    wide = 2 - columns % 2
    col_tab = table(vc, spacing).reshape(columns // wide, wide, 2, 2, window // 2, extent)
    col_tab = col_tab.transpose(0, 3, 1, 2, 4, 5).reshape(-1, extent)
    row_tab = table(us, IMAGE // window).reshape(-1, extent)
    assert extent % window == 0
    fy = extent * (np.arange(facets, dtype=np.int64) % 8)
    fx = extent * (np.arange(facets, dtype=np.int64) // 8)
    real, imag = unit((fy[:, None] * vc)[:, :, None] + (fx[:, None] * us)[:, None, :])
    same = np.stack([real, real], axis=-1)
    cross = np.stack([-imag, imag], axis=-1)
    turn = np.repeat(np.stack([same, cross], axis=3), window, axis=4)
    flat = np.ascontiguousarray
    return flat(col_tab), row_tab, flat(row_tab.T), turn.astype(np.float32)


def spin(value, first, second):
    half = value.shape[1] // 2
    lane = lax.broadcasted_iota(jnp.int32, value.shape, 1)
    return pltpu.roll(value, half, 1) * jnp.where(lane < half, first, second)


def sign(value, first, second):
    lane = lax.broadcasted_iota(jnp.int32, value.shape, 1)
    return value * jnp.where(lane < value.shape[1] // 2, first, second)


def image_rows(blocks):
    half = blocks[0].shape[0] // 2
    cross = []
    for block in blocks:
        cross += [block[half:], -block[:half]]
    return jnp.concatenate(
        [jnp.concatenate(blocks, axis=0).T, jnp.concatenate(cross, axis=0).T], axis=0
    )


def cycle_kernel(
    nf, nc, x_hbm, obs_hbm, cells_hbm, counts_hbm, ctab_hbm, rtab_hbm, ttab_hbm, turn_hbm,
    back_out, base_out, tab,
    xbuf, obs, cells, counts, turn_in, turn_out, t2, tt, acc, bacc,
    s_send, s_recv, g_send, g_recv, right, right_t, r1r, r1i, left, inner, held,
    r_send, r_recv, b_send, b_recv,
    tok, in_sem, tab_sem, sa, ra, sb, rb, sc, rc, sd, rd,
):
    f = lax.axis_index("facet")
    c = lax.axis_index("col")
    window = S // 8
    half = window // 2
    two = 2 * window
    parts = window // 16
    pc = nf
    rows = xbuf.shape[0] // 2
    groups = nf // 8
    vis = obs.shape[2]
    if nc % 2:
        col_steps = [(d, 0) for d in range(1, nc)]
        wide = 1
    else:
        col_steps = [(d, k) for d in range(nc // 2 - 1, -1, -1) for k in range(2) if d or k]
        wide = 2
    near_steps = [step for step in col_steps if step[0] == 0]
    far_steps = [step for step in col_steps if step[0]]

    def col_at(step, sign):
        if nc % 2:
            return lax.rem(c + nc + sign * step[0], nc)
        top = lax.rem(c // 2 + nc // 2 + sign * step[0], nc // 2)
        return 2 * top + lax.rem(c + step[1], 2)

    def pair_at(q):
        return lax.rem(f // 2 + q, 4)

    def group_of(q):
        return 0 if q in waits[0] else 1

    def facet_link(src_buf, dst_buf, send, recv, part, peer, slot, group):
        return pltpu.make_async_remote_copy(
            src_buf.at[part, peer], dst_buf.at[part, slot],
            send.at[part], recv.at[part, group], (peer, c), MESH,
        )

    def col_link(src_buf, dst_buf, send, recv, part, peer, slot):
        return pltpu.make_async_remote_copy(
            src_buf.at[part, peer], dst_buf.at[part, slot], send.at[part], recv, (f, peer), MESH
        )

    def sum_of(buf, part, count, send, recv):
        some = buf.at[part, 0:count]
        return pltpu.make_async_remote_copy(some, some, send, recv, (mate, c), MESH)

    waits = ((0, 1), (3, 2))
    mate = f + 1 - 2 * lax.rem(f, 2)

    barrier = pltpu.get_barrier_semaphore()
    place, last_place = f // 2, nf // 2 - 1
    low, high = place > 0, place < last_place

    def signal(sem, facet, col):
        pl.semaphore_signal(sem, inc=1, device_id=(facet, col), device_id_type=MESH)

    inside = low & high

    def pass_on(way):
        pl.semaphore_wait(tok.at[way], 1)
        signal(tok.at[way], f + 2 - 4 * way, c)

    for d in range(1, nc):
        signal(barrier, f, lax.rem(c + d, nc))
    signal(barrier, mate, c)
    pl.when(high)(lambda: signal(barrier, f + 2, c))
    pl.when(low)(lambda: signal(barrier, f - 2, c))

    n_groups = nc // wide
    chunk = wide * window

    def group_at(d):
        return lax.rem(c // wide + n_groups + d, n_groups)

    far_groups = list(range(n_groups - 1, 0, -1)) if wide == 2 else list(range(1, nc))

    def tab_load(d):
        at = pl.ds(pl.multiple_of(group_at(d) * 2 * chunk, 2 * chunk), 2 * chunk)
        return pltpu.make_async_copy(ctab_hbm.at[at], tab.at[at], tab_sem.at[d])

    x_loads = [
        pltpu.make_async_copy(x_hbm.at[k], xbuf.at[k * rows : (k + 1) * rows], in_sem.at[k])
        for k in range(2)
    ]
    row_load = pltpu.make_async_copy(rtab_hbm, t2, in_sem.at[2])
    small_loads = [
        pltpu.make_async_copy(turn_hbm.at[f, c], turn_in, in_sem.at[3]),
        pltpu.make_async_copy(turn_hbm.at[:, c, f], turn_out, in_sem.at[4]),
        pltpu.make_async_copy(obs_hbm, obs, in_sem.at[5]),
        pltpu.make_async_copy(cells_hbm, cells, in_sem.at[6]),
        pltpu.make_async_copy(counts_hbm, counts, in_sem.at[7]),
    ]
    turned_load = pltpu.make_async_copy(ttab_hbm, tt, in_sem.at[8])
    for n, d in enumerate(far_groups + [0]):
        tab_load(d).start()
        if n == 0:
            for load in x_loads:
                load.start()
    for load in small_loads:
        load.start()

    pl.semaphore_wait(barrier, nc + low.astype(jnp.int32) + high.astype(jnp.int32))
    pl.when(~low)(lambda: signal(tok.at[0], f + 2, c))
    pl.when(~high)(lambda: signal(tok.at[1], f - 2, c))

    for load in x_loads:
        load.wait()
    turned_load.start()

    def strips(d, first_part, n_parts):
        at = pl.multiple_of(group_at(d) * 2 * chunk + first_part * chunk, chunk)
        both = lax.dot_general(
            tab[pl.ds(at, n_parts * chunk), :], xbuf[...], NT, preferred_element_type=F32
        )
        for part in range(n_parts):
            for k in range(wide):
                at = part * chunk + k * window
                real, imag = both[at : at + half], both[at + half : at + window]
                block = [real[:, :rows] - imag[:, rows:], imag[:, :rows] + real[:, rows:]]
                s_send[first_part + part, wide * group_at(d) + k] = jnp.concatenate(
                    block, axis=0
                ).astype(BF)

    def send_strips(d, part):
        for n, step in enumerate(col_steps):
            if step[0] == d:
                at = part * len(col_steps) + n
                col_link(s_send, s_recv, sa, ra.at[at], part, col_at(step, 1), c).start()

    for n, d in enumerate(far_groups):
        tab_load(d).wait()
    for part in range(2):
        for d in far_groups:
            strips(d, part, 1)
            send_strips(d, part)
    pl.when(inside & (place == last_place - 1))(functools.partial(pass_on, 1))
    tab_load(0).wait()
    strips(0, 0, 2)
    for part in range(2):
        send_strips(0, part)
    pl.when(inside & (place == 1))(functools.partial(pass_on, 0))

    turned_load.wait()

    def window_term(block, src):
        at = pl.multiple_of(src * rows, rows)
        return jnp.dot(block, tt[pl.ds(at, rows), :], preferred_element_type=F32)

    acc[...] = window_term(jnp.concatenate([s_send[0, c], s_send[1, c]], axis=0), c)
    pl.when(inside & (place != 1))(functools.partial(pass_on, 0))
    pl.when(inside & (place != last_place - 1))(functools.partial(pass_on, 1))

    for load in small_loads:
        load.wait()

    def each_facet(q, act):
        pair = pair_at(q)
        for g in range(groups):
            for h in range(2):
                index = g * 8 + 2 * pair + h
                if q == 0:
                    pl.when(index != f)(functools.partial(act, index))
                else:
                    act(index)

    def send_facets(src_buf, dst_buf, send, recv, part):
        for q in far_first:
            each_facet(
                q,
                lambda index, q=q: facet_link(
                    src_buf, dst_buf, send, recv, part, index, f, group_of(-q % 4)
                ).start(),
            )
        dst_buf[part, f] = src_buf[part, f]

    def take_facets(buf, send, recv, part, pairs):
        for group in range(2):
            if waits[group][0] in pairs:
                count = 4 * groups - (0 in waits[group])
                sum_of(buf, part, count, send.at[part], recv.at[part, group]).wait_recv()

    far_first = (2, 3, 1, 0)

    def take_strip(part, step):
        src = col_at(step, -1)
        at = part * len(col_steps) + col_steps.index(step)
        col_link(s_send, s_recv, sa, ra.at[at], part, src, src).wait_recv()

    for step in near_steps:
        src = col_at(step, -1)
        for part in range(2):
            take_strip(part, step)
        acc[...] += window_term(jnp.concatenate([s_recv[0, src], s_recv[1, src]], axis=0), src)

    def windows(part):
        total = acc[part * window : (part + 1) * window]
        for step in far_steps:
            src = col_at(step, -1)
            take_strip(part, step)
            total += window_term(s_recv[part, src], src)
        for j in range(pc):
            u = total[:half, j * two : (j + 1) * two]
            v = total[half:, j * two : (j + 1) * two]
            turn = turn_in[j]
            same, cross = turn[0:1], turn[1:2]
            win = u * same + spin(v, -1.0, 1.0) * same
            win += pltpu.roll(u, window, 1) * cross + v * sign(cross, 1.0, -1.0)
            g_send[part, j] = win.astype(BF)
        if part == 0:
            pl.when(~low)(lambda: pl.semaphore_wait(tok.at[1], 1))
            pl.when(~high)(lambda: pl.semaphore_wait(tok.at[0], 1))
        send_facets(g_send, g_recv, sb, rb, part)

    windows(0)

    first = cells[0, pl.ds(f, 1), :]
    second = cells[1, pl.ds(f, 1), :]

    def series(square, first, terms):
        value = jnp.full_like(square, 1.0 / math.factorial(first + 2 * terms))
        for k in range(terms - 1, -1, -1):
            value = 1.0 / math.factorial(first + 2 * k) - value * square
        return value

    def wave(count, step, cell):
        index = step * lax.broadcasted_iota(jnp.int32, (count, vis), 0)
        turn = ((index * cell + S // 2) & (S - 1)) - S // 2
        angle = turn.astype(F32) * (-math.pi / S)
        square = angle * angle
        sine = angle * series(square, 1, 5)
        return 1.0 - 2.0 * sine * sine, 2.0 * sine * series(square, 0, 6)

    scale = 1.0 / math.sqrt(vis)
    live = lax.broadcasted_iota(jnp.int32, (1, vis), 1) < counts[f]
    gain = jnp.where(live, scale, 0.0)
    m0r, m0i = wave(16, 1, second)
    m0r, m0i = m0r * gain, m0i * gain
    r1r[...], r1i[...] = wave(S // 16, 16, second)

    def right_body(i, carry):
        er, ei = r1r[pl.ds(i, 1), :], r1i[pl.ds(i, 1), :]
        b = i // parts
        k = i - b * parts
        h = k // (parts // 2)
        at = pl.multiple_of(h * S + b * window + (k - h * (parts // 2)) * 16, 16)
        right[pl.ds(at, 16), :] = (m0r * er - m0i * ei).astype(BF)
        right[pl.ds(at + half, 16), :] = (m0r * ei + m0i * er).astype(BF)
        return carry

    lax.fori_loop(0, S // 16, right_body, 0)

    windows(1)
    row_load.start()

    def turn_body(i, carry):
        at = pl.multiple_of(i * two, two)
        right_t[:, pl.ds(at, two)] = right[pl.ds(at, two), :].T
        return carry

    lax.fori_loop(0, S // window, turn_body, 0)

    l0r, l0i = wave(16, 1, first)
    l1r, l1i = wave(max(groups * parts, 8), 16, first)
    for i in range(groups * parts):
        er, ei = l1r[i : i + 1], l1i[i : i + 1]
        at = i // parts * two + i % parts * 16
        real = (l0r * er - l0i * ei).astype(BF).astype(F32)
        imag = (l0r * ei + l0i * er).astype(BF).astype(F32)
        left[0, at : at + 16, :] = real
        left[0, at + window : at + window + 16, :] = -imag
        left[1, at : at + 16, :] = imag
        left[1, at + window : at + window + 16, :] = real

    def pred_term(part, pairs, g):
        blocks, tables = [], []
        for q in pairs:
            for h in range(2):
                block = g_recv[part, g * 8 + 2 * pair_at(q) + h].astype(F32)
                blocks += [block, spin(block, -1.0, 1.0)]
            at = pl.multiple_of(part * S + pair_at(q) * two, two)
            tables.append(right[pl.ds(at, two), :])
        return jnp.dot(
            jnp.concatenate(blocks, axis=0).T.astype(BF),
            jnp.concatenate(tables, axis=0),
            preferred_element_type=F32,
        )

    for part in range(2):
        for pairs in waits if part else (waits[0] + waits[1],):
            take_facets(g_recv, sb, rb, part, pairs)
            if pairs == waits[1]:
                continue
            for g in range(groups):
                at = slice(g * two, (g + 1) * two)
                if part == 0:
                    inner[at] = pred_term(part, pairs, g)
                else:
                    inner[at] += pred_term(part, pairs, g)
    res_r, res_i = obs[0, pl.ds(f, 1), :], obs[1, pl.ds(f, 1), :]
    for g in range(groups):
        at = slice(g * two, (g + 1) * two)
        value = inner[at] + pred_term(1, waits[-1], g)
        unscale = 1.0 / (scale * S)
        res_r -= jnp.sum(value * left[0, at], axis=0, keepdims=True) * unscale
        res_i -= jnp.sum(value * left[1, at], axis=0, keepdims=True) * unscale
    held[...] = (res_r * left[0] + res_i * left[1]).astype(BF)

    for part in range(2):
        grid = jnp.dot(
            held[...], right_t[:, part * S : (part + 1) * S], preferred_element_type=F32
        )
        for g in range(groups):
            block_t = grid[g * two : (g + 1) * two].T
            for b in range(8):
                u = block_t[b * window : b * window + half]
                v = block_t[b * window + half : (b + 1) * window]
                turn = turn_out[g * 8 + b]
                same, cross = turn[0:1], turn[1:2]
                block = (u + spin(v, 1.0, -1.0)) * same
                block -= pltpu.roll(u, window, 1) * cross + v * sign(cross, -1.0, 1.0)
                r_send[part, g * 8 + b] = block.astype(BF)
        send_facets(r_send, r_recv, sc, rc, part)

    row_load.wait()

    def back_term(part, pairs):
        total = None
        take_facets(r_recv, sc, rc, part, pairs)
        for q in pairs:
            for g in range(groups):
                first = g * 8 + 2 * pair_at(q)
                pieces = [r_recv[part, first + h] for h in range(2)]
                spun = [spin(piece.astype(F32), 1.0, -1.0).astype(BF) for piece in pieces]
                block = jnp.concatenate(
                    [jnp.concatenate(pieces, axis=1), jnp.concatenate(spun, axis=1)], axis=0
                )
                at = pl.multiple_of(first * two, 2 * two)
                term = jnp.dot(block, t2[pl.ds(at, 2 * two), :], preferred_element_type=F32)
                total = term if total is None else total + term
        return total

    def back_strips(part):
        total = (bacc[...] + back_term(part, waits[1])).astype(BF)
        for cp in range(nc):
            b_send[part, cp] = total[:, cp * rows : (cp + 1) * rows]
        for step in col_steps:
            at = rd.at[0 if step in near_steps else 1 + part]
            col_link(b_send, b_recv, sd, at, part, col_at(step, 1), c).start()
        b_recv[part, c] = b_send[part, c]

    bacc[...] = back_term(0, waits[0])
    back_strips(0)
    bacc[...] = back_term(1, waits[0])
    back_strips(1)
    if near_steps:
        sum_of(b_recv, 0, 2 * len(near_steps), sd.at[0], rd.at[0]).wait_recv()
    mine = [b_recv[part, wide * group_at(0) + k] for part in range(2) for k in range(wide)]
    at = pl.multiple_of(group_at(0) * 2 * chunk, 2 * chunk)
    base_out[...] = jnp.dot(
        image_rows(mine), tab[pl.ds(at, 2 * chunk), :], preferred_element_type=F32
    )
    sum_of(b_recv, 0, len(far_steps), sd.at[0], rd.at[1]).wait_recv()
    sum_of(b_recv, 1, len(far_steps), sd.at[1], rd.at[2]).wait_recv()
    for part in range(2):
        for d in range(1, n_groups):
            for k in range(wide):
                back_out[((d - 1) * 2 + part) * wide + k] = b_recv[part, wide * group_at(d) + k]
    for part in range(2):
        sum_of(s_send, part, nc - 1, sa.at[part], rd.at[0]).wait_send()
        sum_of(b_send, part, nc - 1, sd.at[part], rd.at[0]).wait_send()
        sum_of(g_send, part, nf - 1, sb.at[part], rb.at[0, 0]).wait_send()
        sum_of(r_send, part, nf - 1, sc.at[part], rc.at[0, 0]).wait_send()


def image_kernel(nc, back, base, tab, out, buf, sem):
    c = lax.axis_index("col")
    wide = 2 - nc % 2
    n_groups = nc // wide
    tiles, rows, tile = buf.shape[0], buf.shape[2], buf.shape[3]
    depth = 2 * wide * back.shape[1]
    strip = image_rows([back[k] for k in range(back.shape[0])])
    stores = []
    for t in range(tiles):
        lanes = slice(t * tile, (t + 1) * tile)
        piece = base[:, lanes]
        for d in range(1, n_groups):
            at = pl.multiple_of(lax.rem(c // wide + d, n_groups) * depth, depth)
            piece += jnp.dot(
                strip[:, (d - 1) * depth : d * depth],
                tab[pl.ds(at, depth), lanes],
                preferred_element_type=F32,
            )
        for part in range(2):
            buf[t, part] = piece[part * rows : (part + 1) * rows]
        store = pltpu.make_async_copy(buf.at[t], out.at[:, :, lanes], sem.at[t])
        store.start()
        stores.append(store)
    for store in stores:
        store.wait()


def solution(mesh):
    nf, nc = mesh.shape["facet"], mesh.shape["col"]

    def on_device(facets, observed, uv_cells, counts):
        rows, extent = facets.shape[1:]
        vis = observed.shape[2]
        pc = counts.shape[0]
        window = S // 8
        two = 2 * window
        groups = nf // 8
        wide = 2 - nc % 2
        assert pc == nf and nf % 8 == 0 and nf <= 32 and nc > wide
        constants = make_constants(nf, nc, pc, extent)
        vmem = pl.BlockSpec(memory_space=pltpu.VMEM)
        hbm = pl.BlockSpec(memory_space=pltpu.HBM)
        dma = pltpu.SemaphoreType.DMA
        fixed = functools.partial(pltpu.with_memory_space_constraint, memory_space=pltpu.HBM)
        back, base, tab = pl.pallas_call(
            functools.partial(cycle_kernel, nf, nc),
            out_shape=(
                jax.ShapeDtypeStruct((2 * nc - 2 * wide, window, rows), BF),
                jax.ShapeDtypeStruct((2 * rows, extent), F32),
                jax.ShapeDtypeStruct((nc * two, extent), BF),
            ),
            in_specs=[hbm] * 8,
            out_specs=(vmem, vmem, vmem),
            scratch_shapes=[
                pltpu.VMEM((2 * rows, extent), BF),
                pltpu.VMEM((2, pc, vis), F32),
                pltpu.VMEM((2, pc, vis), jnp.int32),
                pltpu.SMEM((pc,), jnp.int32),
                pltpu.VMEM((pc, 2, two), F32),
                pltpu.VMEM((nf, 2, two), F32),
                pltpu.VMEM((pc * two, extent), BF),
                pltpu.VMEM((extent, pc * two), BF),
                pltpu.VMEM((two, pc * two), F32),
                pltpu.VMEM((window, extent), F32),
                pltpu.VMEM((2, nc, window, rows), BF),
                pltpu.VMEM((2, nc, window, rows), BF),
                pltpu.VMEM((2, pc, window // 2, two), BF),
                pltpu.VMEM((2, nf, window // 2, two), BF),
                pltpu.VMEM((2 * S, vis), BF),
                pltpu.VMEM((vis, 2 * S), BF),
                pltpu.VMEM((S // 16, vis), F32),
                pltpu.VMEM((S // 16, vis), F32),
                pltpu.VMEM((2, groups * two, vis), F32),
                pltpu.VMEM((groups * two, vis), F32),
                pltpu.VMEM((groups * two, vis), BF),
                pltpu.VMEM((2, nf, window // 2, two), BF),
                pltpu.VMEM((2, pc, window // 2, two), BF),
                pltpu.VMEM((2, nc, window, rows), BF),
                pltpu.VMEM((2, nc, window, rows), BF),
                pltpu.SemaphoreType.REGULAR((2,)),
                dma((9,)), dma((nc // wide,)),
                dma((2,)), dma((2 * nc - 2,)), dma((2,)), dma((2, 2)),
                dma((2,)), dma((2, 2)), dma((2,)), dma((3,)),
            ],
            compiler_params=pltpu.CompilerParams(
                collective_id=0, has_side_effects=True, vmem_limit_bytes=44 * 2**20
            ),
            name="cycle",
        )(
            fixed(facets), fixed(observed), fixed(uv_cells), fixed(counts),
            *(fixed(jnp.asarray(constant)) for constant in constants),
        )
        tile = 256
        return pl.pallas_call(
            functools.partial(image_kernel, nc),
            out_shape=jax.ShapeDtypeStruct((2, rows, extent), F32),
            in_specs=[vmem, vmem, vmem],
            out_specs=hbm,
            scratch_shapes=[
                pltpu.VMEM((extent // tile, 2, rows, tile), F32),
                dma((extent // tile,)),
            ],
            compiler_params=pltpu.CompilerParams(vmem_limit_bytes=16 * 2**20),
            name="image",
        )(back, base, tab)

    return jax.shard_map(
        on_device,
        mesh=mesh,
        in_specs=(
            P(None, ("facet", "col"), None),
            P(None, "col", None),
            P(None, "col", None),
            P("col"),
        ),
        out_specs=P(None, ("facet", "col"), None),
        check_vma=False,
    )
```

```python
import functools
import math

import jax
import jax.numpy as jnp
import numpy as np
from jax import lax
from jax.experimental import pallas as pl
from jax.experimental.pallas import tpu as pltpu
from jax.sharding import PartitionSpec as P

S = 512
IMAGE = 65536
MESH = pl.DeviceIdType.MESH
BF = jnp.bfloat16
F32 = jnp.float32
NT = (((1,), (1,)), ((), ()))


def unit(ticks):
    angle = (np.asarray(ticks, np.int64) % IMAGE) * (-2.0 * math.pi / IMAGE)
    return np.cos(angle), np.sin(angle)


def make_constants(facets, columns, per_column, extent):
    window = S // 8
    spacing = IMAGE // extent
    cells = np.arange(extent, dtype=np.int64)
    weight = (0.6 + 0.4 * np.sin(math.pi * (cells + 0.5) / extent) ** 2) / math.sqrt(extent)
    step = np.arange(window, dtype=np.int64)
    col = np.arange(columns, dtype=np.int64)
    vc = col * (IMAGE // 4) + (29 * col + 3) % spacing
    sub = np.arange(per_column, dtype=np.int64)
    us = sub * (IMAGE // 64) + (37 * sub + 5) % (IMAGE * 8 // S)

    def table(start, stride):
        real, imag = unit((start[:, None] + stride * step)[:, :, None] * cells)
        return np.stack([real * weight, imag * weight], axis=1).astype(np.float32).astype(BF)

    wide = 2 - columns % 2
    col_tab = table(vc, spacing).reshape(columns // wide, wide, 2, 2, window // 2, extent)
    col_tab = col_tab.transpose(0, 3, 1, 2, 4, 5).reshape(-1, extent)
    row_tab = table(us, IMAGE // window).reshape(-1, extent)
    assert extent % window == 0
    fy = extent * (np.arange(facets, dtype=np.int64) % 8)
    fx = extent * (np.arange(facets, dtype=np.int64) // 8)
    real, imag = unit((fy[:, None] * vc)[:, :, None] + (fx[:, None] * us)[:, None, :])
    same = np.stack([real, real], axis=-1)
    cross = np.stack([-imag, imag], axis=-1)
    turn = np.repeat(np.stack([same, cross], axis=3), window, axis=4)
    flat = np.ascontiguousarray
    return flat(col_tab), row_tab, flat(row_tab.T), turn.astype(np.float32)


def spin(value, first, second):
    half = value.shape[1] // 2
    lane = lax.broadcasted_iota(jnp.int32, value.shape, 1)
    return pltpu.roll(value, half, 1) * jnp.where(lane < half, first, second)


def sign(value, first, second):
    lane = lax.broadcasted_iota(jnp.int32, value.shape, 1)
    return value * jnp.where(lane < value.shape[1] // 2, first, second)


def image_rows(blocks):
    half = blocks[0].shape[0] // 2
    cross = []
    for block in blocks:
        cross += [block[half:], -block[:half]]
    return jnp.concatenate(
        [jnp.concatenate(blocks, axis=0).T, jnp.concatenate(cross, axis=0).T], axis=0
    )


def cycle_kernel(
    nf, nc, x_hbm, obs_hbm, cells_hbm, counts_hbm, ctab_hbm, rtab_hbm, ttab_hbm, turn_hbm,
    back_out, base_out, tab,
    xbuf, obs, cells, counts, turn_in, turn_out, t2, tt, acc, bacc,
    s_send, s_recv, g_send, g_recv, right, right_t, r1r, r1i, left, inner, held,
    r_send, r_recv, b_send, b_recv,
    tok, in_sem, tab_sem, sa, ra, sb, rb, sc, rc, sd, rd,
):
    f = lax.axis_index("facet")
    c = lax.axis_index("col")
    window = S // 8
    half = window // 2
    two = 2 * window
    parts = window // 16
    pc = nf
    rows = xbuf.shape[0] // 2
    groups = nf // 8
    vis = obs.shape[2]
    if nc % 2:
        col_steps = [(d, 0) for d in range(1, nc)]
        wide = 1
    else:
        col_steps = [(d, k) for d in range(nc // 2 - 1, -1, -1) for k in range(2) if d or k]
        wide = 2
    near_steps = [step for step in col_steps if step[0] == 0]
    far_steps = [step for step in col_steps if step[0]]

    def col_at(step, sign):
        if nc % 2:
            return lax.rem(c + nc + sign * step[0], nc)
        top = lax.rem(c // 2 + nc // 2 + sign * step[0], nc // 2)
        return 2 * top + lax.rem(c + step[1], 2)

    def pair_at(q):
        return lax.rem(f // 2 + q, 4)

    def group_of(q):
        return 0 if q in waits[0] else 1

    def facet_link(src_buf, dst_buf, send, recv, part, peer, slot, group):
        return pltpu.make_async_remote_copy(
            src_buf.at[part, peer], dst_buf.at[part, slot],
            send.at[part], recv.at[part, group], (peer, c), MESH,
        )

    def col_link(src_buf, dst_buf, send, recv, part, peer, slot):
        return pltpu.make_async_remote_copy(
            src_buf.at[part, peer], dst_buf.at[part, slot], send.at[part], recv, (f, peer), MESH
        )

    def sum_of(buf, part, count, send, recv):
        some = buf.at[part, 0:count]
        return pltpu.make_async_remote_copy(some, some, send, recv, (mate, c), MESH)

    waits = ((0, 1), (3, 2))
    mate = f + 1 - 2 * lax.rem(f, 2)

    barrier = pltpu.get_barrier_semaphore()
    place, last_place = f // 2, nf // 2 - 1
    low, high = place > 0, place < last_place
    far_low, far_high = place > 1, place < last_place - 1

    def signal(sem, facet, col):
        pl.semaphore_signal(sem, inc=1, device_id=(facet, col), device_id_type=MESH)

    def pass_on(way):
        pl.semaphore_wait(tok.at[way], 1)
        signal(tok.at[way], f + 2 - 4 * way, c)

    for d in range(1, nc):
        signal(barrier, f, lax.rem(c + d, nc))
    signal(barrier, mate, c)

    @pl.when(high)
    def _():
        signal(barrier, f + 2, c)
        signal(barrier, mate + 2, c)

    @pl.when(low)
    def _():
        signal(barrier, f - 2, c)
        signal(barrier, mate - 2, c)


    n_groups = nc // wide
    chunk = wide * window

    def group_at(d):
        return lax.rem(c // wide + n_groups + d, n_groups)

    far_groups = list(range(n_groups - 1, 0, -1)) if wide == 2 else list(range(1, nc))

    def tab_load(d, lanes, sem):
        at = pl.ds(pl.multiple_of(group_at(d) * 2 * chunk, 2 * chunk), 2 * chunk)
        return pltpu.make_async_copy(ctab_hbm.at[at, lanes], tab.at[at, lanes], sem)

    depth = xbuf.shape[1] // 2
    depths = [slice(k * depth, (k + 1) * depth) for k in range(2)]
    early = [
        [tab_load(d, lanes, tab_sem.at[k, d]) for d in far_groups]
        + [
            pltpu.make_async_copy(
                x_hbm.at[p, :, lanes], xbuf.at[p * rows : (p + 1) * rows, lanes], in_sem.at[2 * k + p]
            )
            for p in range(2)
        ]
        for k, lanes in enumerate(depths)
    ]
    mine_load = tab_load(0, slice(None), tab_sem.at[0, 0])
    row_load = pltpu.make_async_copy(rtab_hbm, t2, in_sem.at[9])
    small_loads = [
        pltpu.make_async_copy(turn_hbm.at[f, c], turn_in, in_sem.at[4]),
        pltpu.make_async_copy(turn_hbm.at[:, c, f], turn_out, in_sem.at[5]),
        pltpu.make_async_copy(obs_hbm, obs, in_sem.at[6]),
        pltpu.make_async_copy(cells_hbm, cells, in_sem.at[7]),
        pltpu.make_async_copy(counts_hbm, counts, in_sem.at[8]),
    ]
    turned_load = pltpu.make_async_copy(ttab_hbm, tt, in_sem.at[10])
    for load in early[0] + early[1]:
        load.start()

    def strip_term(d, lanes):
        at = pl.multiple_of(group_at(d) * 2 * chunk, 2 * chunk)
        return lax.dot_general(
            tab[pl.ds(at, 2 * chunk), lanes], xbuf[:, lanes], NT, preferred_element_type=F32
        )

    def strips(d, both):
        for part in range(2):
            for k in range(wide):
                at = part * chunk + k * window
                real, imag = both[at : at + half], both[at + half : at + window]
                block = [real[:, :rows] - imag[:, rows:], imag[:, :rows] + real[:, rows:]]
                s_send[part, wide * group_at(d) + k] = jnp.concatenate(block, axis=0).astype(BF)

    def send_strips(d, part):
        for n, step in enumerate(col_steps):
            if step[0] == d:
                at = part * len(col_steps) + n
                col_link(s_send, s_recv, sa, ra.at[at], part, col_at(step, 1), c).start()

    for load in early[0]:
        load.wait()
    mine_load.start()
    for load in small_loads:
        load.start()
    sums = [strip_term(d, depths[0]) for d in far_groups]
    for load in early[1]:
        load.wait()
    turned_load.start()
    for d, term in zip(far_groups, sums):
        strips(d, term + strip_term(d, depths[1]))
    pl.semaphore_wait(barrier, nc + 2 * low.astype(jnp.int32) + 2 * high.astype(jnp.int32))
    for part in range(2):
        for d in far_groups:
            send_strips(d, part)
    pl.when((place == 1) & high)(lambda: signal(tok.at[0], f + 2, c))
    pl.when((place == last_place - 1) & low)(lambda: signal(tok.at[1], f - 2, c))
    mine_load.wait()
    strips(0, strip_term(0, slice(None)))
    for part in range(2):
        send_strips(0, part)

    @pl.when(far_low & high)
    def _():
        pass_on(0)

    @pl.when(far_high & low)
    def _():
        pass_on(1)

    turned_load.wait()

    def window_term(block, src):
        at = pl.multiple_of(src * rows, rows)
        return jnp.dot(block, tt[pl.ds(at, rows), :], preferred_element_type=F32)

    acc[...] = window_term(jnp.concatenate([s_send[0, c], s_send[1, c]], axis=0), c)

    for load in small_loads:
        load.wait()

    def each_facet(q, act):
        pair = pair_at(q)
        for g in range(groups):
            for h in range(2):
                index = g * 8 + 2 * pair + h
                if q == 0:
                    pl.when(index != f)(functools.partial(act, index))
                else:
                    act(index)

    def send_facets(src_buf, dst_buf, send, recv, part):
        for q in far_first:
            each_facet(
                q,
                lambda index, q=q: facet_link(
                    src_buf, dst_buf, send, recv, part, index, f, group_of(-q % 4)
                ).start(),
            )
        dst_buf[part, f] = src_buf[part, f]

    def take_facets(buf, send, recv, part, pairs):
        for group in range(2):
            if waits[group][0] in pairs:
                count = 4 * groups - (0 in waits[group])
                sum_of(buf, part, count, send.at[part], recv.at[part, group]).wait_recv()

    far_first = (2, 3, 1, 0)

    def take_strip(part, step):
        src = col_at(step, -1)
        at = part * len(col_steps) + col_steps.index(step)
        col_link(s_send, s_recv, sa, ra.at[at], part, src, src).wait_recv()

    for step in near_steps:
        src = col_at(step, -1)
        for part in range(2):
            take_strip(part, step)
        acc[...] += window_term(jnp.concatenate([s_recv[0, src], s_recv[1, src]], axis=0), src)

    def windows(part):
        total = acc[part * window : (part + 1) * window]
        for step in far_steps:
            src = col_at(step, -1)
            take_strip(part, step)
            total += window_term(s_recv[part, src], src)
        for j in range(pc):
            u = total[:half, j * two : (j + 1) * two]
            v = total[half:, j * two : (j + 1) * two]
            turn = turn_in[j]
            same, cross = turn[0:1], turn[1:2]
            win = u * same + spin(v, -1.0, 1.0) * same
            win += pltpu.roll(u, window, 1) * cross + v * sign(cross, 1.0, -1.0)
            g_send[part, j] = win.astype(BF)
        if part == 0:
            pl.when(far_high & ~low)(lambda: pl.semaphore_wait(tok.at[1], 1))
            pl.when(far_low & ~high)(lambda: pl.semaphore_wait(tok.at[0], 1))
        send_facets(g_send, g_recv, sb, rb, part)

    first = cells[0, pl.ds(f, 1), :]
    second = cells[1, pl.ds(f, 1), :]

    def series(square, first, terms):
        value = jnp.full_like(square, 1.0 / math.factorial(first + 2 * terms))
        for k in range(terms - 1, -1, -1):
            value = 1.0 / math.factorial(first + 2 * k) - value * square
        return value

    def wave(count, step, cell):
        index = step * lax.broadcasted_iota(jnp.int32, (count, vis), 0)
        turn = ((index * cell + S // 2) & (S - 1)) - S // 2
        angle = turn.astype(F32) * (-math.pi / S)
        square = angle * angle
        sine = angle * series(square, 1, 5)
        return 1.0 - 2.0 * sine * sine, 2.0 * sine * series(square, 0, 6)

    scale = 1.0 / math.sqrt(vis)
    live = lax.broadcasted_iota(jnp.int32, (1, vis), 1) < counts[f]
    gain = jnp.where(live, scale, 0.0)
    m0r, m0i = wave(16, 1, second)
    m0r, m0i = m0r * gain, m0i * gain
    r1r[...], r1i[...] = wave(S // 16, 16, second)

    windows(0)

    def right_body(i, carry):
        er, ei = r1r[pl.ds(i, 1), :], r1i[pl.ds(i, 1), :]
        b = i // parts
        k = i - b * parts
        h = k // (parts // 2)
        at = pl.multiple_of(h * S + b * window + (k - h * (parts // 2)) * 16, 16)
        right[pl.ds(at, 16), :] = (m0r * er - m0i * ei).astype(BF)
        right[pl.ds(at + half, 16), :] = (m0r * ei + m0i * er).astype(BF)
        return carry

    lax.fori_loop(0, S // 16, right_body, 0)

    windows(1)
    row_load.start()

    def turn_body(i, carry):
        at = pl.multiple_of(i * two, two)
        right_t[:, pl.ds(at, two)] = right[pl.ds(at, two), :].T
        return carry

    lax.fori_loop(0, S // window, turn_body, 0)

    l0r, l0i = wave(16, 1, first)
    l1r, l1i = wave(max(groups * parts, 8), 16, first)
    for i in range(groups * parts):
        er, ei = l1r[i : i + 1], l1i[i : i + 1]
        at = i // parts * two + i % parts * 16
        real = (l0r * er - l0i * ei).astype(BF).astype(F32)
        imag = (l0r * ei + l0i * er).astype(BF).astype(F32)
        left[0, at : at + 16, :] = real
        left[0, at + window : at + window + 16, :] = -imag
        left[1, at : at + 16, :] = imag
        left[1, at + window : at + window + 16, :] = real

    def pred_term(part, pairs, g):
        blocks, tables = [], []
        for q in pairs:
            for h in range(2):
                block = g_recv[part, g * 8 + 2 * pair_at(q) + h].astype(F32)
                blocks += [block, spin(block, -1.0, 1.0)]
            at = pl.multiple_of(part * S + pair_at(q) * two, two)
            tables.append(right[pl.ds(at, two), :])
        return jnp.dot(
            jnp.concatenate(blocks, axis=0).T.astype(BF),
            jnp.concatenate(tables, axis=0),
            preferred_element_type=F32,
        )

    for part in range(2):
        for pairs in waits if part else (waits[0] + waits[1],):
            take_facets(g_recv, sb, rb, part, pairs)
            if pairs == waits[1]:
                continue
            for g in range(groups):
                at = slice(g * two, (g + 1) * two)
                if part == 0:
                    inner[at] = pred_term(part, pairs, g)
                else:
                    inner[at] += pred_term(part, pairs, g)
    res_r, res_i = obs[0, pl.ds(f, 1), :], obs[1, pl.ds(f, 1), :]
    for g in range(groups):
        at = slice(g * two, (g + 1) * two)
        value = inner[at] + pred_term(1, waits[-1], g)
        unscale = 1.0 / (scale * S)
        res_r -= jnp.sum(value * left[0, at], axis=0, keepdims=True) * unscale
        res_i -= jnp.sum(value * left[1, at], axis=0, keepdims=True) * unscale
    held[...] = (res_r * left[0] + res_i * left[1]).astype(BF)

    for part in range(2):
        grid = jnp.dot(
            held[...], right_t[:, part * S : (part + 1) * S], preferred_element_type=F32
        )
        for g in range(groups):
            block_t = grid[g * two : (g + 1) * two].T
            for b in range(8):
                u = block_t[b * window : b * window + half]
                v = block_t[b * window + half : (b + 1) * window]
                turn = turn_out[g * 8 + b]
                same, cross = turn[0:1], turn[1:2]
                block = (u + spin(v, 1.0, -1.0)) * same
                block -= pltpu.roll(u, window, 1) * cross + v * sign(cross, -1.0, 1.0)
                r_send[part, g * 8 + b] = block.astype(BF)
        send_facets(r_send, r_recv, sc, rc, part)

    row_load.wait()

    def back_term(part, pairs):
        total = None
        take_facets(r_recv, sc, rc, part, pairs)
        for q in pairs:
            for g in range(groups):
                first = g * 8 + 2 * pair_at(q)
                pieces = [r_recv[part, first + h] for h in range(2)]
                spun = [spin(piece.astype(F32), 1.0, -1.0).astype(BF) for piece in pieces]
                block = jnp.concatenate(
                    [jnp.concatenate(pieces, axis=1), jnp.concatenate(spun, axis=1)], axis=0
                )
                at = pl.multiple_of(first * two, 2 * two)
                term = jnp.dot(block, t2[pl.ds(at, 2 * two), :], preferred_element_type=F32)
                total = term if total is None else total + term
        return total

    def back_strips(part):
        total = (bacc[...] + back_term(part, waits[1])).astype(BF)
        for cp in range(nc):
            b_send[part, cp] = total[:, cp * rows : (cp + 1) * rows]
        for step in col_steps:
            at = rd.at[0 if step in near_steps else 1 + part]
            col_link(b_send, b_recv, sd, at, part, col_at(step, 1), c).start()
        b_recv[part, c] = b_send[part, c]

    bacc[...] = back_term(0, waits[0])
    back_strips(0)
    bacc[...] = back_term(1, waits[0])
    back_strips(1)
    if near_steps:
        sum_of(b_recv, 0, 2 * len(near_steps), sd.at[0], rd.at[0]).wait_recv()
    mine = [b_recv[part, wide * group_at(0) + k] for part in range(2) for k in range(wide)]
    at = pl.multiple_of(group_at(0) * 2 * chunk, 2 * chunk)
    base_out[...] = jnp.dot(
        image_rows(mine), tab[pl.ds(at, 2 * chunk), :], preferred_element_type=F32
    )
    sum_of(b_recv, 0, len(far_steps), sd.at[0], rd.at[1]).wait_recv()
    sum_of(b_recv, 1, len(far_steps), sd.at[1], rd.at[2]).wait_recv()
    for part in range(2):
        for d in range(1, n_groups):
            for k in range(wide):
                back_out[((d - 1) * 2 + part) * wide + k] = b_recv[part, wide * group_at(d) + k]
    for part in range(2):
        sum_of(s_send, part, nc - 1, sa.at[part], rd.at[0]).wait_send()
        sum_of(b_send, part, nc - 1, sd.at[part], rd.at[0]).wait_send()
        sum_of(g_send, part, nf - 1, sb.at[part], rb.at[0, 0]).wait_send()
        sum_of(r_send, part, nf - 1, sc.at[part], rc.at[0, 0]).wait_send()


def image_kernel(nc, back, base, tab, out, buf, sem):
    c = lax.axis_index("col")
    wide = 2 - nc % 2
    n_groups = nc // wide
    tiles, rows, tile = buf.shape[0], buf.shape[2], buf.shape[3]
    depth = 2 * wide * back.shape[1]
    strip = image_rows([back[k] for k in range(back.shape[0])])
    stores = []
    for t in range(tiles):
        lanes = slice(t * tile, (t + 1) * tile)
        piece = base[:, lanes]
        for d in range(1, n_groups):
            at = pl.multiple_of(lax.rem(c // wide + d, n_groups) * depth, depth)
            piece += jnp.dot(
                strip[:, (d - 1) * depth : d * depth],
                tab[pl.ds(at, depth), lanes],
                preferred_element_type=F32,
            )
        for part in range(2):
            buf[t, part] = piece[part * rows : (part + 1) * rows]
        store = pltpu.make_async_copy(buf.at[t], out.at[:, :, lanes], sem.at[t])
        store.start()
        stores.append(store)
    for store in stores:
        store.wait()


def solution(mesh):
    nf, nc = mesh.shape["facet"], mesh.shape["col"]

    def on_device(facets, observed, uv_cells, counts):
        rows, extent = facets.shape[1:]
        vis = observed.shape[2]
        pc = counts.shape[0]
        window = S // 8
        two = 2 * window
        groups = nf // 8
        wide = 2 - nc % 2
        assert pc == nf and nf % 8 == 0 and nf <= 32 and nc > wide
        constants = make_constants(nf, nc, pc, extent)
        vmem = pl.BlockSpec(memory_space=pltpu.VMEM)
        hbm = pl.BlockSpec(memory_space=pltpu.HBM)
        dma = pltpu.SemaphoreType.DMA
        fixed = functools.partial(pltpu.with_memory_space_constraint, memory_space=pltpu.HBM)
        back, base, tab = pl.pallas_call(
            functools.partial(cycle_kernel, nf, nc),
            out_shape=(
                jax.ShapeDtypeStruct((2 * nc - 2 * wide, window, rows), BF),
                jax.ShapeDtypeStruct((2 * rows, extent), F32),
                jax.ShapeDtypeStruct((nc * two, extent), BF),
            ),
            in_specs=[hbm] * 8,
            out_specs=(vmem, vmem, vmem),
            scratch_shapes=[
                pltpu.VMEM((2 * rows, extent), BF),
                pltpu.VMEM((2, pc, vis), F32),
                pltpu.VMEM((2, pc, vis), jnp.int32),
                pltpu.SMEM((pc,), jnp.int32),
                pltpu.VMEM((pc, 2, two), F32),
                pltpu.VMEM((nf, 2, two), F32),
                pltpu.VMEM((pc * two, extent), BF),
                pltpu.VMEM((extent, pc * two), BF),
                pltpu.VMEM((two, pc * two), F32),
                pltpu.VMEM((window, extent), F32),
                pltpu.VMEM((2, nc, window, rows), BF),
                pltpu.VMEM((2, nc, window, rows), BF),
                pltpu.VMEM((2, pc, window // 2, two), BF),
                pltpu.VMEM((2, nf, window // 2, two), BF),
                pltpu.VMEM((2 * S, vis), BF),
                pltpu.VMEM((vis, 2 * S), BF),
                pltpu.VMEM((S // 16, vis), F32),
                pltpu.VMEM((S // 16, vis), F32),
                pltpu.VMEM((2, groups * two, vis), F32),
                pltpu.VMEM((groups * two, vis), F32),
                pltpu.VMEM((groups * two, vis), BF),
                pltpu.VMEM((2, nf, window // 2, two), BF),
                pltpu.VMEM((2, pc, window // 2, two), BF),
                pltpu.VMEM((2, nc, window, rows), BF),
                pltpu.VMEM((2, nc, window, rows), BF),
                pltpu.SemaphoreType.REGULAR((2,)),
                dma((11,)), dma((2, nc // wide)),
                dma((2,)), dma((2 * nc - 2,)), dma((2,)), dma((2, 2)),
                dma((2,)), dma((2, 2)), dma((2,)), dma((3,)),
            ],
            compiler_params=pltpu.CompilerParams(
                collective_id=0, has_side_effects=True, vmem_limit_bytes=44 * 2**20
            ),
            name="cycle",
        )(
            fixed(facets), fixed(observed), fixed(uv_cells), fixed(counts),
            *(fixed(jnp.asarray(constant)) for constant in constants),
        )
        tile = 256
        return pl.pallas_call(
            functools.partial(image_kernel, nc),
            out_shape=jax.ShapeDtypeStruct((2, rows, extent), F32),
            in_specs=[vmem, vmem, vmem],
            out_specs=hbm,
            scratch_shapes=[
                pltpu.VMEM((extent // tile, 2, rows, tile), F32),
                dma((extent // tile,)),
            ],
            compiler_params=pltpu.CompilerParams(vmem_limit_bytes=16 * 2**20),
            name="image",
        )(back, base, tab)

    return jax.shard_map(
        on_device,
        mesh=mesh,
        in_specs=(
            P(None, ("facet", "col"), None),
            P(None, "col", None),
            P(None, "col", None),
            P("col"),
        ),
        out_specs=P(None, ("facet", "col"), None),
        check_vma=False,
    )
```

```python
import functools
import math

import jax
import jax.numpy as jnp
import numpy as np
from jax import lax
from jax.experimental import pallas as pl
from jax.experimental.pallas import tpu as pltpu
from jax.sharding import PartitionSpec as P

S = 512
IMAGE = 65536
MESH = pl.DeviceIdType.MESH
BF = jnp.bfloat16
F32 = jnp.float32
NT = (((1,), (1,)), ((), ()))


def unit(ticks):
    angle = (np.asarray(ticks, np.int64) % IMAGE) * (-2.0 * math.pi / IMAGE)
    return np.cos(angle), np.sin(angle)


def make_constants(facets, columns, per_column, extent):
    window = S // 8
    spacing = IMAGE // extent
    cells = np.arange(extent, dtype=np.int64)
    weight = (0.6 + 0.4 * np.sin(math.pi * (cells + 0.5) / extent) ** 2) / math.sqrt(extent)
    step = np.arange(window, dtype=np.int64)
    col = np.arange(columns, dtype=np.int64)
    vc = col * (IMAGE // 4) + (29 * col + 3) % spacing
    sub = np.arange(per_column, dtype=np.int64)
    us = sub * (IMAGE // 64) + (37 * sub + 5) % (IMAGE * 8 // S)

    def table(start, stride):
        real, imag = unit((start[:, None] + stride * step)[:, :, None] * cells)
        return np.stack([real * weight, imag * weight], axis=1).astype(np.float32).astype(BF)

    wide = 2 - columns % 2
    col_tab = table(vc, spacing).reshape(columns // wide, wide, 2, 2, window // 2, extent)
    col_tab = col_tab.transpose(0, 3, 1, 2, 4, 5).reshape(-1, extent)
    row_tab = table(us, IMAGE // window).reshape(-1, extent)
    assert extent % window == 0
    fy = extent * (np.arange(facets, dtype=np.int64) % 8)
    fx = extent * (np.arange(facets, dtype=np.int64) // 8)
    real, imag = unit((fy[:, None] * vc)[:, :, None] + (fx[:, None] * us)[:, None, :])
    same = np.stack([real, real], axis=-1)
    cross = np.stack([-imag, imag], axis=-1)
    turn = np.repeat(np.stack([same, cross], axis=3), window, axis=4)
    flat = np.ascontiguousarray
    return flat(col_tab), row_tab, flat(row_tab.T), turn.astype(np.float32)


def spin(value, first, second):
    half = value.shape[1] // 2
    lane = lax.broadcasted_iota(jnp.int32, value.shape, 1)
    return pltpu.roll(value, half, 1) * jnp.where(lane < half, first, second)


def sign(value, first, second):
    lane = lax.broadcasted_iota(jnp.int32, value.shape, 1)
    return value * jnp.where(lane < value.shape[1] // 2, first, second)


def image_rows(blocks):
    half = blocks[0].shape[0] // 2
    cross = []
    for block in blocks:
        cross += [block[half:], -block[:half]]
    return jnp.concatenate(
        [jnp.concatenate(blocks, axis=0).T, jnp.concatenate(cross, axis=0).T], axis=0
    )


def cycle_kernel(
    nf, nc, x_hbm, obs_hbm, cells_hbm, counts_hbm, ctab_hbm, rtab_hbm, ttab_hbm, turn_hbm,
    back_out, base_out, tab,
    xbuf, obs, cells, counts, turn_in, turn_out, t2, tt, acc, bacc,
    s_send, s_recv, g_send, g_recv, right, right_t, r1r, r1i, left, inner, held,
    r_send, r_recv, b_send, b_recv,
    tok, in_sem, tab_sem, sa, ra, sb, rb, sc, rc, sd, rd,
):
    f = lax.axis_index("facet")
    c = lax.axis_index("col")
    window = S // 8
    half = window // 2
    two = 2 * window
    parts = window // 16
    pc = nf
    rows = xbuf.shape[0] // 2
    groups = nf // 8
    vis = obs.shape[2]
    if nc % 2:
        col_steps = [(d, 0) for d in range(1, nc)]
        wide = 1
    else:
        col_steps = [(d, k) for d in range(nc // 2 - 1, -1, -1) for k in range(2) if d or k]
        wide = 2
    near_steps = [step for step in col_steps if step[0] == 0]
    far_steps = [step for step in col_steps if step[0]]

    def col_at(step, sign):
        if nc % 2:
            return lax.rem(c + nc + sign * step[0], nc)
        top = lax.rem(c // 2 + nc // 2 + sign * step[0], nc // 2)
        return 2 * top + lax.rem(c + step[1], 2)

    def pair_at(q):
        return lax.rem(f // 2 + q, 4)

    def group_of(q):
        return 0 if q in waits[0] else 1

    def facet_link(src_buf, dst_buf, send, recv, part, peer):
        return pltpu.make_async_remote_copy(
            src_buf.at[part * nf + peer], dst_buf.at[part * nf + f], send, recv, (peer, c), MESH
        )

    def col_link(src, dst, send, recv, peer):
        return pltpu.make_async_remote_copy(src, dst, send, recv, (f, peer), MESH)

    def sum_of(buf, start, count, send, recv):
        some = buf.at[start : start + count]
        return pltpu.make_async_remote_copy(some, some, send, recv, (mate, c), MESH)

    waits = ((0, 1), (3, 2))
    mate = f + 1 - 2 * lax.rem(f, 2)

    barrier = pltpu.get_barrier_semaphore()
    place, last_place = f // 2, nf // 2 - 1
    low, high = place > 0, place < last_place
    far_low, far_high = place > 1, place < last_place - 1

    def signal(sem, facet, col):
        pl.semaphore_signal(sem, inc=1, device_id=(facet, col), device_id_type=MESH)

    def pass_on(way):
        pl.semaphore_wait(tok.at[way], 1)
        signal(tok.at[way], f + 2 - 4 * way, c)

    for d in range(1, nc):
        signal(barrier, f, lax.rem(c + d, nc))
    signal(barrier, mate, c)

    @pl.when(high)
    def _():
        signal(barrier, f + 2, c)
        pl.when(~low)(lambda: signal(barrier, mate + 2, c))

    @pl.when(low)
    def _():
        signal(barrier, f - 2, c)
        pl.when(~high)(lambda: signal(barrier, mate - 2, c))


    n_groups = nc // wide
    chunk = wide * window

    def group_at(d):
        return lax.rem(c // wide + n_groups + d, n_groups)

    far_groups = list(range(n_groups - 1, 0, -1)) if wide == 2 else list(range(1, nc))

    def tab_load(d, lanes, sem):
        at = pl.ds(pl.multiple_of(group_at(d) * 2 * chunk, 2 * chunk), 2 * chunk)
        return pltpu.make_async_copy(ctab_hbm.at[at, lanes], tab.at[at, lanes], sem)

    quarter = xbuf.shape[1] // 4
    depths = [slice(0, quarter), slice(quarter, 2 * quarter), slice(2 * quarter, 4 * quarter)]
    early = [
        [tab_load(d, lanes, tab_sem.at[k, d]) for d in far_groups]
        + [
            pltpu.make_async_copy(
                x_hbm.at[p, :, lanes], xbuf.at[p * rows : (p + 1) * rows, lanes], in_sem.at[2 * k + p]
            )
            for p in range(2)
        ]
        for k, lanes in enumerate(depths)
    ]
    mine_load = tab_load(0, slice(None), tab_sem.at[0, 0])
    row_load = pltpu.make_async_copy(rtab_hbm, t2, in_sem.at[13])
    small_loads = [
        pltpu.make_async_copy(turn_hbm.at[f, c], turn_in, in_sem.at[8]),
        pltpu.make_async_copy(turn_hbm.at[:, c, f], turn_out, in_sem.at[9]),
        pltpu.make_async_copy(obs_hbm, obs, in_sem.at[10]),
        pltpu.make_async_copy(cells_hbm, cells, in_sem.at[11]),
        pltpu.make_async_copy(counts_hbm, counts, in_sem.at[12]),
    ]
    turned_load = pltpu.make_async_copy(ttab_hbm, tt, in_sem.at[14])
    for load in sum(early, []):
        load.start()

    def strip_term(d, lanes):
        at = pl.multiple_of(group_at(d) * 2 * chunk, 2 * chunk)
        return lax.dot_general(
            tab[pl.ds(at, 2 * chunk), lanes], xbuf[:, lanes], NT, preferred_element_type=F32
        )

    def strips(d, both):
        for k in range(wide):
            for part in range(parts):
                at = part // 2 * chunk + k * window + part % 2 * 16
                real, imag = both[at : at + 16], both[at + half : at + half + 16]
                block = [real[:, :rows] - imag[:, rows:], imag[:, :rows] + real[:, rows:]]
                s_send[wide * group_at(d) + k, part] = jnp.concatenate(block, axis=0).astype(BF)

    def strip_link(step, part):
        peer = col_at(step, 1)
        at = ra.at[part * len(far_steps) + far_steps.index(step)]
        return col_link(s_send.at[peer, part], s_recv.at[c, part], sa.at[0], at, peer)

    def near_link(step):
        peer = col_at(step, 1)
        at = ra.at[parts * len(far_steps) + near_steps.index(step)]
        return col_link(s_send.at[peer], s_recv.at[c], sa.at[0], at, peer)

    sums = [0.0] * len(far_groups)
    for lanes, loads in zip(depths, early):
        for load in loads:
            load.wait()
        if lanes is depths[0]:
            mine_load.start()
            for load in small_loads:
                load.start()
        if lanes is depths[-1]:
            turned_load.start()
        for n, d in enumerate(far_groups):
            sums[n] += strip_term(d, lanes)
    for d, both in zip(far_groups, sums):
        strips(d, both)
    greeted = (low, high, place == 1, place == last_place - 1)
    pl.semaphore_wait(barrier, nc + sum(one.astype(jnp.int32) for one in greeted))
    for part in range(parts):
        for step in far_steps:
            strip_link(step, part).start()
    pl.when((place == 1) & high)(lambda: signal(tok.at[0], f + 2, c))
    pl.when((place == last_place - 1) & low)(lambda: signal(tok.at[1], f - 2, c))
    mine_load.wait()
    strips(0, strip_term(0, slice(None)))
    for step in near_steps:
        near_link(step).start()

    @pl.when(far_low & high)
    def _():
        pass_on(0)

    @pl.when(far_high & low)
    def _():
        pass_on(1)

    turned_load.wait()

    def window_term(block, src):
        at = pl.multiple_of(src * rows, rows)
        return jnp.dot(block, tt[pl.ds(at, rows), :], preferred_element_type=F32)

    acc[...] = window_term(s_send[c].reshape(two, rows), c)

    for load in small_loads:
        load.wait()

    def send_windows(part):
        def act(index):
            facet_link(g_send, g_recv, sb.at[0], rb.at[part], part, index).start()

        for index in range(nf - 1, -1, -1):
            pl.when(index != f)(functools.partial(act, index))
        g_recv[part * nf + f] = g_send[part * nf + f]

    first = cells[0, pl.ds(f, 1), :]
    second = cells[1, pl.ds(f, 1), :]

    def series(square, first, terms):
        value = jnp.full_like(square, 1.0 / math.factorial(first + 2 * terms))
        for k in range(terms - 1, -1, -1):
            value = 1.0 / math.factorial(first + 2 * k) - value * square
        return value

    def wave(count, step, cell):
        index = step * lax.broadcasted_iota(jnp.int32, (count, vis), 0)
        turn = ((index * cell + S // 2) & (S - 1)) - S // 2
        angle = turn.astype(F32) * (-math.pi / S)
        square = angle * angle
        sine = angle * series(square, 1, 5)
        return 1.0 - 2.0 * sine * sine, 2.0 * sine * series(square, 0, 6)

    scale = 1.0 / math.sqrt(vis)
    live = lax.broadcasted_iota(jnp.int32, (1, vis), 1) < counts[f]
    gain = jnp.where(live, scale, 0.0)
    m0r, m0i = wave(16, 1, second)
    m0r, m0i = m0r * gain, m0i * gain
    r1r[...], r1i[...] = wave(S // 16, 16, second)

    def right_body(i, carry):
        er, ei = r1r[pl.ds(i, 1), :], r1i[pl.ds(i, 1), :]
        b = i // parts
        k = i - b * parts
        at = pl.multiple_of(k * (2 * S // parts) + b * half, 16)
        right[pl.ds(at, 16), :] = (m0r * er - m0i * ei).astype(BF)
        right[pl.ds(at + 16, 16), :] = (m0r * ei + m0i * er).astype(BF)
        return carry

    lax.fori_loop(0, S // 16, right_body, 0)

    for step in near_steps:
        near_link(step).wait_recv()
        src = col_at(step, -1)
        acc[...] += window_term(s_recv[src].reshape(two, rows), src)

    def windows(some):
        lo, hi = some[0], some[-1] + 1
        total = acc[lo * half : hi * half]
        for step in far_steps:
            for part in some:
                strip_link(step, part).wait_recv()
            src = col_at(step, -1)
            block = s_recv[src, lo:hi].reshape((hi - lo) * half, rows)
            total += window_term(block, src)
        for part in some:
            at = (part - lo) * half
            for j in range(pc):
                u = total[at : at + 16, j * two : (j + 1) * two]
                v = total[at + 16 : at + half, j * two : (j + 1) * two]
                turn = turn_in[j]
                same, cross = turn[0:1], turn[1:2]
                win = u * same + spin(v, -1.0, 1.0) * same
                win += pltpu.roll(u, window, 1) * cross + v * sign(cross, 1.0, -1.0)
                g_send[part * pc + j] = win.astype(BF)
        if 0 in some:
            pl.when(far_high & ~low)(lambda: pl.semaphore_wait(tok.at[1], 1))
            pl.when(far_low & ~high)(lambda: pl.semaphore_wait(tok.at[0], 1))
        for part in some:
            send_windows(part)

    windows([0])

    windows([1])
    windows(list(range(2, parts)))
    row_load.start()

    l0r, l0i = wave(16, 1, first)
    l1r, l1i = wave(max(groups * parts, 8), 16, first)
    for i in range(groups * parts):
        er, ei = l1r[i : i + 1], l1i[i : i + 1]
        at = i // parts * two + i % parts * 16
        real = (l0r * er - l0i * ei).astype(BF).astype(F32)
        imag = (l0r * ei + l0i * er).astype(BF).astype(F32)
        left[0, at : at + 16, :] = real
        left[0, at + window : at + window + 16, :] = -imag
        left[1, at : at + 16, :] = imag
        left[1, at + window : at + window + 16, :] = real

    deep = 2 * S // parts

    def turn_body(b, carry):
        pieces = [right[pl.ds(pl.multiple_of(k * deep + b * half, 16), half), :] for k in range(parts)]
        at = pl.multiple_of(b * two, two)
        right_t[:, pl.ds(at, two)] = jnp.concatenate(pieces, axis=0).T
        return carry

    lax.fori_loop(0, S // window, turn_body, 0)

    def pred_term(some, g):
        blocks = []
        for part in some:
            for b in range(8):
                block = g_recv[part * nf + g * 8 + b].astype(F32)
                blocks += [block, spin(block, -1.0, 1.0)]
        return jnp.dot(
            jnp.concatenate(blocks, axis=0).T.astype(BF),
            right[some[0] * deep : (some[-1] + 1) * deep, :],
            preferred_element_type=F32,
        )

    def take_windows(some):
        for part in some:
            sum_of(g_recv, part * nf, nf - 1, sb.at[0], rb.at[part]).wait_recv()

    early_parts, late_parts = list(range(parts // 2)), list(range(parts // 2, parts))
    take_windows(early_parts)
    for g in range(groups):
        inner[g * two : (g + 1) * two] = pred_term(early_parts, g)

    for part in late_parts[:-1]:
        take_windows([part])
        for g in range(groups):
            inner[g * two : (g + 1) * two] += pred_term([part], g)
    take_windows(late_parts[-1:])
    res_r, res_i = obs[0, pl.ds(f, 1), :], obs[1, pl.ds(f, 1), :]
    for g in range(groups):
        at = slice(g * two, (g + 1) * two)
        value = inner[at] + pred_term(late_parts[-1:], g)
        unscale = 1.0 / (scale * S)
        res_r -= jnp.sum(value * left[0, at], axis=0, keepdims=True) * unscale
        res_i -= jnp.sum(value * left[1, at], axis=0, keepdims=True) * unscale
    held[...] = (res_r * left[0] + res_i * left[1]).astype(BF)

    def send_back(part, index):
        def act(group):
            recv = rc.at[2 * part + group]
            facet_link(r_send, r_recv, sc.at[0], recv, part, index).start()

        near = lax.rem(place - index // 2 + nf // 2, 4)
        pl.when((near < 2) & (index != f))(lambda: act(0))
        pl.when(near >= 2)(lambda: act(1))

    def grid_blocks(lo, hi):
        grid = jnp.dot(held[...], right_t[:, lo * two : hi * two], preferred_element_type=F32)
        for g in range(groups):
            block_t = grid[g * two : (g + 1) * two].T
            for b in range(lo, hi):
                turn = turn_out[g * 8 + b]
                same, cross = turn[0:1], turn[1:2]
                for part in range(2):
                    starts = [(b - lo) * two + (2 * part + k) * half for k in range(2)]
                    u = jnp.concatenate([block_t[at : at + 16] for at in starts], axis=0)
                    v = jnp.concatenate([block_t[at + 16 : at + half] for at in starts], axis=0)
                    block = (u + spin(v, 1.0, -1.0)) * same
                    block -= pltpu.roll(u, window, 1) * cross + v * sign(cross, -1.0, 1.0)
                    r_send[part * nf + g * 8 + b] = block.astype(BF)

    grid_blocks(0, 2)
    for part in range(2):
        for index in range(2):
            send_back(part, index)
    grid_blocks(2, 8)
    for part in range(2):
        for index in range(2, nf):
            send_back(part, index)
        r_recv[part * nf + f] = r_send[part * nf + f]

    row_load.wait()

    def back_term(part, pairs):
        total = None
        group = waits.index(pairs)
        count = 4 * groups - (0 in pairs)
        sum_of(r_recv, part * nf, count, sc.at[0], rc.at[2 * part + group]).wait_recv()
        for q in pairs:
            for g in range(groups):
                first = g * 8 + 2 * pair_at(q)
                pieces = [r_recv[part * nf + first + h] for h in range(2)]
                spun = [spin(piece.astype(F32), 1.0, -1.0).astype(BF) for piece in pieces]
                block = jnp.concatenate(
                    [jnp.concatenate(pieces, axis=1), jnp.concatenate(spun, axis=1)], axis=0
                )
                at = pl.multiple_of(first * two, 2 * two)
                term = jnp.dot(block, t2[pl.ds(at, 2 * two), :], preferred_element_type=F32)
                total = term if total is None else total + term
        return total

    def back_strips(part):
        total = (bacc[...] + back_term(part, waits[1])).astype(BF)
        for cp in range(nc):
            b_send[part * nc + cp] = total[:, cp * rows : (cp + 1) * rows]
        for step in col_steps:
            peer = col_at(step, 1)
            at = rd.at[0 if step in near_steps else 1 + part]
            col_link(
                b_send.at[part * nc + peer], b_recv.at[part * nc + c], sd.at[0], at, peer
            ).start()
        b_recv[part * nc + c] = b_send[part * nc + c]

    bacc[...] = back_term(0, waits[0])
    back_strips(0)
    bacc[...] = back_term(1, waits[0])
    back_strips(1)
    if near_steps:
        sum_of(b_recv, 0, 2 * len(near_steps), sd.at[0], rd.at[0]).wait_recv()
    mine = [b_recv[part * nc + wide * group_at(0) + k] for part in range(2) for k in range(wide)]
    at = pl.multiple_of(group_at(0) * 2 * chunk, 2 * chunk)
    base_out[...] = jnp.dot(
        image_rows(mine), tab[pl.ds(at, 2 * chunk), :], preferred_element_type=F32
    )
    for part in range(2):
        sum_of(b_recv, 0, len(far_steps), sd.at[0], rd.at[1 + part]).wait_recv()
        for d in range(1, n_groups):
            for k in range(wide):
                at = part * nc + wide * group_at(d) + k
                back_out[((d - 1) * 2 + part) * wide + k] = b_recv[at]
    sum_of(s_send, 0, nc - 1, sa.at[0], ra.at[0]).wait_send()
    sum_of(b_send, 0, 2 * (nc - 1), sd.at[0], rd.at[0]).wait_send()
    sum_of(g_send, 0, parts * (nf - 1), sb.at[0], rb.at[0]).wait_send()
    sum_of(r_send, 0, 2 * (nf - 1), sc.at[0], rc.at[0]).wait_send()


def image_kernel(nc, back, base, tab, out, buf, sem):
    c = lax.axis_index("col")
    wide = 2 - nc % 2
    n_groups = nc // wide
    tiles, rows, tile = buf.shape[0], buf.shape[2], buf.shape[3]
    depth = 2 * wide * back.shape[1]
    strip = image_rows([back[k] for k in range(back.shape[0])])
    stores = []
    for t in range(tiles):
        lanes = slice(t * tile, (t + 1) * tile)
        piece = base[:, lanes]
        for d in range(1, n_groups):
            at = pl.multiple_of(lax.rem(c // wide + d, n_groups) * depth, depth)
            piece += jnp.dot(
                strip[:, (d - 1) * depth : d * depth],
                tab[pl.ds(at, depth), lanes],
                preferred_element_type=F32,
            )
        for part in range(2):
            buf[t, part] = piece[part * rows : (part + 1) * rows]
        store = pltpu.make_async_copy(buf.at[t], out.at[:, :, lanes], sem.at[t])
        store.start()
        stores.append(store)
    for store in stores:
        store.wait()


def solution(mesh):
    nf, nc = mesh.shape["facet"], mesh.shape["col"]

    def on_device(facets, observed, uv_cells, counts):
        rows, extent = facets.shape[1:]
        vis = observed.shape[2]
        pc = counts.shape[0]
        window = S // 8
        two = 2 * window
        groups = nf // 8
        wide = 2 - nc % 2
        parts = window // 16
        assert pc == nf and nf % 8 == 0 and nf <= 32 and nc > wide
        constants = make_constants(nf, nc, pc, extent)
        vmem = pl.BlockSpec(memory_space=pltpu.VMEM)
        hbm = pl.BlockSpec(memory_space=pltpu.HBM)
        dma = pltpu.SemaphoreType.DMA
        fixed = functools.partial(pltpu.with_memory_space_constraint, memory_space=pltpu.HBM)
        back, base, tab = pl.pallas_call(
            functools.partial(cycle_kernel, nf, nc),
            out_shape=(
                jax.ShapeDtypeStruct((2 * nc - 2 * wide, window, rows), BF),
                jax.ShapeDtypeStruct((2 * rows, extent), F32),
                jax.ShapeDtypeStruct((nc * two, extent), BF),
            ),
            in_specs=[hbm] * 8,
            out_specs=(vmem, vmem, vmem),
            scratch_shapes=[
                pltpu.VMEM((2 * rows, extent), BF),
                pltpu.VMEM((2, pc, vis), F32),
                pltpu.VMEM((2, pc, vis), jnp.int32),
                pltpu.SMEM((pc,), jnp.int32),
                pltpu.VMEM((pc, 2, two), F32),
                pltpu.VMEM((nf, 2, two), F32),
                pltpu.VMEM((pc * two, extent), BF),
                pltpu.VMEM((extent, pc * two), BF),
                pltpu.VMEM((two, pc * two), F32),
                pltpu.VMEM((window, extent), F32),
                pltpu.VMEM((nc, parts, window // 2, rows), BF),
                pltpu.VMEM((nc, parts, window // 2, rows), BF),
                pltpu.VMEM((parts * pc, 16, two), BF),
                pltpu.VMEM((parts * nf, 16, two), BF),
                pltpu.VMEM((2 * S, vis), BF),
                pltpu.VMEM((vis, 2 * S), BF),
                pltpu.VMEM((S // 16, vis), F32),
                pltpu.VMEM((S // 16, vis), F32),
                pltpu.VMEM((2, groups * two, vis), F32),
                pltpu.VMEM((groups * two, vis), F32),
                pltpu.VMEM((groups * two, vis), BF),
                pltpu.VMEM((2 * nf, window // 2, two), BF),
                pltpu.VMEM((2 * pc, window // 2, two), BF),
                pltpu.VMEM((2 * nc, window, rows), BF),
                pltpu.VMEM((2 * nc, window, rows), BF),
                pltpu.SemaphoreType.REGULAR((2,)),
                dma((15,)), dma((4, nc // wide)),
                dma((1,)), dma((parts * (nc - wide) + wide - 1,)), dma((1,)), dma((parts,)),
                dma((1,)), dma((4,)), dma((1,)), dma((3,)),
            ],
            compiler_params=pltpu.CompilerParams(
                collective_id=0, has_side_effects=True, vmem_limit_bytes=44 * 2**20
            ),
            name="cycle",
        )(
            fixed(facets), fixed(observed), fixed(uv_cells), fixed(counts),
            *(fixed(jnp.asarray(constant)) for constant in constants),
        )
        tile = 256
        return pl.pallas_call(
            functools.partial(image_kernel, nc),
            out_shape=jax.ShapeDtypeStruct((2, rows, extent), F32),
            in_specs=[vmem, vmem, vmem],
            out_specs=hbm,
            scratch_shapes=[
                pltpu.VMEM((extent // tile, 2, rows, tile), F32),
                dma((extent // tile,)),
            ],
            compiler_params=pltpu.CompilerParams(vmem_limit_bytes=16 * 2**20),
            name="image",
        )(back, base, tab)

    return jax.shard_map(
        on_device,
        mesh=mesh,
        in_specs=(
            P(None, ("facet", "col"), None),
            P(None, "col", None),
            P(None, "col", None),
            P("col"),
        ),
        out_specs=P(None, ("facet", "col"), None),
        check_vma=False,
    )
```

```python
import functools
import math

import jax
import jax.numpy as jnp
import numpy as np
from jax import lax
from jax.experimental import pallas as pl
from jax.experimental.pallas import tpu as pltpu
from jax.sharding import PartitionSpec as P

S = 512
IMAGE = 65536
MESH = pl.DeviceIdType.MESH
BF = jnp.bfloat16
F32 = jnp.float32
NT = (((1,), (1,)), ((), ()))


def unit(ticks):
    angle = (np.asarray(ticks, np.int64) % IMAGE) * (-2.0 * math.pi / IMAGE)
    return np.cos(angle), np.sin(angle)


def make_constants(facets, columns, per_column, extent):
    window = S // 8
    spacing = IMAGE // extent
    cells = np.arange(extent, dtype=np.int64)
    weight = (0.6 + 0.4 * np.sin(math.pi * (cells + 0.5) / extent) ** 2) / math.sqrt(extent)
    step = np.arange(window, dtype=np.int64)
    col = np.arange(columns, dtype=np.int64)
    vc = col * (IMAGE // 4) + (29 * col + 3) % spacing
    sub = np.arange(per_column, dtype=np.int64)
    us = sub * (IMAGE // 64) + (37 * sub + 5) % (IMAGE * 8 // S)

    def table(start, stride):
        real, imag = unit((start[:, None] + stride * step)[:, :, None] * cells)
        return np.stack([real * weight, imag * weight], axis=1).astype(np.float32).astype(BF)

    wide = 2 - columns % 2
    col_tab = table(vc, spacing).reshape(columns // wide, wide, 2, 2, window // 2, extent)
    col_tab = col_tab.transpose(0, 3, 1, 2, 4, 5).reshape(-1, extent)
    row_tab = table(us, IMAGE // window).reshape(-1, extent)
    assert extent % window == 0
    fy = extent * (np.arange(facets, dtype=np.int64) % 8)
    fx = extent * (np.arange(facets, dtype=np.int64) // 8)
    real, imag = unit((fy[:, None] * vc)[:, :, None] + (fx[:, None] * us)[:, None, :])
    same = np.stack([real, real], axis=-1)
    cross = np.stack([-imag, imag], axis=-1)
    turn = np.repeat(np.stack([same, cross], axis=3), window, axis=4)
    flat = np.ascontiguousarray
    return flat(col_tab), row_tab, flat(row_tab.T), turn.astype(np.float32)


def spin(value, first, second):
    half = value.shape[1] // 2
    lane = lax.broadcasted_iota(jnp.int32, value.shape, 1)
    return pltpu.roll(value, half, 1) * jnp.where(lane < half, first, second)


def sign(value, first, second):
    lane = lax.broadcasted_iota(jnp.int32, value.shape, 1)
    return value * jnp.where(lane < value.shape[1] // 2, first, second)


def series(square, first, terms):
    value = jnp.full_like(square, 1.0 / math.factorial(first + 2 * terms))
    for k in range(terms - 1, -1, -1):
        value = 1.0 / math.factorial(first + 2 * k) - value * square
    return value


def turns(ticks, whole):
    turn = ((ticks + whole // 2) & (whole - 1)) - whole // 2
    angle = turn.astype(F32) * (-math.pi / whole)
    square = angle * angle
    sine = angle * series(square, 1, 5)
    return 1.0 - 2.0 * sine * sine, 2.0 * sine * series(square, 0, 6)


def image_rows(blocks):
    half = blocks[0].shape[0] // 2
    cross = []
    for block in blocks:
        cross += [block[half:], -block[:half]]
    return jnp.concatenate(
        [jnp.concatenate(blocks, axis=0).T, jnp.concatenate(cross, axis=0).T], axis=0
    )


def cycle_kernel(
    nf, nc, x_hbm, obs_hbm, cells_hbm, counts_hbm, ctab_hbm, rtab_hbm, ttab_hbm, turn_hbm,
    back_out, base_out, tab,
    xbuf, obs, cells, counts, turn_in, turn_out, t2, tt, acc, bacc,
    s_send, s_recv, g_send, g_recv, right, right_t, r1r, r1i, left, inner, held,
    r_send, r_recv, b_send, b_recv,
    tok, in_sem, sa, ra, sb, rb, sc, rc, sd, rd,
):
    f = lax.axis_index("facet")
    c = lax.axis_index("col")
    window = S // 8
    half = window // 2
    two = 2 * window
    parts = window // 16
    pc = nf
    rows = xbuf.shape[1]
    groups = nf // 8
    vis = obs.shape[2]
    if nc % 2:
        col_steps = [(d, 0) for d in range(1, nc)]
        wide = 1
    else:
        col_steps = [(d, k) for d in range(nc // 2 - 1, -1, -1) for k in range(2) if d or k]
        wide = 2
    near_steps = [step for step in col_steps if step[0] == 0]
    far_steps = [step for step in col_steps if step[0]]

    def col_at(step, sign):
        if nc % 2:
            return lax.rem(c + nc + sign * step[0], nc)
        top = lax.rem(c // 2 + nc // 2 + sign * step[0], nc // 2)
        return 2 * top + lax.rem(c + step[1], 2)

    def pair_at(q):
        return lax.rem(f // 2 + q, 4)

    def group_of(q):
        return 0 if q in waits[0] else 1

    def facet_link(src_buf, dst_buf, send, recv, part, peer):
        return pltpu.make_async_remote_copy(
            src_buf.at[part * nf + peer], dst_buf.at[part * nf + f], send, recv, (peer, c), MESH
        )

    def col_link(src, dst, send, recv, peer):
        return pltpu.make_async_remote_copy(src, dst, send, recv, (f, peer), MESH)

    def sum_of(buf, start, count, send, recv):
        some = buf.at[start : start + count]
        return pltpu.make_async_remote_copy(some, some, send, recv, (mate, c), MESH)

    waits = ((0, 1), (3, 2))
    mate = f + 1 - 2 * lax.rem(f, 2)

    barrier = pltpu.get_barrier_semaphore()
    place, last_place = f // 2, nf // 2 - 1
    low, high = place > 0, place < last_place
    far_low, far_high = place > 1, place < last_place - 1

    def signal(sem, facet, col):
        pl.semaphore_signal(sem, inc=1, device_id=(facet, col), device_id_type=MESH)

    def pass_on(way):
        pl.semaphore_wait(tok.at[way], 1)
        signal(tok.at[way], f + 2 - 4 * way, c)

    for d in range(1, nc):
        signal(barrier, f, lax.rem(c + d, nc))
    signal(barrier, mate, c)

    @pl.when(high)
    def _():
        signal(barrier, f + 2, c)
        pl.when(~low)(lambda: signal(barrier, mate + 2, c))

    @pl.when(low)
    def _():
        signal(barrier, f - 2, c)
        pl.when(~high)(lambda: signal(barrier, mate - 2, c))


    n_groups = nc // wide
    chunk = wide * window

    def group_at(d):
        return lax.rem(c // wide + n_groups + d, n_groups)

    far_groups = list(range(n_groups - 1, 0, -1)) if wide == 2 else list(range(1, nc))

    extent = xbuf.shape[2]
    quarter = extent // 4
    depths = [slice(0, quarter), slice(quarter, 2 * quarter), slice(2 * quarter, 4 * quarter)]
    x_loads = [
        pltpu.make_async_copy(x_hbm.at[:, :, lanes], xbuf.at[:, :, lanes], in_sem.at[n])
        for n, lanes in enumerate(depths)
    ]
    mine_at = pl.ds(pl.multiple_of(group_at(0) * 2 * chunk, 2 * chunk), 2 * chunk)
    mine_load = pltpu.make_async_copy(ctab_hbm.at[mine_at], tab.at[mine_at], in_sem.at[3])
    row_load = pltpu.make_async_copy(rtab_hbm, t2, in_sem.at[9])
    small_loads = [
        pltpu.make_async_copy(turn_hbm.at[f, c], turn_in, in_sem.at[4]),
        pltpu.make_async_copy(turn_hbm.at[:, c, f], turn_out, in_sem.at[5]),
        pltpu.make_async_copy(obs_hbm, obs, in_sem.at[6]),
        pltpu.make_async_copy(cells_hbm, cells, in_sem.at[7]),
        pltpu.make_async_copy(counts_hbm, counts, in_sem.at[8]),
    ]
    turned_load = pltpu.make_async_copy(ttab_hbm, tt, in_sem.at[10])
    for load in x_loads:
        load.start()

    spacing = IMAGE // extent
    lr, li = turns(
        lax.broadcasted_iota(jnp.int32, (16, extent), 0)
        * lax.broadcasted_iota(jnp.int32, (16, extent), 1),
        extent,
    )
    high_rows = lax.broadcasted_iota(jnp.int32, (wide * parts, extent), 0)
    place_q = lax.broadcasted_iota(jnp.int32, (wide * parts, extent), 1)
    taper = 0.8 - 0.2 * turns(2 * place_q + 1, 2 * extent)[0]
    taper *= 1.0 / math.sqrt(extent)
    for d in far_groups:
        cols = wide * group_at(d) + high_rows // parts
        freqs = cols * (IMAGE // 4) + ((29 * cols + 3) & (spacing - 1))
        freqs += spacing * 16 * (high_rows & (parts - 1))
        hr, hi = turns(freqs * place_q, IMAGE)
        hr, hi = hr * taper, hi * taper
        for i in range(wide * parts):
            er, ei = hr[i : i + 1], hi[i : i + 1]
            k, u = i // parts, i % parts
            at = group_at(d) * 2 * chunk + u // 2 * chunk + k * window + u % 2 * 16
            at = pl.multiple_of(at, 16)
            tab[pl.ds(at, 16), :] = (lr * er - li * ei).astype(BF)
            tab[pl.ds(at + half, 16), :] = (lr * ei + li * er).astype(BF)

    def strip_term(d, lanes):
        at = pl.multiple_of(group_at(d) * 2 * chunk, 2 * chunk)
        return lax.dot_general(
            tab[pl.ds(at, 2 * chunk), lanes],
            xbuf[:, :, lanes].reshape(2 * rows, -1),
            NT,
            preferred_element_type=F32,
        )

    def strips(d, both):
        for k in range(wide):
            for part in range(parts):
                at = part // 2 * chunk + k * window + part % 2 * 16
                real, imag = both[at : at + 16], both[at + half : at + half + 16]
                block = [real[:, :rows] - imag[:, rows:], imag[:, :rows] + real[:, rows:]]
                s_send[wide * group_at(d) + k, part] = jnp.concatenate(block, axis=0).astype(BF)

    messages = [[0], [1], list(range(2, parts))]

    def strip_link(step, some):
        peer = col_at(step, 1)
        at = ra.at[messages.index(some) * len(far_steps) + far_steps.index(step)]
        some = slice(some[0], some[-1] + 1)
        return col_link(s_send.at[peer, some], s_recv.at[c, some], sa.at[0], at, peer)

    def near_link(step):
        peer = col_at(step, 1)
        at = ra.at[len(messages) * len(far_steps) + near_steps.index(step)]
        return col_link(s_send.at[peer], s_recv.at[c], sa.at[0], at, peer)

    sums = [0.0] * len(far_groups)
    for lanes, load in zip(depths, x_loads):
        load.wait()
        if lanes is depths[0]:
            mine_load.start()
            for load in small_loads:
                load.start()
        if lanes is depths[-1]:
            turned_load.start()
        for n, d in enumerate(far_groups):
            sums[n] += strip_term(d, lanes)
    for d, both in zip(far_groups, sums):
        strips(d, both)
    greeted = (low, high, place == 1, place == last_place - 1)
    pl.semaphore_wait(barrier, nc + sum(one.astype(jnp.int32) for one in greeted))
    for some in messages:
        for step in far_steps:
            strip_link(step, some).start()
    pl.when((place == 1) & high)(lambda: signal(tok.at[0], f + 2, c))
    pl.when((place == last_place - 1) & low)(lambda: signal(tok.at[1], f - 2, c))
    mine_load.wait()
    strips(0, strip_term(0, slice(None)))
    for step in near_steps:
        near_link(step).start()

    @pl.when(far_low & high)
    def _():
        pass_on(0)

    @pl.when(far_high & low)
    def _():
        pass_on(1)

    turned_load.wait()

    def window_term(block, src):
        at = pl.multiple_of(src * rows, rows)
        return jnp.dot(block, tt[pl.ds(at, rows), :], preferred_element_type=F32)

    acc[...] = window_term(s_send[c].reshape(two, rows), c)

    for load in small_loads:
        load.wait()

    def send_windows(part):
        def act(index):
            facet_link(g_send, g_recv, sb.at[0], rb.at[part], part, index).start()

        for index in range(nf - 1, -1, -1):
            pl.when(index != f)(functools.partial(act, index))
        g_recv[part * nf + f] = g_send[part * nf + f]

    first = cells[0, pl.ds(f, 1), :]
    second = cells[1, pl.ds(f, 1), :]

    def wave(count, step, cell):
        return turns(step * lax.broadcasted_iota(jnp.int32, (count, vis), 0) * cell, S)

    scale = 1.0 / math.sqrt(vis)
    live = lax.broadcasted_iota(jnp.int32, (1, vis), 1) < counts[f]
    gain = jnp.where(live, scale, 0.0)
    m0r, m0i = wave(16, 1, second)
    m0r, m0i = m0r * gain, m0i * gain
    r1r[...], r1i[...] = wave(S // 16, 16, second)

    def right_body(i, carry):
        er, ei = r1r[pl.ds(i, 1), :], r1i[pl.ds(i, 1), :]
        b = i // parts
        k = i - b * parts
        at = pl.multiple_of(k * (2 * S // parts) + b * half, 16)
        right[pl.ds(at, 16), :] = (m0r * er - m0i * ei).astype(BF)
        right[pl.ds(at + 16, 16), :] = (m0r * ei + m0i * er).astype(BF)
        return carry

    lax.fori_loop(0, S // 16, right_body, 0)

    for step in near_steps:
        near_link(step).wait_recv()
        src = col_at(step, -1)
        acc[...] += window_term(s_recv[src].reshape(two, rows), src)

    def windows(some):
        lo, hi = some[0], some[-1] + 1
        total = acc[lo * half : hi * half]
        for step in far_steps:
            strip_link(step, some).wait_recv()
            src = col_at(step, -1)
            block = s_recv[src, lo:hi].reshape((hi - lo) * half, rows)
            total += window_term(block, src)
        for part in some:
            at = (part - lo) * half
            for j in range(pc):
                u = total[at : at + 16, j * two : (j + 1) * two]
                v = total[at + 16 : at + half, j * two : (j + 1) * two]
                turn = turn_in[j]
                same, cross = turn[0:1], turn[1:2]
                win = u * same + spin(v, -1.0, 1.0) * same
                win += pltpu.roll(u, window, 1) * cross + v * sign(cross, 1.0, -1.0)
                g_send[part * pc + j] = win.astype(BF)
        if 0 in some:
            pl.when(far_high & ~low)(lambda: pl.semaphore_wait(tok.at[1], 1))
            pl.when(far_low & ~high)(lambda: pl.semaphore_wait(tok.at[0], 1))
        for part in some:
            send_windows(part)

    windows(messages[0])

    windows(messages[1])
    windows(messages[2])
    row_load.start()

    l0r, l0i = wave(16, 1, first)
    l1r, l1i = wave(max(groups * parts, 8), 16, first)
    for i in range(groups * parts):
        er, ei = l1r[i : i + 1], l1i[i : i + 1]
        at = i // parts * two + i % parts * 16
        real = (l0r * er - l0i * ei).astype(BF).astype(F32)
        imag = (l0r * ei + l0i * er).astype(BF).astype(F32)
        left[0, at : at + 16, :] = real
        left[0, at + window : at + window + 16, :] = -imag
        left[1, at : at + 16, :] = imag
        left[1, at + window : at + window + 16, :] = real

    deep = 2 * S // parts

    def turn_body(b, carry):
        pieces = [right[pl.ds(pl.multiple_of(k * deep + b * half, 16), half), :] for k in range(parts)]
        at = pl.multiple_of(b * two, two)
        right_t[:, pl.ds(at, two)] = jnp.concatenate(pieces, axis=0).T
        return carry

    lax.fori_loop(0, S // window, turn_body, 0)

    def pred_term(some, g):
        blocks = []
        for part in some:
            for b in range(8):
                block = g_recv[part * nf + g * 8 + b].astype(F32)
                blocks += [block, spin(block, -1.0, 1.0)]
        return jnp.dot(
            jnp.concatenate(blocks, axis=0).T.astype(BF),
            right[some[0] * deep : (some[-1] + 1) * deep, :],
            preferred_element_type=F32,
        )

    def take_windows(some):
        for part in some:
            sum_of(g_recv, part * nf, nf - 1, sb.at[0], rb.at[part]).wait_recv()

    early_parts, late_parts = list(range(parts // 2)), list(range(parts // 2, parts))
    take_windows(early_parts)
    for g in range(groups):
        inner[g * two : (g + 1) * two] = pred_term(early_parts, g)

    take_windows(late_parts)
    res_r, res_i = obs[0, pl.ds(f, 1), :], obs[1, pl.ds(f, 1), :]
    for g in range(groups):
        at = slice(g * two, (g + 1) * two)
        value = inner[at] + pred_term(late_parts, g)
        unscale = 1.0 / (scale * S)
        res_r -= jnp.sum(value * left[0, at], axis=0, keepdims=True) * unscale
        res_i -= jnp.sum(value * left[1, at], axis=0, keepdims=True) * unscale
    held[...] = (res_r * left[0] + res_i * left[1]).astype(BF)

    def send_back(part, index):
        def act(group):
            recv = rc.at[2 * part + group]
            facet_link(r_send, r_recv, sc.at[0], recv, part, index).start()

        near = lax.rem(place - index // 2 + nf // 2, 4)
        pl.when((near < 2) & (index != f))(lambda: act(0))
        pl.when(near >= 2)(lambda: act(1))

    def grid_blocks(lo, hi):
        grid = jnp.dot(held[...], right_t[:, lo * two : hi * two], preferred_element_type=F32)
        for g in range(groups):
            block_t = grid[g * two : (g + 1) * two].T
            for b in range(lo, hi):
                turn = turn_out[g * 8 + b]
                same, cross = turn[0:1], turn[1:2]
                for part in range(2):
                    starts = [(b - lo) * two + (2 * part + k) * half for k in range(2)]
                    u = jnp.concatenate([block_t[at : at + 16] for at in starts], axis=0)
                    v = jnp.concatenate([block_t[at + 16 : at + half] for at in starts], axis=0)
                    block = (u + spin(v, 1.0, -1.0)) * same
                    block -= pltpu.roll(u, window, 1) * cross + v * sign(cross, -1.0, 1.0)
                    r_send[part * nf + g * 8 + b] = block.astype(BF)

    def send_backs(part, lo, hi):
        for index in range(lo, hi):
            send_back(part, index)

    grid_blocks(0, 2)
    send_backs(0, 0, 2)
    grid_blocks(2, 5)
    send_backs(1, 0, 2)
    grid_blocks(5, 8)
    for part in range(2):
        send_backs(part, 2, nf)
        r_recv[part * nf + f] = r_send[part * nf + f]

    row_load.wait()

    def back_blocks(part, pairs):
        group = waits.index(pairs)
        count = 4 * groups - (0 in pairs)
        sum_of(r_recv, part * nf, count, sc.at[0], rc.at[2 * part + group]).wait_recv()
        blocks = []
        for q in pairs:
            for g in range(groups):
                first = g * 8 + 2 * pair_at(q)
                pieces = [r_recv[part * nf + first + h] for h in range(2)]
                spun = [spin(piece.astype(F32), 1.0, -1.0).astype(BF) for piece in pieces]
                block = jnp.concatenate(
                    [jnp.concatenate(pieces, axis=1), jnp.concatenate(spun, axis=1)], axis=0
                )
                blocks.append((block, pl.multiple_of(first * two, 2 * two)))
        return blocks

    def back_term(blocks, lanes):
        return sum(
            jnp.dot(block, t2[pl.ds(at, 2 * two), lanes], preferred_element_type=F32)
            for block, at in blocks
        )

    def back_strips(part):
        blocks = back_blocks(part, waits[1])
        for d in far_groups + [0]:
            col = wide * group_at(d)
            lanes = pl.ds(pl.multiple_of(col * rows, wide * rows), wide * rows)
            total = (bacc[:, lanes] + back_term(blocks, lanes)).astype(BF)
            for k in range(wide):
                b_send[part * nc + col + k] = total[:, k * rows : (k + 1) * rows]
            for step in col_steps:
                if step[0] == d:
                    peer = col_at(step, 1)
                    at = rd.at[0 if step in near_steps else 1 + part]
                    col_link(
                        b_send.at[part * nc + peer], b_recv.at[part * nc + c], sd.at[0], at, peer
                    ).start()
        b_recv[part * nc + c] = b_send[part * nc + c]

    bacc[...] = back_term(back_blocks(0, waits[0]), slice(None))
    back_strips(0)
    bacc[...] = back_term(back_blocks(1, waits[0]), slice(None))
    back_strips(1)
    if near_steps:
        sum_of(b_recv, 0, 2 * len(near_steps), sd.at[0], rd.at[0]).wait_recv()
    mine = [b_recv[part * nc + wide * group_at(0) + k] for part in range(2) for k in range(wide)]
    base_out[...] = jnp.dot(
        image_rows(mine), tab[mine_at, :], preferred_element_type=F32
    )
    for part in range(2):
        sum_of(b_recv, 0, len(far_steps), sd.at[0], rd.at[1 + part]).wait_recv()
        for d in range(1, n_groups):
            for k in range(wide):
                at = part * nc + wide * group_at(d) + k
                back_out[((d - 1) * 2 + part) * wide + k] = b_recv[at]
    sum_of(s_send, 0, nc - 1, sa.at[0], ra.at[0]).wait_send()
    sum_of(b_send, 0, 2 * (nc - 1), sd.at[0], rd.at[0]).wait_send()
    sum_of(g_send, 0, parts * (nf - 1), sb.at[0], rb.at[0]).wait_send()
    sum_of(r_send, 0, 2 * (nf - 1), sc.at[0], rc.at[0]).wait_send()


def image_kernel(nc, back, base, tab, out, buf, sem):
    c = lax.axis_index("col")
    wide = 2 - nc % 2
    n_groups = nc // wide
    tiles, rows, tile = buf.shape[0], buf.shape[2], buf.shape[3]
    depth = 2 * wide * back.shape[1]
    strip = image_rows([back[k] for k in range(back.shape[0])])
    stores = []
    for t in range(tiles):
        lanes = slice(t * tile, (t + 1) * tile)
        piece = base[:, lanes]
        for d in range(1, n_groups):
            at = pl.multiple_of(lax.rem(c // wide + d, n_groups) * depth, depth)
            piece += jnp.dot(
                strip[:, (d - 1) * depth : d * depth],
                tab[pl.ds(at, depth), lanes],
                preferred_element_type=F32,
            )
        for part in range(2):
            buf[t, part] = piece[part * rows : (part + 1) * rows]
        store = pltpu.make_async_copy(buf.at[t], out.at[:, :, lanes], sem.at[t])
        store.start()
        stores.append(store)
    for store in stores:
        store.wait()


def solution(mesh):
    nf, nc = mesh.shape["facet"], mesh.shape["col"]

    def on_device(facets, observed, uv_cells, counts):
        rows, extent = facets.shape[1:]
        vis = observed.shape[2]
        pc = counts.shape[0]
        window = S // 8
        two = 2 * window
        groups = nf // 8
        wide = 2 - nc % 2
        parts = window // 16
        assert pc == nf and nf % 8 == 0 and nf <= 32 and nc > wide
        constants = make_constants(nf, nc, pc, extent)
        vmem = pl.BlockSpec(memory_space=pltpu.VMEM)
        hbm = pl.BlockSpec(memory_space=pltpu.HBM)
        dma = pltpu.SemaphoreType.DMA
        fixed = functools.partial(pltpu.with_memory_space_constraint, memory_space=pltpu.HBM)
        back, base, tab = pl.pallas_call(
            functools.partial(cycle_kernel, nf, nc),
            out_shape=(
                jax.ShapeDtypeStruct((2 * nc - 2 * wide, window, rows), BF),
                jax.ShapeDtypeStruct((2 * rows, extent), F32),
                jax.ShapeDtypeStruct((nc * two, extent), BF),
            ),
            in_specs=[hbm] * 8,
            out_specs=(vmem, vmem, vmem),
            scratch_shapes=[
                pltpu.VMEM((2, rows, extent), BF),
                pltpu.VMEM((2, pc, vis), F32),
                pltpu.VMEM((2, pc, vis), jnp.int32),
                pltpu.SMEM((pc,), jnp.int32),
                pltpu.VMEM((pc, 2, two), F32),
                pltpu.VMEM((nf, 2, two), F32),
                pltpu.VMEM((pc * two, extent), BF),
                pltpu.VMEM((extent, pc * two), BF),
                pltpu.VMEM((two, pc * two), F32),
                pltpu.VMEM((window, extent), F32),
                pltpu.VMEM((nc, parts, window // 2, rows), BF),
                pltpu.VMEM((nc, parts, window // 2, rows), BF),
                pltpu.VMEM((parts * pc, 16, two), BF),
                pltpu.VMEM((parts * nf, 16, two), BF),
                pltpu.VMEM((2 * S, vis), BF),
                pltpu.VMEM((vis, 2 * S), BF),
                pltpu.VMEM((S // 16, vis), F32),
                pltpu.VMEM((S // 16, vis), F32),
                pltpu.VMEM((2, groups * two, vis), F32),
                pltpu.VMEM((groups * two, vis), F32),
                pltpu.VMEM((groups * two, vis), BF),
                pltpu.VMEM((2 * nf, window // 2, two), BF),
                pltpu.VMEM((2 * pc, window // 2, two), BF),
                pltpu.VMEM((2 * nc, window, rows), BF),
                pltpu.VMEM((2 * nc, window, rows), BF),
                pltpu.SemaphoreType.REGULAR((2,)),
                dma((11,)),
                dma((1,)), dma((3 * (nc - wide) + wide - 1,)), dma((1,)), dma((parts,)),
                dma((1,)), dma((4,)), dma((1,)), dma((3,)),
            ],
            compiler_params=pltpu.CompilerParams(
                collective_id=0, has_side_effects=True, vmem_limit_bytes=44 * 2**20
            ),
            name="cycle",
        )(
            fixed(facets), fixed(observed), fixed(uv_cells), fixed(counts),
            *(fixed(jnp.asarray(constant)) for constant in constants),
        )
        tile = 256
        return pl.pallas_call(
            functools.partial(image_kernel, nc),
            out_shape=jax.ShapeDtypeStruct((2, rows, extent), F32),
            in_specs=[vmem, vmem, vmem],
            out_specs=hbm,
            scratch_shapes=[
                pltpu.VMEM((extent // tile, 2, rows, tile), F32),
                dma((extent // tile,)),
            ],
            compiler_params=pltpu.CompilerParams(vmem_limit_bytes=16 * 2**20),
            name="image",
        )(back, base, tab)

    return jax.shard_map(
        on_device,
        mesh=mesh,
        in_specs=(
            P(None, ("facet", "col"), None),
            P(None, "col", None),
            P(None, "col", None),
            P("col"),
        ),
        out_specs=P(None, ("facet", "col"), None),
        check_vma=False,
    )
```

```python
import functools
import math

import jax
import jax.numpy as jnp
import numpy as np
from jax import lax
from jax.experimental import pallas as pl
from jax.experimental.pallas import tpu as pltpu
from jax.sharding import PartitionSpec as P

S = 512
IMAGE = 65536
MESH = pl.DeviceIdType.MESH
BF = jnp.bfloat16
F32 = jnp.float32
NT = (((1,), (1,)), ((), ()))


def unit(ticks):
    angle = (np.asarray(ticks, np.int64) % IMAGE) * (-2.0 * math.pi / IMAGE)
    return np.cos(angle), np.sin(angle)


def make_constants(facets, columns, per_column, extent):
    window = S // 8
    spacing = IMAGE // extent
    cells = np.arange(extent, dtype=np.int64)
    weight = (0.6 + 0.4 * np.sin(math.pi * (cells + 0.5) / extent) ** 2) / math.sqrt(extent)
    step = np.arange(window, dtype=np.int64)
    col = np.arange(columns, dtype=np.int64)
    vc = col * (IMAGE // 4) + (29 * col + 3) % spacing
    sub = np.arange(per_column, dtype=np.int64)
    us = sub * (IMAGE // 64) + (37 * sub + 5) % (IMAGE * 8 // S)

    def table(start, stride):
        real, imag = unit((start[:, None] + stride * step)[:, :, None] * cells)
        return np.stack([real * weight, imag * weight], axis=1).astype(np.float32).astype(BF)

    wide = 2 - columns % 2
    col_tab = table(vc, spacing).reshape(columns // wide, wide, 2, 2, window // 2, extent)
    col_tab = col_tab.transpose(0, 3, 1, 2, 4, 5).reshape(-1, extent)
    row_tab = table(us, IMAGE // window).reshape(-1, extent)
    assert extent % window == 0
    fy = extent * (np.arange(facets, dtype=np.int64) % 8)
    fx = extent * (np.arange(facets, dtype=np.int64) // 8)
    real, imag = unit((fy[:, None] * vc)[:, :, None] + (fx[:, None] * us)[:, None, :])
    same = np.stack([real, real], axis=-1)
    cross = np.stack([-imag, imag], axis=-1)
    turn = np.repeat(np.stack([same, cross], axis=3), window, axis=4)
    flat = np.ascontiguousarray
    return flat(col_tab), row_tab, flat(row_tab.T), turn.astype(np.float32)


def spin(value, first, second):
    half = value.shape[1] // 2
    lane = lax.broadcasted_iota(jnp.int32, value.shape, 1)
    return pltpu.roll(value, half, 1) * jnp.where(lane < half, first, second)


def sign(value, first, second):
    lane = lax.broadcasted_iota(jnp.int32, value.shape, 1)
    return value * jnp.where(lane < value.shape[1] // 2, first, second)


def series(square, first, terms):
    value = jnp.full_like(square, 1.0 / math.factorial(first + 2 * terms))
    for k in range(terms - 1, -1, -1):
        value = 1.0 / math.factorial(first + 2 * k) - value * square
    return value


def turns(ticks, whole):
    turn = ((ticks + whole // 2) & (whole - 1)) - whole // 2
    angle = turn.astype(F32) * (-math.pi / whole)
    square = angle * angle
    sine = angle * series(square, 1, 5)
    return 1.0 - 2.0 * sine * sine, 2.0 * sine * series(square, 0, 6)


def image_rows(blocks):
    half = blocks[0].shape[0] // 2
    cross = []
    for block in blocks:
        cross += [block[half:], -block[:half]]
    return jnp.concatenate(
        [jnp.concatenate(blocks, axis=0).T, jnp.concatenate(cross, axis=0).T], axis=0
    )


def cycle_kernel(
    nf, nc, x_hbm, obs_hbm, cells_hbm, counts_hbm, ctab_hbm, rtab_hbm, ttab_hbm, turn_hbm,
    back_out, base_out, tab,
    xbuf, obs, cells, counts, turn_in, turn_out, t2, tt, acc, bacc,
    s_send, s_recv, g_send, g_recv, right, right_t, r1r, r1i, left, inner, held,
    r_send, r_recv, b_send, b_recv,
    tok, in_sem, sa, ra, sb, rb, sc, rc, sd, rd,
):
    f = lax.axis_index("facet")
    c = lax.axis_index("col")
    window = S // 8
    half = window // 2
    two = 2 * window
    parts = window // 16
    pc = nf
    rows = xbuf.shape[1]
    groups = nf // 8
    vis = obs.shape[2]
    if nc % 2:
        col_steps = [(d, 0) for d in range(1, nc)]
        wide = 1
    else:
        col_steps = [(d, k) for d in range(nc // 2 - 1, -1, -1) for k in range(2) if d or k]
        wide = 2
    near_steps = [step for step in col_steps if step[0] == 0]
    far_steps = [step for step in col_steps if step[0]]

    def col_at(step, sign):
        if nc % 2:
            return lax.rem(c + nc + sign * step[0], nc)
        top = lax.rem(c // 2 + nc // 2 + sign * step[0], nc // 2)
        return 2 * top + lax.rem(c + step[1], 2)

    def pair_at(q):
        return lax.rem(f // 2 + q, 4)

    def group_of(q):
        return 0 if q in waits[0] else 1

    def facet_link(src_buf, dst_buf, send, recv, part, peer):
        return pltpu.make_async_remote_copy(
            src_buf.at[part * nf + peer], dst_buf.at[part * nf + f], send, recv, (peer, c), MESH
        )

    def col_link(src, dst, send, recv, peer):
        return pltpu.make_async_remote_copy(src, dst, send, recv, (f, peer), MESH)

    def sum_of(buf, start, count, send, recv):
        some = buf.at[start : start + count]
        return pltpu.make_async_remote_copy(some, some, send, recv, (mate, c), MESH)

    waits = ((0, 1), (3, 2))
    mate = f + 1 - 2 * lax.rem(f, 2)

    barrier = pltpu.get_barrier_semaphore()
    place, last_place = f // 2, nf // 2 - 1
    low, high = place > 0, place < last_place
    far_low, far_high = place > 1, place < last_place - 1

    def signal(sem, facet, col):
        pl.semaphore_signal(sem, inc=1, device_id=(facet, col), device_id_type=MESH)

    def pass_on(way):
        pl.semaphore_wait(tok.at[way], 1)
        signal(tok.at[way], f + 2 - 4 * way, c)

    for d in range(1, nc):
        signal(barrier, f, lax.rem(c + d, nc))
    signal(barrier, mate, c)

    @pl.when(high)
    def _():
        signal(barrier, f + 2, c)
        pl.when(~low)(lambda: signal(barrier, mate + 2, c))

    @pl.when(low)
    def _():
        signal(barrier, f - 2, c)
        pl.when(~high)(lambda: signal(barrier, mate - 2, c))


    n_groups = nc // wide
    chunk = wide * window

    def group_at(d):
        return lax.rem(c // wide + n_groups + d, n_groups)

    far_groups = list(range(n_groups - 1, 0, -1)) if wide == 2 else list(range(1, nc))

    extent = xbuf.shape[2]
    quarter = extent // 4
    depths = [slice(0, quarter), slice(quarter, 2 * quarter), slice(2 * quarter, 4 * quarter)]
    x_loads = [
        pltpu.make_async_copy(x_hbm.at[:, :, lanes], xbuf.at[:, :, lanes], in_sem.at[n])
        for n, lanes in enumerate(depths)
    ]
    mine_at = pl.ds(pl.multiple_of(group_at(0) * 2 * chunk, 2 * chunk), 2 * chunk)
    mine_load = pltpu.make_async_copy(ctab_hbm.at[mine_at], tab.at[mine_at], in_sem.at[3])
    row_load = pltpu.make_async_copy(rtab_hbm, t2, in_sem.at[9])
    small_loads = [
        pltpu.make_async_copy(turn_hbm.at[f, c], turn_in, in_sem.at[4]),
        pltpu.make_async_copy(turn_hbm.at[:, c, f], turn_out, in_sem.at[5]),
        pltpu.make_async_copy(obs_hbm, obs, in_sem.at[6]),
        pltpu.make_async_copy(cells_hbm, cells, in_sem.at[7]),
        pltpu.make_async_copy(counts_hbm, counts, in_sem.at[8]),
    ]
    turned_load = pltpu.make_async_copy(ttab_hbm, tt, in_sem.at[10])
    for load in x_loads:
        load.start()

    spacing = IMAGE // extent
    lr, li = turns(
        lax.broadcasted_iota(jnp.int32, (16, extent), 0)
        * lax.broadcasted_iota(jnp.int32, (16, extent), 1),
        extent,
    )
    high_rows = lax.broadcasted_iota(jnp.int32, (wide * parts, extent), 0)
    place_q = lax.broadcasted_iota(jnp.int32, (wide * parts, extent), 1)
    taper = 0.8 - 0.2 * turns(2 * place_q + 1, 2 * extent)[0]
    taper *= 1.0 / math.sqrt(extent)
    for d in far_groups:
        cols = wide * group_at(d) + high_rows // parts
        freqs = cols * (IMAGE // 4) + ((29 * cols + 3) & (spacing - 1))
        freqs += spacing * 16 * (high_rows & (parts - 1))
        hr, hi = turns(freqs * place_q, IMAGE)
        hr, hi = hr * taper, hi * taper
        for i in range(wide * parts):
            er, ei = hr[i : i + 1], hi[i : i + 1]
            k, u = i // parts, i % parts
            at = group_at(d) * 2 * chunk + u // 2 * chunk + k * window + u % 2 * 16
            at = pl.multiple_of(at, 16)
            tab[pl.ds(at, 16), :] = (lr * er - li * ei).astype(BF)
            tab[pl.ds(at + half, 16), :] = (lr * ei + li * er).astype(BF)

    def strip_term(d, lanes):
        at = pl.multiple_of(group_at(d) * 2 * chunk, 2 * chunk)
        return lax.dot_general(
            tab[pl.ds(at, 2 * chunk), lanes],
            xbuf[:, :, lanes].reshape(2 * rows, -1),
            NT,
            preferred_element_type=F32,
        )

    def strips(d, both):
        for k in range(wide):
            for part in range(parts):
                at = part // 2 * chunk + k * window + part % 2 * 16
                real, imag = both[at : at + 16], both[at + half : at + half + 16]
                block = [real[:, :rows] - imag[:, rows:], imag[:, :rows] + real[:, rows:]]
                s_send[wide * group_at(d) + k, part] = jnp.concatenate(block, axis=0).astype(BF)

    messages = [[0], [1], list(range(2, parts))]

    def strip_link(step, some):
        peer = col_at(step, 1)
        at = ra.at[messages.index(some) * len(far_steps) + far_steps.index(step)]
        some = slice(some[0], some[-1] + 1)
        return col_link(s_send.at[peer, some], s_recv.at[c, some], sa.at[0], at, peer)

    def near_link(step):
        peer = col_at(step, 1)
        at = ra.at[len(messages) * len(far_steps) + near_steps.index(step)]
        return col_link(s_send.at[peer], s_recv.at[c], sa.at[0], at, peer)

    sums = [0.0] * len(far_groups)
    for lanes, load in zip(depths, x_loads):
        load.wait()
        if lanes is depths[0]:
            mine_load.start()
            for load in small_loads:
                load.start()
        if lanes is depths[-1]:
            turned_load.start()
        for n, d in enumerate(far_groups):
            sums[n] += strip_term(d, lanes)
    for d, both in zip(far_groups, sums):
        strips(d, both)
    greeted = (low, high, place == 1, place == last_place - 1)
    pl.semaphore_wait(barrier, nc + sum(one.astype(jnp.int32) for one in greeted))
    for some in messages:
        for step in far_steps:
            strip_link(step, some).start()
    pl.when((place == 1) & high)(lambda: signal(tok.at[0], f + 2, c))
    pl.when((place == last_place - 1) & low)(lambda: signal(tok.at[1], f - 2, c))
    mine_load.wait()
    strips(0, strip_term(0, slice(None)))
    for step in near_steps:
        near_link(step).start()

    @pl.when(far_low & high)
    def _():
        pass_on(0)

    @pl.when(far_high & low)
    def _():
        pass_on(1)

    turned_load.wait()

    def window_term(block, src):
        at = pl.multiple_of(src * rows, rows)
        return jnp.dot(block, tt[pl.ds(at, rows), :], preferred_element_type=F32)

    acc[...] = window_term(s_send[c].reshape(two, rows), c)

    for load in small_loads:
        load.wait()

    def send_windows(some):
        def act(index):
            for part in some:
                facet_link(g_send, g_recv, sb.at[0], rb.at[part], part, index).start()

        for index in range(nf - 1, -1, -1):
            pl.when(index != f)(functools.partial(act, index))
        for part in some:
            g_recv[part * nf + f] = g_send[part * nf + f]

    first = cells[0, pl.ds(f, 1), :]
    second = cells[1, pl.ds(f, 1), :]

    def wave(count, step, cell):
        return turns(step * lax.broadcasted_iota(jnp.int32, (count, vis), 0) * cell, S)

    scale = 1.0 / math.sqrt(vis)
    live = lax.broadcasted_iota(jnp.int32, (1, vis), 1) < counts[f]
    gain = jnp.where(live, scale, 0.0)
    m0r, m0i = wave(16, 1, second)
    m0r, m0i = m0r * gain, m0i * gain
    r1r[...], r1i[...] = wave(S // 16, 16, second)

    def right_body(i, carry):
        er, ei = r1r[pl.ds(i, 1), :], r1i[pl.ds(i, 1), :]
        b = i // parts
        k = i - b * parts
        at = pl.multiple_of(k * (2 * S // parts) + b * half, 16)
        right[pl.ds(at, 16), :] = (m0r * er - m0i * ei).astype(BF)
        right[pl.ds(at + 16, 16), :] = (m0r * ei + m0i * er).astype(BF)
        return carry

    lax.fori_loop(0, S // 16, right_body, 0)

    for step in near_steps:
        near_link(step).wait_recv()
        src = col_at(step, -1)
        acc[...] += window_term(s_recv[src].reshape(two, rows), src)

    def windows(some):
        lo, hi = some[0], some[-1] + 1
        total = acc[lo * half : hi * half]
        for step in far_steps:
            strip_link(step, some).wait_recv()
            src = col_at(step, -1)
            block = s_recv[src, lo:hi].reshape((hi - lo) * half, rows)
            total += window_term(block, src)
        for part in some:
            at = (part - lo) * half
            for j in range(pc):
                u = total[at : at + 16, j * two : (j + 1) * two]
                v = total[at + 16 : at + half, j * two : (j + 1) * two]
                turn = turn_in[j]
                same, cross = turn[0:1], turn[1:2]
                win = u * same + spin(v, -1.0, 1.0) * same
                win += pltpu.roll(u, window, 1) * cross + v * sign(cross, 1.0, -1.0)
                g_send[part * pc + j] = win.astype(BF)
        if 0 in some:
            pl.when(far_high & ~low)(lambda: pl.semaphore_wait(tok.at[1], 1))
            pl.when(far_low & ~high)(lambda: pl.semaphore_wait(tok.at[0], 1))
        send_windows(some)

    windows(messages[0])

    windows(messages[1])
    windows(messages[2])
    row_load.start()

    l0r, l0i = wave(16, 1, first)
    l1r, l1i = wave(max(groups * parts, 8), 16, first)
    for i in range(groups * parts):
        er, ei = l1r[i : i + 1], l1i[i : i + 1]
        at = i // parts * two + i % parts * 16
        real = (l0r * er - l0i * ei).astype(BF).astype(F32)
        imag = (l0r * ei + l0i * er).astype(BF).astype(F32)
        left[0, at : at + 16, :] = real
        left[0, at + window : at + window + 16, :] = -imag
        left[1, at : at + 16, :] = imag
        left[1, at + window : at + window + 16, :] = real

    deep = 2 * S // parts

    def turn_body(b, carry):
        pieces = [right[pl.ds(pl.multiple_of(k * deep + b * half, 16), half), :] for k in range(parts)]
        at = pl.multiple_of(b * two, two)
        right_t[:, pl.ds(at, two)] = jnp.concatenate(pieces, axis=0).T
        return carry

    lax.fori_loop(0, S // window, turn_body, 0)

    def pred_term(some, g):
        blocks = []
        for part in some:
            for b in range(8):
                block = g_recv[part * nf + g * 8 + b].astype(F32)
                blocks += [block, spin(block, -1.0, 1.0)]
        return jnp.dot(
            jnp.concatenate(blocks, axis=0).T.astype(BF),
            right[some[0] * deep : (some[-1] + 1) * deep, :],
            preferred_element_type=F32,
        )

    def take_windows(some):
        for part in some:
            sum_of(g_recv, part * nf, nf - 1, sb.at[0], rb.at[part]).wait_recv()

    early_parts, late_parts = list(range(parts // 2)), list(range(parts // 2, parts))
    take_windows(early_parts)
    for g in range(groups):
        inner[g * two : (g + 1) * two] = pred_term(early_parts, g)

    take_windows(late_parts)
    res_r, res_i = obs[0, pl.ds(f, 1), :], obs[1, pl.ds(f, 1), :]
    for g in range(groups):
        at = slice(g * two, (g + 1) * two)
        value = inner[at] + pred_term(late_parts, g)
        unscale = 1.0 / (scale * S)
        res_r -= jnp.sum(value * left[0, at], axis=0, keepdims=True) * unscale
        res_i -= jnp.sum(value * left[1, at], axis=0, keepdims=True) * unscale
    held[...] = (res_r * left[0] + res_i * left[1]).astype(BF)

    def send_back(part, index):
        def act(group):
            recv = rc.at[2 * part + group]
            facet_link(r_send, r_recv, sc.at[0], recv, part, index).start()

        near = lax.rem(place - index // 2 + nf // 2, 4)
        pl.when((near < 2) & (index != f))(lambda: act(0))
        pl.when(near >= 2)(lambda: act(1))

    def grid_blocks(lo, hi):
        grid = jnp.dot(held[...], right_t[:, lo * two : hi * two], preferred_element_type=F32)
        for g in range(groups):
            block_t = grid[g * two : (g + 1) * two].T
            for b in range(lo, hi):
                turn = turn_out[g * 8 + b]
                same, cross = turn[0:1], turn[1:2]
                for part in range(2):
                    starts = [(b - lo) * two + (2 * part + k) * half for k in range(2)]
                    u = jnp.concatenate([block_t[at : at + 16] for at in starts], axis=0)
                    v = jnp.concatenate([block_t[at + 16 : at + half] for at in starts], axis=0)
                    block = (u + spin(v, 1.0, -1.0)) * same
                    block -= pltpu.roll(u, window, 1) * cross + v * sign(cross, -1.0, 1.0)
                    r_send[part * nf + g * 8 + b] = block.astype(BF)

    def send_backs(part, lo, hi):
        for g in range(groups):
            for b in range(lo, hi):
                send_back(part, g * 8 + b)

    grid_blocks(0, 2)
    send_backs(0, 0, 2)
    grid_blocks(5, 8)
    send_backs(1, 0, 2)
    for part in range(2):
        send_backs(part, 5, 8)
    grid_blocks(2, 5)
    for part in range(2):
        send_backs(part, 2, 5)
        r_recv[part * nf + f] = r_send[part * nf + f]

    row_load.wait()

    def take_backs(part, pairs):
        count = 4 * groups - (0 in pairs)
        at = rc.at[2 * part + waits.index(pairs)]
        sum_of(r_recv, part * nf, count, sc.at[0], at).wait_recv()

    def back_blocks(part, pairs):
        blocks = []
        for q in pairs:
            for g in range(groups):
                first = g * 8 + 2 * pair_at(q)
                pieces = [r_recv[part * nf + first + h] for h in range(2)]
                spun = [spin(piece.astype(F32), 1.0, -1.0).astype(BF) for piece in pieces]
                block = jnp.concatenate(
                    [jnp.concatenate(pieces, axis=1), jnp.concatenate(spun, axis=1)], axis=0
                )
                blocks.append((block, pl.multiple_of(first * two, 2 * two)))
        return blocks

    def lanes_of(d):
        return pl.ds(pl.multiple_of(wide * group_at(d) * rows, wide * rows), wide * rows)

    def back_term(blocks, d):
        return sum(
            jnp.dot(block, t2[pl.ds(at, 2 * two), lanes_of(d)], preferred_element_type=F32)
            for block, at in blocks
        )

    def keep(part, d, total):
        for k in range(wide):
            piece = total[:, k * rows : (k + 1) * rows]
            b_send[part * nc + wide * group_at(d) + k] = piece.astype(BF)

    def send_strips_back(part, d):
        for step in col_steps:
            if step[0] == d:
                peer = col_at(step, 1)
                at = rd.at[0 if step in near_steps else 1 + part]
                col_link(
                    b_send.at[part * nc + peer], b_recv.at[part * nc + c], sd.at[0], at, peer
                ).start()

    take_backs(0, waits[0])
    for d in far_groups:
        bacc[:, lanes_of(d)] = back_term(back_blocks(0, waits[0]), d)
    take_backs(0, waits[1])
    for d in far_groups:
        keep(0, d, bacc[:, lanes_of(d)] + back_term(back_blocks(0, waits[1]), d))
        send_strips_back(0, d)
    for pairs in waits:
        take_backs(1, pairs)
    for d in far_groups:
        keep(1, d, back_term(back_blocks(1, waits[0] + waits[1]), d))
        send_strips_back(1, d)
    both = [back_blocks(part, waits[0] + waits[1]) for part in range(2)]
    both = [(jnp.concatenate([one[0], two_[0]], axis=0), one[1]) for one, two_ in zip(*both)]
    total = back_term(both, 0)
    for part in range(2):
        keep(part, 0, total[part * window : (part + 1) * window])
        send_strips_back(part, 0)
        b_recv[part * nc + c] = b_send[part * nc + c]
    if near_steps:
        sum_of(b_recv, 0, 2 * len(near_steps), sd.at[0], rd.at[0]).wait_recv()
    mine = [b_recv[part * nc + wide * group_at(0) + k] for part in range(2) for k in range(wide)]
    base_out[...] = jnp.dot(
        image_rows(mine), tab[mine_at, :], preferred_element_type=F32
    )
    for part in range(2):
        sum_of(b_recv, 0, len(far_steps), sd.at[0], rd.at[1 + part]).wait_recv()
        for d in range(1, n_groups):
            for k in range(wide):
                at = part * nc + wide * group_at(d) + k
                back_out[((d - 1) * 2 + part) * wide + k] = b_recv[at]
    sum_of(s_send, 0, nc - 1, sa.at[0], ra.at[0]).wait_send()
    sum_of(b_send, 0, 2 * (nc - 1), sd.at[0], rd.at[0]).wait_send()
    sum_of(g_send, 0, parts * (nf - 1), sb.at[0], rb.at[0]).wait_send()
    sum_of(r_send, 0, 2 * (nf - 1), sc.at[0], rc.at[0]).wait_send()


def image_kernel(nc, back, base, tab, out, buf, sem):
    c = lax.axis_index("col")
    wide = 2 - nc % 2
    n_groups = nc // wide
    tiles, rows, tile = buf.shape[0], buf.shape[2], buf.shape[3]
    depth = 2 * wide * back.shape[1]
    strip = image_rows([back[k] for k in range(back.shape[0])])
    stores = []
    for t in range(tiles):
        lanes = slice(t * tile, (t + 1) * tile)
        piece = base[:, lanes]
        for d in range(1, n_groups):
            at = pl.multiple_of(lax.rem(c // wide + d, n_groups) * depth, depth)
            piece += jnp.dot(
                strip[:, (d - 1) * depth : d * depth],
                tab[pl.ds(at, depth), lanes],
                preferred_element_type=F32,
            )
        for part in range(2):
            buf[t, part] = piece[part * rows : (part + 1) * rows]
        store = pltpu.make_async_copy(buf.at[t], out.at[:, :, lanes], sem.at[t])
        store.start()
        stores.append(store)
    for store in stores:
        store.wait()


def solution(mesh):
    nf, nc = mesh.shape["facet"], mesh.shape["col"]

    def on_device(facets, observed, uv_cells, counts):
        rows, extent = facets.shape[1:]
        vis = observed.shape[2]
        pc = counts.shape[0]
        window = S // 8
        two = 2 * window
        groups = nf // 8
        wide = 2 - nc % 2
        parts = window // 16
        assert pc == nf and nf % 8 == 0 and nf <= 32 and nc > wide
        constants = make_constants(nf, nc, pc, extent)
        vmem = pl.BlockSpec(memory_space=pltpu.VMEM)
        hbm = pl.BlockSpec(memory_space=pltpu.HBM)
        dma = pltpu.SemaphoreType.DMA
        fixed = functools.partial(pltpu.with_memory_space_constraint, memory_space=pltpu.HBM)
        back, base, tab = pl.pallas_call(
            functools.partial(cycle_kernel, nf, nc),
            out_shape=(
                jax.ShapeDtypeStruct((2 * nc - 2 * wide, window, rows), BF),
                jax.ShapeDtypeStruct((2 * rows, extent), F32),
                jax.ShapeDtypeStruct((nc * two, extent), BF),
            ),
            in_specs=[hbm] * 8,
            out_specs=(vmem, vmem, vmem),
            scratch_shapes=[
                pltpu.VMEM((2, rows, extent), BF),
                pltpu.VMEM((2, pc, vis), F32),
                pltpu.VMEM((2, pc, vis), jnp.int32),
                pltpu.SMEM((pc,), jnp.int32),
                pltpu.VMEM((pc, 2, two), F32),
                pltpu.VMEM((nf, 2, two), F32),
                pltpu.VMEM((pc * two, extent), BF),
                pltpu.VMEM((extent, pc * two), BF),
                pltpu.VMEM((two, pc * two), F32),
                pltpu.VMEM((window, extent), F32),
                pltpu.VMEM((nc, parts, window // 2, rows), BF),
                pltpu.VMEM((nc, parts, window // 2, rows), BF),
                pltpu.VMEM((parts * pc, 16, two), BF),
                pltpu.VMEM((parts * nf, 16, two), BF),
                pltpu.VMEM((2 * S, vis), BF),
                pltpu.VMEM((vis, 2 * S), BF),
                pltpu.VMEM((S // 16, vis), F32),
                pltpu.VMEM((S // 16, vis), F32),
                pltpu.VMEM((2, groups * two, vis), F32),
                pltpu.VMEM((groups * two, vis), F32),
                pltpu.VMEM((groups * two, vis), BF),
                pltpu.VMEM((2 * nf, window // 2, two), BF),
                pltpu.VMEM((2 * pc, window // 2, two), BF),
                pltpu.VMEM((2 * nc, window, rows), BF),
                pltpu.VMEM((2 * nc, window, rows), BF),
                pltpu.SemaphoreType.REGULAR((2,)),
                dma((11,)),
                dma((1,)), dma((3 * (nc - wide) + wide - 1,)), dma((1,)), dma((parts,)),
                dma((1,)), dma((4,)), dma((1,)), dma((3,)),
            ],
            compiler_params=pltpu.CompilerParams(
                collective_id=0, has_side_effects=True, vmem_limit_bytes=44 * 2**20
            ),
            name="cycle",
        )(
            fixed(facets), fixed(observed), fixed(uv_cells), fixed(counts),
            *(fixed(jnp.asarray(constant)) for constant in constants),
        )
        tile = 256
        return pl.pallas_call(
            functools.partial(image_kernel, nc),
            out_shape=jax.ShapeDtypeStruct((2, rows, extent), F32),
            in_specs=[vmem, vmem, vmem],
            out_specs=hbm,
            scratch_shapes=[
                pltpu.VMEM((extent // tile, 2, rows, tile), F32),
                dma((extent // tile,)),
            ],
            compiler_params=pltpu.CompilerParams(vmem_limit_bytes=16 * 2**20),
            name="image",
        )(back, base, tab)

    return jax.shard_map(
        on_device,
        mesh=mesh,
        in_specs=(
            P(None, ("facet", "col"), None),
            P(None, "col", None),
            P(None, "col", None),
            P("col"),
        ),
        out_specs=P(None, ("facet", "col"), None),
        check_vma=False,
    )
```

```python
import functools
import math

import jax
import jax.numpy as jnp
import numpy as np
from jax import lax
from jax.experimental import pallas as pl
from jax.experimental.pallas import tpu as pltpu
from jax.sharding import PartitionSpec as P

S = 512
IMAGE = 65536
MESH = pl.DeviceIdType.MESH
BF = jnp.bfloat16
F32 = jnp.float32
NT = (((1,), (1,)), ((), ()))


def unit(ticks):
    angle = (np.asarray(ticks, np.int64) % IMAGE) * (-2.0 * math.pi / IMAGE)
    return np.cos(angle), np.sin(angle)


def make_constants(facets, columns, per_column, extent):
    window = S // 8
    spacing = IMAGE // extent
    cells = np.arange(extent, dtype=np.int64)
    weight = (0.6 + 0.4 * np.sin(math.pi * (cells + 0.5) / extent) ** 2) / math.sqrt(extent)
    step = np.arange(window, dtype=np.int64)
    col = np.arange(columns, dtype=np.int64)
    vc = col * (IMAGE // 4) + (29 * col + 3) % spacing
    sub = np.arange(per_column, dtype=np.int64)
    us = sub * (IMAGE // 64) + (37 * sub + 5) % (IMAGE * 8 // S)

    def table(start, stride):
        real, imag = unit((start[:, None] + stride * step)[:, :, None] * cells)
        return np.stack([real * weight, imag * weight], axis=1).astype(np.float32).astype(BF)

    wide = 2 - columns % 2
    col_tab = table(vc, spacing).reshape(columns // wide, wide, 2, 2, window // 2, extent)
    col_tab = col_tab.transpose(0, 3, 1, 2, 4, 5).reshape(-1, extent)
    row_tab = table(us, IMAGE // window).reshape(-1, extent)
    assert extent % window == 0
    fy = extent * (np.arange(facets, dtype=np.int64) % 8)
    fx = extent * (np.arange(facets, dtype=np.int64) // 8)
    real, imag = unit((fy[:, None] * vc)[:, :, None] + (fx[:, None] * us)[:, None, :])
    same = np.stack([real, real], axis=-1)
    cross = np.stack([-imag, imag], axis=-1)
    turn = np.repeat(np.stack([same, cross], axis=3), window, axis=4)
    flat = np.ascontiguousarray
    return flat(col_tab), row_tab, flat(row_tab.T), turn.astype(np.float32)


def spin(value, first, second):
    half = value.shape[1] // 2
    lane = lax.broadcasted_iota(jnp.int32, value.shape, 1)
    return pltpu.roll(value, half, 1) * jnp.where(lane < half, first, second)


def sign(value, first, second):
    lane = lax.broadcasted_iota(jnp.int32, value.shape, 1)
    return value * jnp.where(lane < value.shape[1] // 2, first, second)


def series(square, first, terms):
    value = jnp.full_like(square, 1.0 / math.factorial(first + 2 * terms))
    for k in range(terms - 1, -1, -1):
        value = 1.0 / math.factorial(first + 2 * k) - value * square
    return value


def turns(ticks, whole):
    turn = ((ticks + whole // 2) & (whole - 1)) - whole // 2
    angle = turn.astype(F32) * (-math.pi / whole)
    square = angle * angle
    sine = angle * series(square, 1, 5)
    return 1.0 - 2.0 * sine * sine, 2.0 * sine * series(square, 0, 6)


def image_rows(blocks):
    half = blocks[0].shape[0] // 2
    cross = []
    for block in blocks:
        cross += [block[half:], -block[:half]]
    return jnp.concatenate(
        [jnp.concatenate(blocks, axis=0).T, jnp.concatenate(cross, axis=0).T], axis=0
    )


def cycle_kernel(
    nf, nc, x_hbm, obs_hbm, cells_hbm, counts_hbm, ctab_hbm, rtab_hbm, ttab_hbm, turn_hbm,
    back_out, base_out, tab,
    xbuf, obs, cells, counts, turn_in, turn_out, t2, tt, acc, bacc,
    s_send, s_recv, g_send, g_recv, right, right_t, r1r, r1i, left, inner, held,
    r_send, r_recv, b_send, b_recv,
    tok, in_sem, sa, ra, sb, rb, sc, rc, sd, rd,
):
    f = lax.axis_index("facet")
    c = lax.axis_index("col")
    window = S // 8
    half = window // 2
    two = 2 * window
    parts = window // 16
    pc = nf
    rows = xbuf.shape[1]
    groups = nf // 8
    vis = obs.shape[2]
    if nc % 2:
        col_steps = [(d, 0) for d in range(1, nc)]
        wide = 1
    else:
        col_steps = [(d, k) for d in range(nc // 2 - 1, -1, -1) for k in range(2) if d or k]
        wide = 2
    near_steps = [step for step in col_steps if step[0] == 0]
    far_steps = [step for step in col_steps if step[0]]

    def col_at(step, sign):
        if nc % 2:
            return lax.rem(c + nc + sign * step[0], nc)
        top = lax.rem(c // 2 + nc // 2 + sign * step[0], nc // 2)
        return 2 * top + lax.rem(c + step[1], 2)

    def pair_at(q):
        return lax.rem(f // 2 + q, 4)

    def group_of(q):
        return 0 if q in waits[0] else 1

    def facet_link(src_buf, dst_buf, send, recv, part, peer):
        return pltpu.make_async_remote_copy(
            src_buf.at[part * nf + peer], dst_buf.at[part * nf + f], send, recv, (peer, c), MESH
        )

    def col_link(src, dst, send, recv, peer):
        return pltpu.make_async_remote_copy(src, dst, send, recv, (f, peer), MESH)

    def sum_of(buf, start, count, send, recv):
        some = buf.at[start : start + count]
        return pltpu.make_async_remote_copy(some, some, send, recv, (mate, c), MESH)

    waits = ((0, 1), (3, 2))
    mate = f + 1 - 2 * lax.rem(f, 2)

    barrier = pltpu.get_barrier_semaphore()
    place, last_place = f // 2, nf // 2 - 1
    low, high = place > 0, place < last_place
    far_low, far_high = place > 1, place < last_place - 1

    def signal(sem, facet, col):
        pl.semaphore_signal(sem, inc=1, device_id=(facet, col), device_id_type=MESH)

    def pass_on(way):
        pl.semaphore_wait(tok.at[way], 1)
        signal(tok.at[way], f + 2 - 4 * way, c)

    for d in range(1, nc):
        signal(barrier, f, lax.rem(c + d, nc))
    signal(barrier, mate, c)

    @pl.when(high)
    def _():
        signal(barrier, f + 2, c)
        pl.when(~low)(lambda: signal(barrier, mate + 2, c))

    @pl.when(low)
    def _():
        signal(barrier, f - 2, c)
        pl.when(~high)(lambda: signal(barrier, mate - 2, c))


    n_groups = nc // wide
    chunk = wide * window

    def group_at(d):
        return lax.rem(c // wide + n_groups + d, n_groups)

    far_groups = list(range(n_groups - 1, 0, -1)) if wide == 2 else list(range(1, nc))

    extent = xbuf.shape[2]
    quarter = extent // 4
    depths = [slice(0, quarter), slice(quarter, 2 * quarter), slice(2 * quarter, 4 * quarter)]
    x_loads = [
        pltpu.make_async_copy(x_hbm.at[:, :, lanes], xbuf.at[:, :, lanes], in_sem.at[n])
        for n, lanes in enumerate(depths)
    ]
    mine_at = pl.ds(pl.multiple_of(group_at(0) * 2 * chunk, 2 * chunk), 2 * chunk)
    mine_load = pltpu.make_async_copy(ctab_hbm.at[mine_at], tab.at[mine_at], in_sem.at[3])
    row_load = pltpu.make_async_copy(rtab_hbm, t2, in_sem.at[9])
    small_loads = [
        pltpu.make_async_copy(turn_hbm.at[f, c], turn_in, in_sem.at[4]),
        pltpu.make_async_copy(turn_hbm.at[:, c, f], turn_out, in_sem.at[5]),
        pltpu.make_async_copy(obs_hbm, obs, in_sem.at[6]),
        pltpu.make_async_copy(cells_hbm, cells, in_sem.at[7]),
        pltpu.make_async_copy(counts_hbm, counts, in_sem.at[8]),
    ]
    turned_load = pltpu.make_async_copy(ttab_hbm, tt, in_sem.at[10])
    for load in x_loads:
        load.start()

    spacing = IMAGE // extent
    lr, li = turns(
        lax.broadcasted_iota(jnp.int32, (16, extent), 0)
        * lax.broadcasted_iota(jnp.int32, (16, extent), 1),
        extent,
    )
    high_rows = lax.broadcasted_iota(jnp.int32, (wide * parts, extent), 0)
    place_q = lax.broadcasted_iota(jnp.int32, (wide * parts, extent), 1)
    taper = 0.8 - 0.2 * turns(2 * place_q + 1, 2 * extent)[0]
    taper *= 1.0 / math.sqrt(extent)
    for d in far_groups:
        cols = wide * group_at(d) + high_rows // parts
        freqs = cols * (IMAGE // 4) + ((29 * cols + 3) & (spacing - 1))
        freqs += spacing * 16 * (high_rows & (parts - 1))
        hr, hi = turns(freqs * place_q, IMAGE)
        hr, hi = hr * taper, hi * taper
        for i in range(wide * parts):
            er, ei = hr[i : i + 1], hi[i : i + 1]
            k, u = i // parts, i % parts
            at = group_at(d) * 2 * chunk + u // 2 * chunk + k * window + u % 2 * 16
            at = pl.multiple_of(at, 16)
            tab[pl.ds(at, 16), :] = (lr * er - li * ei).astype(BF)
            tab[pl.ds(at + half, 16), :] = (lr * ei + li * er).astype(BF)

    def strip_term(d, lanes):
        at = pl.multiple_of(group_at(d) * 2 * chunk, 2 * chunk)
        return lax.dot_general(
            tab[pl.ds(at, 2 * chunk), lanes],
            xbuf[:, :, lanes].reshape(2 * rows, -1),
            NT,
            preferred_element_type=F32,
        )

    def strips(d, both):
        for k in range(wide):
            for part in range(parts):
                at = part // 2 * chunk + k * window + part % 2 * 16
                real, imag = both[at : at + 16], both[at + half : at + half + 16]
                block = [real[:, :rows] - imag[:, rows:], imag[:, :rows] + real[:, rows:]]
                s_send[wide * group_at(d) + k, part] = jnp.concatenate(block, axis=0).astype(BF)

    messages = [[0], [1], list(range(2, parts))]

    def strip_link(step, some):
        peer = col_at(step, 1)
        at = ra.at[messages.index(some) * len(far_steps) + far_steps.index(step)]
        some = slice(some[0], some[-1] + 1)
        return col_link(s_send.at[peer, some], s_recv.at[c, some], sa.at[0], at, peer)

    def near_link(step):
        peer = col_at(step, 1)
        at = ra.at[len(messages) * len(far_steps) + near_steps.index(step)]
        return col_link(s_send.at[peer], s_recv.at[c], sa.at[0], at, peer)

    sums = [0.0] * len(far_groups)
    for lanes, load in zip(depths, x_loads):
        load.wait()
        if lanes is depths[0]:
            mine_load.start()
            for load in small_loads:
                load.start()
        if lanes is depths[-1]:
            turned_load.start()
        for n, d in enumerate(far_groups):
            sums[n] += strip_term(d, lanes)
    for d, both in zip(far_groups, sums):
        strips(d, both)
    greeted = (low, high, place == 1, place == last_place - 1)
    pl.semaphore_wait(barrier, nc + sum(one.astype(jnp.int32) for one in greeted))
    for some in messages:
        for step in far_steps:
            strip_link(step, some).start()
    pl.when((place == 1) & high)(lambda: signal(tok.at[0], f + 2, c))
    pl.when((place == last_place - 1) & low)(lambda: signal(tok.at[1], f - 2, c))
    mine_load.wait()
    strips(0, strip_term(0, slice(None)))
    for step in near_steps:
        near_link(step).start()

    @pl.when(far_low & high)
    def _():
        pass_on(0)

    @pl.when(far_high & low)
    def _():
        pass_on(1)

    turned_load.wait()

    def window_term(block, src):
        at = pl.multiple_of(src * rows, rows)
        return jnp.dot(block, tt[pl.ds(at, rows), :], preferred_element_type=F32)

    acc[...] = window_term(s_send[c].reshape(two, rows), c)

    for load in small_loads:
        load.wait()

    def send_windows(some):
        def act(index):
            for part in some:
                facet_link(g_send, g_recv, sb.at[0], rb.at[part], part, index).start()

        for index in range(nf - 1, -1, -1):
            pl.when(index != f)(functools.partial(act, index))
        for part in some:
            g_recv[part * nf + f] = g_send[part * nf + f]

    first = cells[0, pl.ds(f, 1), :]
    second = cells[1, pl.ds(f, 1), :]

    def wave(count, step, cell):
        return turns(step * lax.broadcasted_iota(jnp.int32, (count, vis), 0) * cell, S)

    scale = 1.0 / math.sqrt(vis)
    live = lax.broadcasted_iota(jnp.int32, (1, vis), 1) < counts[f]
    gain = jnp.where(live, scale, 0.0)
    m0r, m0i = wave(16, 1, second)
    m0r, m0i = m0r * gain, m0i * gain
    r1r[...], r1i[...] = wave(S // 16, 16, second)

    def right_body(i, carry):
        er, ei = r1r[pl.ds(i, 1), :], r1i[pl.ds(i, 1), :]
        b = i // parts
        k = i - b * parts
        at = pl.multiple_of(k * (2 * S // parts) + b * half, 16)
        right[pl.ds(at, 16), :] = (m0r * er - m0i * ei).astype(BF)
        right[pl.ds(at + 16, 16), :] = (m0r * ei + m0i * er).astype(BF)
        return carry

    lax.fori_loop(0, S // 16, right_body, 0)

    for step in near_steps:
        near_link(step).wait_recv()
        src = col_at(step, -1)
        acc[...] += window_term(s_recv[src].reshape(two, rows), src)

    def windows(some):
        lo, hi = some[0], some[-1] + 1
        total = acc[lo * half : hi * half]
        for step in far_steps:
            strip_link(step, some).wait_recv()
            src = col_at(step, -1)
            block = s_recv[src, lo:hi].reshape((hi - lo) * half, rows)
            total += window_term(block, src)
        for part in some:
            at = (part - lo) * half
            for j in range(pc):
                u = total[at : at + 16, j * two : (j + 1) * two]
                v = total[at + 16 : at + half, j * two : (j + 1) * two]
                turn = turn_in[j]
                same, cross = turn[0:1], turn[1:2]
                win = u * same + spin(v, -1.0, 1.0) * same
                win += pltpu.roll(u, window, 1) * cross + v * sign(cross, 1.0, -1.0)
                g_send[part * pc + j] = win.astype(BF)
        if 0 in some:
            pl.when(far_high & ~low)(lambda: pl.semaphore_wait(tok.at[1], 1))
            pl.when(far_low & ~high)(lambda: pl.semaphore_wait(tok.at[0], 1))
        send_windows(some)

    windows(messages[0])

    windows(messages[1])
    windows(messages[2])
    row_load.start()

    l0r, l0i = wave(16, 1, first)
    l1r, l1i = wave(max(groups * parts, 8), 16, first)
    for i in range(groups * parts):
        er, ei = l1r[i : i + 1], l1i[i : i + 1]
        at = i // parts * two + i % parts * 16
        real = (l0r * er - l0i * ei).astype(BF).astype(F32)
        imag = (l0r * ei + l0i * er).astype(BF).astype(F32)
        left[0, at : at + 16, :] = real
        left[0, at + window : at + window + 16, :] = -imag
        left[1, at : at + 16, :] = imag
        left[1, at + window : at + window + 16, :] = real

    deep = 2 * S // parts

    def turn_body(b, carry):
        pieces = [right[pl.ds(pl.multiple_of(k * deep + b * half, 16), half), :] for k in range(parts)]
        at = pl.multiple_of(b * two, two)
        right_t[:, pl.ds(at, two)] = jnp.concatenate(pieces, axis=0).T
        return carry

    lax.fori_loop(0, S // window, turn_body, 0)

    def pred_term(some, g):
        blocks = []
        for part in some:
            for b in range(8):
                block = g_recv[part * nf + g * 8 + b].astype(F32)
                blocks += [block, spin(block, -1.0, 1.0)]
        return jnp.dot(
            jnp.concatenate(blocks, axis=0).T.astype(BF),
            right[some[0] * deep : (some[-1] + 1) * deep, :],
            preferred_element_type=F32,
        )

    def take_windows(some):
        for part in some:
            sum_of(g_recv, part * nf, nf - 1, sb.at[0], rb.at[part]).wait_recv()

    early_parts, late_parts = list(range(parts // 2)), list(range(parts // 2, parts))
    take_windows(early_parts)
    for g in range(groups):
        inner[g * two : (g + 1) * two] = pred_term(early_parts, g)

    take_windows(late_parts)
    res_r, res_i = obs[0, pl.ds(f, 1), :], obs[1, pl.ds(f, 1), :]
    for g in range(groups):
        at = slice(g * two, (g + 1) * two)
        value = inner[at] + pred_term(late_parts, g)
        unscale = 1.0 / (scale * S)
        res_r -= jnp.sum(value * left[0, at], axis=0, keepdims=True) * unscale
        res_i -= jnp.sum(value * left[1, at], axis=0, keepdims=True) * unscale
    held[...] = (res_r * left[0] + res_i * left[1]).astype(BF)

    def send_back(part, index):
        def act(group):
            recv = rc.at[2 * part + group]
            facet_link(r_send, r_recv, sc.at[0], recv, part, index).start()

        near = lax.rem(place - index // 2 + nf // 2, 4)
        pl.when((near < 2) & (index != f))(lambda: act(0))
        pl.when(near >= 2)(lambda: act(1))

    def grid_blocks(lo, hi, after=None):
        grid = jnp.dot(held[...], right_t[:, lo * two : hi * two], preferred_element_type=F32)
        turned = [grid[g * two : (g + 1) * two].T for g in range(groups)]
        for part in range(2):
            for g in range(groups):
                for b in range(lo, hi):
                    turn = turn_out[g * 8 + b]
                    same, cross = turn[0:1], turn[1:2]
                    starts = [(b - lo) * two + (2 * part + k) * half for k in range(2)]
                    u, v = (
                        jnp.concatenate([turned[g][at + k : at + k + 16] for at in starts], axis=0)
                        for k in (0, 16)
                    )
                    block = (u + spin(v, 1.0, -1.0)) * same
                    block -= pltpu.roll(u, window, 1) * cross + v * sign(cross, -1.0, 1.0)
                    r_send[part * nf + g * 8 + b] = block.astype(BF)
            if after is not None and part == 0:
                after()

    def send_backs(part, lo, hi):
        for g in range(groups):
            for b in range(lo, hi):
                send_back(part, g * 8 + b)

    grid_blocks(0, 2, lambda: send_backs(0, 0, 2))
    grid_blocks(5, 8)
    send_backs(1, 0, 2)
    for part in range(2):
        send_backs(part, 5, 8)
    grid_blocks(2, 5)
    for part in range(2):
        send_backs(part, 2, 5)
        r_recv[part * nf + f] = r_send[part * nf + f]

    row_load.wait()

    def take_backs(part, pairs):
        count = 4 * groups - (0 in pairs)
        at = rc.at[2 * part + waits.index(pairs)]
        sum_of(r_recv, part * nf, count, sc.at[0], at).wait_recv()

    def back_blocks(part, pairs):
        blocks = []
        for q in pairs:
            for g in range(groups):
                first = g * 8 + 2 * pair_at(q)
                pieces = [r_recv[part * nf + first + h] for h in range(2)]
                spun = [spin(piece.astype(F32), 1.0, -1.0).astype(BF) for piece in pieces]
                block = jnp.concatenate(
                    [jnp.concatenate(pieces, axis=1), jnp.concatenate(spun, axis=1)], axis=0
                )
                blocks.append((block, pl.multiple_of(first * two, 2 * two)))
        return blocks

    def lanes_of(d):
        return pl.ds(pl.multiple_of(wide * group_at(d) * rows, wide * rows), wide * rows)

    def back_term(blocks, d):
        return sum(
            jnp.dot(block, t2[pl.ds(at, 2 * two), lanes_of(d)], preferred_element_type=F32)
            for block, at in blocks
        )

    def keep(part, d, total):
        for k in range(wide):
            piece = total[:, k * rows : (k + 1) * rows]
            b_send[part * nc + wide * group_at(d) + k] = piece.astype(BF)

    def send_strips_back(part, d):
        for step in col_steps:
            if step[0] == d:
                peer = col_at(step, 1)
                at = rd.at[0 if step in near_steps else 1 + part]
                col_link(
                    b_send.at[part * nc + peer], b_recv.at[part * nc + c], sd.at[0], at, peer
                ).start()

    take_backs(0, waits[0])
    for d in far_groups:
        bacc[:, lanes_of(d)] = back_term(back_blocks(0, waits[0]), d)
    take_backs(0, waits[1])
    for d in far_groups:
        keep(0, d, bacc[:, lanes_of(d)] + back_term(back_blocks(0, waits[1]), d))
        send_strips_back(0, d)
    for pairs in waits:
        take_backs(1, pairs)
    for d in far_groups:
        keep(1, d, back_term(back_blocks(1, waits[0] + waits[1]), d))
        send_strips_back(1, d)
    both = [back_blocks(part, waits[0] + waits[1]) for part in range(2)]
    both = [(jnp.concatenate([one[0], two_[0]], axis=0), one[1]) for one, two_ in zip(*both)]
    total = back_term(both, 0)
    for part in range(2):
        keep(part, 0, total[part * window : (part + 1) * window])
        send_strips_back(part, 0)
        b_recv[part * nc + c] = b_send[part * nc + c]
    if near_steps:
        sum_of(b_recv, 0, 2 * len(near_steps), sd.at[0], rd.at[0]).wait_recv()
    mine = [b_recv[part * nc + wide * group_at(0) + k] for part in range(2) for k in range(wide)]
    base_out[...] = jnp.dot(
        image_rows(mine), tab[mine_at, :], preferred_element_type=F32
    )
    for part in range(2):
        sum_of(b_recv, 0, len(far_steps), sd.at[0], rd.at[1 + part]).wait_recv()
        for d in range(1, n_groups):
            for k in range(wide):
                at = part * nc + wide * group_at(d) + k
                back_out[((d - 1) * 2 + part) * wide + k] = b_recv[at]
    sum_of(s_send, 0, nc - 1, sa.at[0], ra.at[0]).wait_send()
    sum_of(b_send, 0, 2 * (nc - 1), sd.at[0], rd.at[0]).wait_send()
    sum_of(g_send, 0, parts * (nf - 1), sb.at[0], rb.at[0]).wait_send()
    sum_of(r_send, 0, 2 * (nf - 1), sc.at[0], rc.at[0]).wait_send()


def image_kernel(nc, back, base, tab, out, buf, sem):
    c = lax.axis_index("col")
    wide = 2 - nc % 2
    n_groups = nc // wide
    tiles, rows, tile = buf.shape[0], buf.shape[2], buf.shape[3]
    depth = 2 * wide * back.shape[1]
    strip = image_rows([back[k] for k in range(back.shape[0])])
    stores = []
    for t in range(tiles):
        lanes = slice(t * tile, (t + 1) * tile)
        piece = base[:, lanes]
        for d in range(1, n_groups):
            at = pl.multiple_of(lax.rem(c // wide + d, n_groups) * depth, depth)
            piece += jnp.dot(
                strip[:, (d - 1) * depth : d * depth],
                tab[pl.ds(at, depth), lanes],
                preferred_element_type=F32,
            )
        for part in range(2):
            buf[t, part] = piece[part * rows : (part + 1) * rows]
        store = pltpu.make_async_copy(buf.at[t], out.at[:, :, lanes], sem.at[t])
        store.start()
        stores.append(store)
    for store in stores:
        store.wait()


def solution(mesh):
    nf, nc = mesh.shape["facet"], mesh.shape["col"]

    def on_device(facets, observed, uv_cells, counts):
        rows, extent = facets.shape[1:]
        vis = observed.shape[2]
        pc = counts.shape[0]
        window = S // 8
        two = 2 * window
        groups = nf // 8
        wide = 2 - nc % 2
        parts = window // 16
        assert pc == nf and nf % 8 == 0 and nf <= 32 and nc > wide
        constants = make_constants(nf, nc, pc, extent)
        vmem = pl.BlockSpec(memory_space=pltpu.VMEM)
        hbm = pl.BlockSpec(memory_space=pltpu.HBM)
        dma = pltpu.SemaphoreType.DMA
        fixed = functools.partial(pltpu.with_memory_space_constraint, memory_space=pltpu.HBM)
        back, base, tab = pl.pallas_call(
            functools.partial(cycle_kernel, nf, nc),
            out_shape=(
                jax.ShapeDtypeStruct((2 * nc - 2 * wide, window, rows), BF),
                jax.ShapeDtypeStruct((2 * rows, extent), F32),
                jax.ShapeDtypeStruct((nc * two, extent), BF),
            ),
            in_specs=[hbm] * 8,
            out_specs=(vmem, vmem, vmem),
            scratch_shapes=[
                pltpu.VMEM((2, rows, extent), BF),
                pltpu.VMEM((2, pc, vis), F32),
                pltpu.VMEM((2, pc, vis), jnp.int32),
                pltpu.SMEM((pc,), jnp.int32),
                pltpu.VMEM((pc, 2, two), F32),
                pltpu.VMEM((nf, 2, two), F32),
                pltpu.VMEM((pc * two, extent), BF),
                pltpu.VMEM((extent, pc * two), BF),
                pltpu.VMEM((two, pc * two), F32),
                pltpu.VMEM((window, extent), F32),
                pltpu.VMEM((nc, parts, window // 2, rows), BF),
                pltpu.VMEM((nc, parts, window // 2, rows), BF),
                pltpu.VMEM((parts * pc, 16, two), BF),
                pltpu.VMEM((parts * nf, 16, two), BF),
                pltpu.VMEM((2 * S, vis), BF),
                pltpu.VMEM((vis, 2 * S), BF),
                pltpu.VMEM((S // 16, vis), F32),
                pltpu.VMEM((S // 16, vis), F32),
                pltpu.VMEM((2, groups * two, vis), F32),
                pltpu.VMEM((groups * two, vis), F32),
                pltpu.VMEM((groups * two, vis), BF),
                pltpu.VMEM((2 * nf, window // 2, two), BF),
                pltpu.VMEM((2 * pc, window // 2, two), BF),
                pltpu.VMEM((2 * nc, window, rows), BF),
                pltpu.VMEM((2 * nc, window, rows), BF),
                pltpu.SemaphoreType.REGULAR((2,)),
                dma((11,)),
                dma((1,)), dma((3 * (nc - wide) + wide - 1,)), dma((1,)), dma((parts,)),
                dma((1,)), dma((4,)), dma((1,)), dma((3,)),
            ],
            compiler_params=pltpu.CompilerParams(
                collective_id=0, has_side_effects=True, vmem_limit_bytes=44 * 2**20
            ),
            name="cycle",
        )(
            fixed(facets), fixed(observed), fixed(uv_cells), fixed(counts),
            *(fixed(jnp.asarray(constant)) for constant in constants),
        )
        tile = 256
        return pl.pallas_call(
            functools.partial(image_kernel, nc),
            out_shape=jax.ShapeDtypeStruct((2, rows, extent), F32),
            in_specs=[vmem, vmem, vmem],
            out_specs=hbm,
            scratch_shapes=[
                pltpu.VMEM((extent // tile, 2, rows, tile), F32),
                dma((extent // tile,)),
            ],
            compiler_params=pltpu.CompilerParams(vmem_limit_bytes=16 * 2**20),
            name="image",
        )(back, base, tab)

    return jax.shard_map(
        on_device,
        mesh=mesh,
        in_specs=(
            P(None, ("facet", "col"), None),
            P(None, "col", None),
            P(None, "col", None),
            P("col"),
        ),
        out_specs=P(None, ("facet", "col"), None),
        check_vma=False,
    )
```

```python
import functools
import math

import jax
import jax.numpy as jnp
import numpy as np
from jax import lax
from jax.experimental import pallas as pl
from jax.experimental.pallas import tpu as pltpu
from jax.sharding import PartitionSpec as P

S = 512
IMAGE = 65536
MESH = pl.DeviceIdType.MESH
BF = jnp.bfloat16
F32 = jnp.float32
NT = (((1,), (1,)), ((), ()))


def unit(ticks):
    angle = (np.asarray(ticks, np.int64) % IMAGE) * (-2.0 * math.pi / IMAGE)
    return np.cos(angle), np.sin(angle)


def make_constants(facets, columns, per_column, extent):
    window = S // 8
    spacing = IMAGE // extent
    cells = np.arange(extent, dtype=np.int64)
    weight = (0.6 + 0.4 * np.sin(math.pi * (cells + 0.5) / extent) ** 2) / math.sqrt(extent)
    step = np.arange(window, dtype=np.int64)
    col = np.arange(columns, dtype=np.int64)
    vc = col * (IMAGE // 4) + (29 * col + 3) % spacing
    sub = np.arange(per_column, dtype=np.int64)
    us = sub * (IMAGE // 64) + (37 * sub + 5) % (IMAGE * 8 // S)

    def table(start, stride):
        real, imag = unit((start[:, None] + stride * step)[:, :, None] * cells)
        return np.stack([real * weight, imag * weight], axis=1).astype(np.float32).astype(BF)

    wide = 2 - columns % 2
    col_tab = table(vc, spacing).reshape(columns // wide, wide, 2, 2, window // 2, extent)
    col_tab = col_tab.transpose(0, 3, 1, 2, 4, 5).reshape(-1, extent)
    row_tab = table(us, IMAGE // window).reshape(-1, extent)
    assert extent % window == 0
    fy = extent * (np.arange(facets, dtype=np.int64) % 8)
    fx = extent * (np.arange(facets, dtype=np.int64) // 8)
    real, imag = unit((fy[:, None] * vc)[:, :, None] + (fx[:, None] * us)[:, None, :])
    same = np.stack([real, real], axis=-1)
    cross = np.stack([-imag, imag], axis=-1)
    turn = np.repeat(np.stack([same, cross], axis=3), window, axis=4)
    flat = np.ascontiguousarray
    return flat(col_tab), row_tab, flat(row_tab.T), turn.astype(np.float32)


def spin(value, first, second):
    half = value.shape[1] // 2
    lane = lax.broadcasted_iota(jnp.int32, value.shape, 1)
    return pltpu.roll(value, half, 1) * jnp.where(lane < half, first, second)


def sign(value, first, second):
    lane = lax.broadcasted_iota(jnp.int32, value.shape, 1)
    return value * jnp.where(lane < value.shape[1] // 2, first, second)


def series(square, first, terms):
    value = jnp.full_like(square, 1.0 / math.factorial(first + 2 * terms))
    for k in range(terms - 1, -1, -1):
        value = 1.0 / math.factorial(first + 2 * k) - value * square
    return value


def turns(ticks, whole):
    turn = ((ticks + whole // 2) & (whole - 1)) - whole // 2
    angle = turn.astype(F32) * (-math.pi / whole)
    square = angle * angle
    sine = angle * series(square, 1, 5)
    return 1.0 - 2.0 * sine * sine, 2.0 * sine * series(square, 0, 6)


def image_rows(blocks):
    half = blocks[0].shape[0] // 2
    cross = []
    for block in blocks:
        cross += [block[half:], -block[:half]]
    return jnp.concatenate(
        [jnp.concatenate(blocks, axis=0).T, jnp.concatenate(cross, axis=0).T], axis=0
    )


def cycle_kernel(
    nf, nc, x_hbm, obs_hbm, cells_hbm, counts_hbm, ctab_hbm, rtab_hbm, ttab_hbm, turn_hbm,
    back_out, base_out, tab,
    xbuf, obs, cells, counts, turn_in, turn_out, t2, tt, acc, bacc,
    s_send, s_recv, g_send, g_recv, right, right_t, r1r, r1i, left, inner, held,
    r_send, r_recv, b_send, b_recv,
    tok, in_sem, sa, ra, sb, rb, sc, rc, sd, rd,
):
    f = lax.axis_index("facet")
    c = lax.axis_index("col")
    window = S // 8
    half = window // 2
    two = 2 * window
    parts = window // 16
    pc = nf
    rows = xbuf.shape[1]
    groups = nf // 8
    vis = obs.shape[2]
    if nc % 2:
        col_steps = [(d, 0) for d in range(1, nc)]
        wide = 1
    else:
        col_steps = [(d, k) for d in range(nc // 2 - 1, -1, -1) for k in range(2) if d or k]
        wide = 2
    near_steps = [step for step in col_steps if step[0] == 0]
    far_steps = [step for step in col_steps if step[0]]

    def col_at(step, sign):
        if nc % 2:
            return lax.rem(c + nc + sign * step[0], nc)
        top = lax.rem(c // 2 + nc // 2 + sign * step[0], nc // 2)
        return 2 * top + lax.rem(c + step[1], 2)

    def pair_at(q):
        return lax.rem(f // 2 + q, 4)

    def group_of(q):
        return 0 if q in waits[0] else 1

    def facet_link(src_buf, dst_buf, send, recv, part, peer):
        return pltpu.make_async_remote_copy(
            src_buf.at[part * nf + peer], dst_buf.at[part * nf + f], send, recv, (peer, c), MESH
        )

    def col_link(src, dst, send, recv, peer):
        return pltpu.make_async_remote_copy(src, dst, send, recv, (f, peer), MESH)

    def sum_of(buf, start, count, send, recv):
        some = buf.at[start : start + count]
        return pltpu.make_async_remote_copy(some, some, send, recv, (mate, c), MESH)

    waits = ((0, 1), (3, 2))
    mate = f + 1 - 2 * lax.rem(f, 2)

    barrier = pltpu.get_barrier_semaphore()
    place, last_place = f // 2, nf // 2 - 1
    low, high = place > 0, place < last_place
    far_low, far_high = place > 1, place < last_place - 1

    def signal(sem, facet, col):
        pl.semaphore_signal(sem, inc=1, device_id=(facet, col), device_id_type=MESH)

    def pass_on(way):
        pl.semaphore_wait(tok.at[way], 1)
        signal(tok.at[way], f + 2 - 4 * way, c)

    for d in range(1, nc):
        signal(barrier, f, lax.rem(c + d, nc))
    signal(barrier, mate, c)

    @pl.when(high)
    def _():
        signal(barrier, f + 2, c)
        pl.when(~low)(lambda: signal(barrier, mate + 2, c))

    @pl.when(low)
    def _():
        signal(barrier, f - 2, c)
        pl.when(~high)(lambda: signal(barrier, mate - 2, c))


    n_groups = nc // wide
    chunk = wide * window

    def group_at(d):
        return lax.rem(c // wide + n_groups + d, n_groups)

    far_groups = list(range(n_groups - 1, 0, -1)) if wide == 2 else list(range(1, nc))

    extent = xbuf.shape[2]
    quarter = extent // 4
    depths = [slice(0, quarter), slice(quarter, 2 * quarter), slice(2 * quarter, 4 * quarter)]
    x_loads = [
        pltpu.make_async_copy(x_hbm.at[:, :, lanes], xbuf.at[:, :, lanes], in_sem.at[n])
        for n, lanes in enumerate(depths)
    ]
    mine_at = pl.ds(pl.multiple_of(group_at(0) * 2 * chunk, 2 * chunk), 2 * chunk)
    mine_load = pltpu.make_async_copy(ctab_hbm.at[mine_at], tab.at[mine_at], in_sem.at[3])
    row_load = pltpu.make_async_copy(rtab_hbm, t2, in_sem.at[9])
    small_loads = [
        pltpu.make_async_copy(turn_hbm.at[f, c], turn_in, in_sem.at[4]),
        pltpu.make_async_copy(turn_hbm.at[:, c, f], turn_out, in_sem.at[5]),
        pltpu.make_async_copy(obs_hbm, obs, in_sem.at[6]),
        pltpu.make_async_copy(cells_hbm, cells, in_sem.at[7]),
        pltpu.make_async_copy(counts_hbm, counts, in_sem.at[8]),
    ]
    turned_load = pltpu.make_async_copy(ttab_hbm, tt, in_sem.at[10])
    for load in x_loads:
        load.start()

    spacing = IMAGE // extent
    lr, li = turns(
        lax.broadcasted_iota(jnp.int32, (16, extent), 0)
        * lax.broadcasted_iota(jnp.int32, (16, extent), 1),
        extent,
    )
    high_rows = lax.broadcasted_iota(jnp.int32, (wide * parts, extent), 0)
    place_q = lax.broadcasted_iota(jnp.int32, (wide * parts, extent), 1)
    taper = 0.8 - 0.2 * turns(2 * place_q + 1, 2 * extent)[0]
    taper *= 1.0 / math.sqrt(extent)
    for d in far_groups:
        cols = wide * group_at(d) + high_rows // parts
        freqs = cols * (IMAGE // 4) + ((29 * cols + 3) & (spacing - 1))
        freqs += spacing * 16 * (high_rows & (parts - 1))
        hr, hi = turns(freqs * place_q, IMAGE)
        hr, hi = hr * taper, hi * taper
        for i in range(wide * parts):
            er, ei = hr[i : i + 1], hi[i : i + 1]
            k, u = i // parts, i % parts
            at = group_at(d) * 2 * chunk + u // 2 * chunk + k * window + u % 2 * 16
            at = pl.multiple_of(at, 16)
            tab[pl.ds(at, 16), :] = (lr * er - li * ei).astype(BF)
            tab[pl.ds(at + half, 16), :] = (lr * ei + li * er).astype(BF)

    def strip_term(d, lanes):
        at = pl.multiple_of(group_at(d) * 2 * chunk, 2 * chunk)
        return lax.dot_general(
            tab[pl.ds(at, 2 * chunk), lanes],
            xbuf[:, :, lanes].reshape(2 * rows, -1),
            NT,
            preferred_element_type=F32,
        )

    def strips(d, both):
        for k in range(wide):
            for part in range(parts):
                at = part // 2 * chunk + k * window + part % 2 * 16
                real, imag = both[at : at + 16], both[at + half : at + half + 16]
                block = [real[:, :rows] - imag[:, rows:], imag[:, :rows] + real[:, rows:]]
                s_send[wide * group_at(d) + k, part] = jnp.concatenate(block, axis=0).astype(BF)

    messages = [[0], [1], list(range(2, parts))]

    def strip_link(step, some):
        peer = col_at(step, 1)
        at = ra.at[messages.index(some) * len(far_steps) + far_steps.index(step)]
        some = slice(some[0], some[-1] + 1)
        return col_link(s_send.at[peer, some], s_recv.at[c, some], sa.at[0], at, peer)

    def near_link(step):
        peer = col_at(step, 1)
        at = ra.at[len(messages) * len(far_steps) + near_steps.index(step)]
        return col_link(s_send.at[peer], s_recv.at[c], sa.at[0], at, peer)

    sums = [0.0] * len(far_groups)
    for lanes, load in zip(depths, x_loads):
        load.wait()
        if lanes is depths[0]:
            mine_load.start()
            for load in small_loads:
                load.start()
        if lanes is depths[-1]:
            turned_load.start()
        for n, d in enumerate(far_groups):
            sums[n] += strip_term(d, lanes)
    for d, both in zip(far_groups, sums):
        strips(d, both)
    greeted = (low, high, place == 1, place == last_place - 1)
    pl.semaphore_wait(barrier, nc + sum(one.astype(jnp.int32) for one in greeted))
    for some in messages:
        for step in far_steps:
            strip_link(step, some).start()
    pl.when((place == 1) & high)(lambda: signal(tok.at[0], f + 2, c))
    pl.when((place == last_place - 1) & low)(lambda: signal(tok.at[1], f - 2, c))
    mine_load.wait()
    strips(0, strip_term(0, slice(None)))
    for step in near_steps:
        near_link(step).start()

    @pl.when(far_low & high)
    def _():
        pass_on(0)

    @pl.when(far_high & low)
    def _():
        pass_on(1)

    turned_load.wait()

    def window_term(block, src):
        at = pl.multiple_of(src * rows, rows)
        return jnp.dot(block, tt[pl.ds(at, rows), :], preferred_element_type=F32)

    acc[...] = window_term(s_send[c].reshape(two, rows), c)

    for load in small_loads:
        load.wait()

    def send_windows(some):
        def act(index):
            for part in some:
                facet_link(g_send, g_recv, sb.at[0], rb.at[part], part, index).start()

        for index in range(nf - 1, -1, -1):
            pl.when(index != f)(functools.partial(act, index))
        for part in some:
            g_recv[part * nf + f] = g_send[part * nf + f]

    first = cells[0, pl.ds(f, 1), :]
    second = cells[1, pl.ds(f, 1), :]

    def wave(count, step, cell):
        return turns(step * lax.broadcasted_iota(jnp.int32, (count, vis), 0) * cell, S)

    scale = 1.0 / math.sqrt(vis)
    live = lax.broadcasted_iota(jnp.int32, (1, vis), 1) < counts[f]
    gain = jnp.where(live, scale, 0.0)
    m0r, m0i = wave(16, 1, second)
    m0r, m0i = m0r * gain, m0i * gain
    r1r[...], r1i[...] = wave(S // 16, 16, second)

    def right_body(i, carry):
        er, ei = r1r[pl.ds(i, 1), :], r1i[pl.ds(i, 1), :]
        b = i // parts
        k = i - b * parts
        at = pl.multiple_of(k * (2 * S // parts) + b * half, 16)
        right[pl.ds(at, 16), :] = (m0r * er - m0i * ei).astype(BF)
        right[pl.ds(at + 16, 16), :] = (m0r * ei + m0i * er).astype(BF)
        return carry

    lax.fori_loop(0, S // 16, right_body, 0)

    for step in near_steps:
        near_link(step).wait_recv()
        src = col_at(step, -1)
        acc[...] += window_term(s_recv[src].reshape(two, rows), src)

    def windows(some):
        lo, hi = some[0], some[-1] + 1
        total = acc[lo * half : hi * half]
        for step in far_steps:
            strip_link(step, some).wait_recv()
            src = col_at(step, -1)
            block = s_recv[src, lo:hi].reshape((hi - lo) * half, rows)
            total += window_term(block, src)
        for part in some:
            at = (part - lo) * half
            for j in range(pc):
                u = total[at : at + 16, j * two : (j + 1) * two]
                v = total[at + 16 : at + half, j * two : (j + 1) * two]
                turn = turn_in[j]
                same, cross = turn[0:1], turn[1:2]
                win = u * same + spin(v, -1.0, 1.0) * same
                win += pltpu.roll(u, window, 1) * cross + v * sign(cross, 1.0, -1.0)
                g_send[part * pc + j] = win.astype(BF)
        if 0 in some:
            pl.when(far_high & ~low)(lambda: pl.semaphore_wait(tok.at[1], 1))
            pl.when(far_low & ~high)(lambda: pl.semaphore_wait(tok.at[0], 1))
        send_windows(some)

    windows(messages[0])

    windows(messages[1])
    windows(messages[2])
    row_load.start()

    l0r, l0i = wave(16, 1, first)
    l1r, l1i = wave(max(groups * parts, 8), 16, first)
    for i in range(groups * parts):
        er, ei = l1r[i : i + 1], l1i[i : i + 1]
        at = i // parts * two + i % parts * 16
        real = (l0r * er - l0i * ei).astype(BF).astype(F32)
        imag = (l0r * ei + l0i * er).astype(BF).astype(F32)
        left[0, at : at + 16, :] = real
        left[0, at + window : at + window + 16, :] = -imag
        left[1, at : at + 16, :] = imag
        left[1, at + window : at + window + 16, :] = real

    deep = 2 * S // parts

    def turn_body(b, carry):
        pieces = [right[pl.ds(pl.multiple_of(k * deep + b * half, 16), half), :] for k in range(parts)]
        at = pl.multiple_of(b * two, two)
        right_t[:, pl.ds(at, two)] = jnp.concatenate(pieces, axis=0).T
        return carry

    lax.fori_loop(0, S // window, turn_body, 0)

    def pred_term(some, g):
        blocks = []
        for part in some:
            for b in range(8):
                block = g_recv[part * nf + g * 8 + b].astype(F32)
                blocks += [block, spin(block, -1.0, 1.0)]
        return jnp.dot(
            jnp.concatenate(blocks, axis=0).T.astype(BF),
            right[some[0] * deep : (some[-1] + 1) * deep, :],
            preferred_element_type=F32,
        )

    def take_windows(some):
        for part in some:
            sum_of(g_recv, part * nf, nf - 1, sb.at[0], rb.at[part]).wait_recv()

    early_parts, late_parts = list(range(parts // 2)), list(range(parts // 2, parts))
    take_windows(early_parts)
    for g in range(groups):
        inner[g * two : (g + 1) * two] = pred_term(early_parts, g)

    take_windows(late_parts)
    res_r, res_i = obs[0, pl.ds(f, 1), :], obs[1, pl.ds(f, 1), :]
    for g in range(groups):
        at = slice(g * two, (g + 1) * two)
        value = inner[at] + pred_term(late_parts, g)
        unscale = 1.0 / (scale * S)
        res_r -= jnp.sum(value * left[0, at], axis=0, keepdims=True) * unscale
        res_i -= jnp.sum(value * left[1, at], axis=0, keepdims=True) * unscale
    held[...] = (res_r * left[0] + res_i * left[1]).astype(BF)

    def send_back(part, index):
        def act(group):
            recv = rc.at[2 * part + group]
            facet_link(r_send, r_recv, sc.at[0], recv, part, index).start()

        near = lax.rem(place - index // 2 + nf // 2, 4)
        pl.when((near < 2) & (index != f))(lambda: act(0))
        pl.when(near >= 2)(lambda: act(1))

    def grid_blocks(lo, hi, after=None):
        grid = jnp.dot(held[...], right_t[:, lo * two : hi * two], preferred_element_type=F32)
        turned = [grid[g * two : (g + 1) * two].T for g in range(groups)]
        for part in range(2):
            for g in range(groups):
                for b in range(lo, hi):
                    turn = turn_out[g * 8 + b]
                    same, cross = turn[0:1], turn[1:2]
                    starts = [(b - lo) * two + (2 * part + k) * half for k in range(2)]
                    u, v = (
                        jnp.concatenate([turned[g][at + k : at + k + 16] for at in starts], axis=0)
                        for k in (0, 16)
                    )
                    block = (u + spin(v, 1.0, -1.0)) * same
                    block -= pltpu.roll(u, window, 1) * cross + v * sign(cross, -1.0, 1.0)
                    r_send[part * nf + g * 8 + b] = block.astype(BF)
            if after is not None and part == 0:
                after()

    def send_backs(part, lo, hi):
        for g in range(groups):
            for b in range(lo, hi):
                send_back(part, g * 8 + b)

    grid_blocks(0, 2, lambda: send_backs(0, 0, 2))
    grid_blocks(6, 8)
    send_backs(1, 0, 2)
    for part in range(2):
        send_backs(part, 6, 8)
    grid_blocks(2, 6)
    for part in range(2):
        send_backs(part, 2, 6)
        r_recv[part * nf + f] = r_send[part * nf + f]

    row_load.wait()

    def take_backs(part, pairs):
        count = 4 * groups - (0 in pairs)
        at = rc.at[2 * part + waits.index(pairs)]
        sum_of(r_recv, part * nf, count, sc.at[0], at).wait_recv()

    def back_blocks(part, pairs):
        blocks = []
        for q in pairs:
            for g in range(groups):
                first = g * 8 + 2 * pair_at(q)
                pieces = [r_recv[part * nf + first + h] for h in range(2)]
                spun = [spin(piece.astype(F32), 1.0, -1.0).astype(BF) for piece in pieces]
                block = jnp.concatenate(
                    [jnp.concatenate(pieces, axis=1), jnp.concatenate(spun, axis=1)], axis=0
                )
                blocks.append((block, pl.multiple_of(first * two, 2 * two)))
        return blocks

    def lanes_of(d):
        return pl.ds(pl.multiple_of(wide * group_at(d) * rows, wide * rows), wide * rows)

    def back_term(blocks, d):
        return sum(
            jnp.dot(block, t2[pl.ds(at, 2 * two), lanes_of(d)], preferred_element_type=F32)
            for block, at in blocks
        )

    def keep(part, d, total):
        for k in range(wide):
            piece = total[:, k * rows : (k + 1) * rows]
            b_send[part * nc + wide * group_at(d) + k] = piece.astype(BF)

    def send_strips_back(part, d):
        for step in col_steps:
            if step[0] == d:
                peer = col_at(step, 1)
                at = rd.at[0 if step in near_steps else 1 + part]
                col_link(
                    b_send.at[part * nc + peer], b_recv.at[part * nc + c], sd.at[0], at, peer
                ).start()

    take_backs(0, waits[0])
    for d in far_groups:
        bacc[:, lanes_of(d)] = back_term(back_blocks(0, waits[0]), d)
    take_backs(0, waits[1])
    for d in far_groups:
        keep(0, d, bacc[:, lanes_of(d)] + back_term(back_blocks(0, waits[1]), d))
        send_strips_back(0, d)
    for pairs in waits:
        take_backs(1, pairs)
    for d in far_groups:
        keep(1, d, back_term(back_blocks(1, waits[0] + waits[1]), d))
        send_strips_back(1, d)
    both = [back_blocks(part, waits[0] + waits[1]) for part in range(2)]
    both = [(jnp.concatenate([one[0], two_[0]], axis=0), one[1]) for one, two_ in zip(*both)]
    total = back_term(both, 0)
    for part in range(2):
        keep(part, 0, total[part * window : (part + 1) * window])
        send_strips_back(part, 0)
        b_recv[part * nc + c] = b_send[part * nc + c]
    if near_steps:
        sum_of(b_recv, 0, 2 * len(near_steps), sd.at[0], rd.at[0]).wait_recv()
    mine = [b_recv[part * nc + wide * group_at(0) + k] for part in range(2) for k in range(wide)]
    base_out[...] = jnp.dot(
        image_rows(mine), tab[mine_at, :], preferred_element_type=F32
    )
    for part in range(2):
        sum_of(b_recv, 0, len(far_steps), sd.at[0], rd.at[1 + part]).wait_recv()
        for d in range(1, n_groups):
            for k in range(wide):
                at = part * nc + wide * group_at(d) + k
                back_out[((d - 1) * 2 + part) * wide + k] = b_recv[at]
    sum_of(s_send, 0, nc - 1, sa.at[0], ra.at[0]).wait_send()
    sum_of(b_send, 0, 2 * (nc - 1), sd.at[0], rd.at[0]).wait_send()
    sum_of(g_send, 0, parts * (nf - 1), sb.at[0], rb.at[0]).wait_send()
    sum_of(r_send, 0, 2 * (nf - 1), sc.at[0], rc.at[0]).wait_send()


def image_kernel(nc, back, base, tab, out, buf, sem):
    c = lax.axis_index("col")
    wide = 2 - nc % 2
    n_groups = nc // wide
    tiles, rows, tile = buf.shape[0], buf.shape[2], buf.shape[3]
    depth = 2 * wide * back.shape[1]
    strip = image_rows([back[k] for k in range(back.shape[0])])
    stores = []
    for t in range(tiles):
        lanes = slice(t * tile, (t + 1) * tile)
        piece = base[:, lanes]
        for d in range(1, n_groups):
            at = pl.multiple_of(lax.rem(c // wide + d, n_groups) * depth, depth)
            piece += jnp.dot(
                strip[:, (d - 1) * depth : d * depth],
                tab[pl.ds(at, depth), lanes],
                preferred_element_type=F32,
            )
        for part in range(2):
            buf[t, part] = piece[part * rows : (part + 1) * rows]
        store = pltpu.make_async_copy(buf.at[t], out.at[:, :, lanes], sem.at[t])
        store.start()
        stores.append(store)
    for store in stores:
        store.wait()


def solution(mesh):
    nf, nc = mesh.shape["facet"], mesh.shape["col"]

    def on_device(facets, observed, uv_cells, counts):
        rows, extent = facets.shape[1:]
        vis = observed.shape[2]
        pc = counts.shape[0]
        window = S // 8
        two = 2 * window
        groups = nf // 8
        wide = 2 - nc % 2
        parts = window // 16
        assert pc == nf and nf % 8 == 0 and nf <= 32 and nc > wide
        constants = make_constants(nf, nc, pc, extent)
        vmem = pl.BlockSpec(memory_space=pltpu.VMEM)
        hbm = pl.BlockSpec(memory_space=pltpu.HBM)
        dma = pltpu.SemaphoreType.DMA
        fixed = functools.partial(pltpu.with_memory_space_constraint, memory_space=pltpu.HBM)
        back, base, tab = pl.pallas_call(
            functools.partial(cycle_kernel, nf, nc),
            out_shape=(
                jax.ShapeDtypeStruct((2 * nc - 2 * wide, window, rows), BF),
                jax.ShapeDtypeStruct((2 * rows, extent), F32),
                jax.ShapeDtypeStruct((nc * two, extent), BF),
            ),
            in_specs=[hbm] * 8,
            out_specs=(vmem, vmem, vmem),
            scratch_shapes=[
                pltpu.VMEM((2, rows, extent), BF),
                pltpu.VMEM((2, pc, vis), F32),
                pltpu.VMEM((2, pc, vis), jnp.int32),
                pltpu.SMEM((pc,), jnp.int32),
                pltpu.VMEM((pc, 2, two), F32),
                pltpu.VMEM((nf, 2, two), F32),
                pltpu.VMEM((pc * two, extent), BF),
                pltpu.VMEM((extent, pc * two), BF),
                pltpu.VMEM((two, pc * two), F32),
                pltpu.VMEM((window, extent), F32),
                pltpu.VMEM((nc, parts, window // 2, rows), BF),
                pltpu.VMEM((nc, parts, window // 2, rows), BF),
                pltpu.VMEM((parts * pc, 16, two), BF),
                pltpu.VMEM((parts * nf, 16, two), BF),
                pltpu.VMEM((2 * S, vis), BF),
                pltpu.VMEM((vis, 2 * S), BF),
                pltpu.VMEM((S // 16, vis), F32),
                pltpu.VMEM((S // 16, vis), F32),
                pltpu.VMEM((2, groups * two, vis), F32),
                pltpu.VMEM((groups * two, vis), F32),
                pltpu.VMEM((groups * two, vis), BF),
                pltpu.VMEM((2 * nf, window // 2, two), BF),
                pltpu.VMEM((2 * pc, window // 2, two), BF),
                pltpu.VMEM((2 * nc, window, rows), BF),
                pltpu.VMEM((2 * nc, window, rows), BF),
                pltpu.SemaphoreType.REGULAR((2,)),
                dma((11,)),
                dma((1,)), dma((3 * (nc - wide) + wide - 1,)), dma((1,)), dma((parts,)),
                dma((1,)), dma((4,)), dma((1,)), dma((3,)),
            ],
            compiler_params=pltpu.CompilerParams(
                collective_id=0, has_side_effects=True, vmem_limit_bytes=44 * 2**20
            ),
            name="cycle",
        )(
            fixed(facets), fixed(observed), fixed(uv_cells), fixed(counts),
            *(fixed(jnp.asarray(constant)) for constant in constants),
        )
        tile = 256
        return pl.pallas_call(
            functools.partial(image_kernel, nc),
            out_shape=jax.ShapeDtypeStruct((2, rows, extent), F32),
            in_specs=[vmem, vmem, vmem],
            out_specs=hbm,
            scratch_shapes=[
                pltpu.VMEM((extent // tile, 2, rows, tile), F32),
                dma((extent // tile,)),
            ],
            compiler_params=pltpu.CompilerParams(vmem_limit_bytes=16 * 2**20),
            name="image",
        )(back, base, tab)

    return jax.shard_map(
        on_device,
        mesh=mesh,
        in_specs=(
            P(None, ("facet", "col"), None),
            P(None, "col", None),
            P(None, "col", None),
            P("col"),
        ),
        out_specs=P(None, ("facet", "col"), None),
        check_vma=False,
    )
```
